8 devices in a mesh: my: 4 (over z, y, x), mx: 2 (over core).
Axes of the slice: x: 2, y: 2, z: 1, core: 2. Of those that a mesh axis runs over, the one named last changes fastest.
Arguments:
- x_in: bfloat16 [256, 5120], P(None, 'mx')
- seq_lens: int32 [256], P('mx')
- gain_attn: bfloat16 [5120], P('mx')
- gain_mlp: bfloat16 [5120], P('mx')
- w_q: bfloat16 [5120, 5120], P('mx', 'my')
- b_q: bfloat16 [5120], P('my')
- w_k: bfloat16 [5120, 1024], P('mx', 'my')
- b_k: bfloat16 [1024], P('my')
- w_v: bfloat16 [5120, 1024], P('mx', 'my')
- b_v: bfloat16 [1024], P('my')
- w_o: bfloat16 [5120, 5120], P('my', 'mx')
- w_gate: bfloat16 [5120, 27392], P('mx', 'my')
- w_up: bfloat16 [5120, 27392], P('mx', 'my')
- w_down: bfloat16 [27392, 5120], P('my', 'mx')
- k_cache: bfloat16 [256, 256, 8, 128], P('mx', None, 'my')
- v_cache: bfloat16 [256, 256, 8, 128], P('mx', None, 'my')
Outputs:
- output 1: bfloat16 [256, 5120], P(None, 'mx')
- output 2: bfloat16 [256, 256, 8, 128], P('mx', None, 'my')
- output 3: bfloat16 [256, 256, 8, 128], P('mx', None, 'my')
All inputs are finite; a program needn't handle non-finite values.
Results may differ from the reference program's by a relative error of at most 0.0165306.
Values are sent between devices in bfloat16 or wider.
A program may use at most 1 GiB of HBM per device.

```python
import jax
import jax.numpy as jnp
from jax import lax

D = 5120
HEADS = 40
KV_HEADS = 8
HEAD = 128
FF = 27392
BATCH = 256
SEQ = 256
NORM_EPS = 1e-6
ROPE_THETA = 1000000.0
GROUP = HEADS // KV_HEADS


def setup_inputs(seed: int = 0) -> dict:
    key_list = jax.random.split(jax.random.key(seed), 17)
    q_width = HEADS * HEAD
    kv_width = KV_HEADS * HEAD
    cache_shape = (BATCH, SEQ, KV_HEADS, HEAD)

    def normal(key_index, shape, scale, offset=0.0):
        samples = jax.random.normal(key_list[key_index], shape, jnp.float32)
        return (offset + scale * samples).astype(jnp.bfloat16)

    lens_draw = jax.random.randint(key_list[0], (BATCH,), 0, SEQ)
    full_row = jax.random.randint(key_list[1], (), 0, BATCH)
    seq_lens = jnp.where(jnp.arange(BATCH) == full_row, SEQ - 1, lens_draw).astype(jnp.int32)
    return {
        "x_in": normal(2, (BATCH, D), 1.0),
        "seq_lens": seq_lens,
        "gain_attn": normal(3, (D,), 0.3, 1.0),
        "gain_mlp": normal(4, (D,), 0.3, 1.0),
        "w_q": normal(5, (D, q_width), 2.0 * D ** -0.5),
        "b_q": normal(6, (q_width,), 1.0),
        "w_k": normal(7, (D, kv_width), D ** -0.5),
        "b_k": normal(8, (kv_width,), 1.0),
        "w_v": normal(9, (D, kv_width), D ** -0.5),
        "b_v": normal(10, (kv_width,), 1.0),
        "w_o": normal(11, (q_width, D), q_width ** -0.5),
        "w_gate": normal(12, (D, FF), D ** -0.5),
        "w_up": normal(13, (D, FF), D ** -0.5),
        "w_down": normal(14, (FF, D), FF ** -0.5),
        "k_cache": normal(15, cache_shape, 1.0),
        "v_cache": normal(16, cache_shape, 1.0),
    }


def rms_norm(rows_in, gain_vec):
    rows_f32 = rows_in.astype(jnp.float32)
    mean_sq = jnp.mean(rows_f32 * rows_f32, axis=-1, keepdims=True)
    return (rows_f32 * lax.rsqrt(mean_sq + NORM_EPS) * gain_vec.astype(jnp.float32)).astype(jnp.bfloat16)


def apply_rotary(vectors, positions):
    half_dim = HEAD // 2
    inv_freq = ROPE_THETA ** (-2.0 * jnp.arange(half_dim, dtype=jnp.float32) / HEAD)
    angles = positions.astype(jnp.float32)[:, None, None] * inv_freq
    cos_tab = jnp.cos(angles)
    sin_tab = jnp.sin(angles)
    lower_half = vectors[..., :half_dim]
    upper_half = vectors[..., half_dim:]
    return jnp.concatenate([lower_half * cos_tab - upper_half * sin_tab, upper_half * cos_tab + lower_half * sin_tab], axis=-1)


def attend_one(row_inputs):
    q_row, k_rows, v_rows, length = row_inputs
    q_grouped = q_row.reshape(KV_HEADS, GROUP, HEAD).astype(jnp.float32)
    scores = jnp.einsum("kgd,skd->kgs", q_grouped, k_rows.astype(jnp.float32)) * HEAD ** -0.5
    visible = (jnp.arange(SEQ) <= length)[None, None, :]
    scores = jnp.where(visible, scores, -jnp.inf)
    weights = jnp.exp(scores - jnp.max(scores, axis=-1, keepdims=True))
    weight_sum = jnp.sum(weights, axis=-1, keepdims=True)
    weighted = jnp.einsum("kgs,skd->kgd", weights.astype(jnp.bfloat16).astype(jnp.float32), v_rows.astype(jnp.float32))
    return (weighted / weight_sum).astype(jnp.bfloat16).reshape(HEADS * HEAD)


def reference(x_in, seq_lens, gain_attn, gain_mlp, w_q, b_q, w_k, b_k, w_v, b_v, w_o, w_gate, w_up, w_down, k_cache, v_cache):
    normed = rms_norm(x_in, gain_attn)
    q_vals = jnp.dot(normed, w_q, preferred_element_type=jnp.float32) + b_q.astype(jnp.float32)
    k_vals = jnp.dot(normed, w_k, preferred_element_type=jnp.float32) + b_k.astype(jnp.float32)
    v_vals = jnp.dot(normed, w_v, preferred_element_type=jnp.float32) + b_v.astype(jnp.float32)
    q_rot = apply_rotary(q_vals.reshape(BATCH, HEADS, HEAD), seq_lens).astype(jnp.bfloat16)
    k_rot = apply_rotary(k_vals.reshape(BATCH, KV_HEADS, HEAD), seq_lens).astype(jnp.bfloat16)
    v_new = v_vals.reshape(BATCH, KV_HEADS, HEAD).astype(jnp.bfloat16)
    at_slot = (jnp.arange(SEQ)[None, :] == seq_lens[:, None])[:, :, None, None]
    k_cache_out = jnp.where(at_slot, k_rot[:, None], k_cache)
    v_cache_out = jnp.where(at_slot, v_new[:, None], v_cache)
    attn_rows = lax.map(attend_one, (q_rot, k_cache_out, v_cache_out, seq_lens))
    x_mid = (x_in.astype(jnp.float32) + jnp.dot(attn_rows, w_o, preferred_element_type=jnp.float32)).astype(jnp.bfloat16)
    normed_mlp = rms_norm(x_mid, gain_mlp)
    gate_proj = jnp.dot(normed_mlp, w_gate, preferred_element_type=jnp.float32)
    up_proj = jnp.dot(normed_mlp, w_up, preferred_element_type=jnp.float32)
    hidden_act = (jax.nn.silu(gate_proj) * up_proj).astype(jnp.bfloat16)
    x_out = (x_mid.astype(jnp.float32) + jnp.dot(hidden_act, w_down, preferred_element_type=jnp.float32)).astype(jnp.bfloat16)
    return (x_out, k_cache_out, v_cache_out)
```

```python
import jax
import jax.numpy as jnp
from jax import lax
from jax.experimental import pallas as pl
from jax.experimental.pallas import tpu as pltpu
from jax.sharding import PartitionSpec as P

HEAD = 128
NORM_EPS = 1e-6
ROPE_THETA = 1000000.0
MESH = pl.DeviceIdType.MESH
F32 = jnp.float32
BF16 = jnp.bfloat16
QPAD = 16
VMEM = pltpu.VMEM
DMA = pltpu.SemaphoreType.DMA


def any_specs(count):
    return [pl.BlockSpec(memory_space=pl.ANY)] * count


def vmem_specs(count):
    return [pl.BlockSpec(memory_space=pltpu.VMEM)] * count


def project_kernel(x_ref, gain_ref, bias_ref, cos_ref, sin_ref, wq_hbm, wk_hbm, wv_hbm, q_out, kv_out,
                   w_buf, normed, sq_send, sq_recv, part_send, part_recv, part_own, w_sems, send_sems, recv_sems):
    me = lax.axis_index("mx")
    peer = 1 - me
    rows, depth = x_ref.shape
    half = rows // 2
    width = 2 * HEAD
    q_chunks = wq_hbm.shape[1] // width
    chunks = q_chunks + 2

    def weight_copy(index):
        if index < q_chunks:
            source = wq_hbm.at[:, pl.ds(index * width, width)]
        else:
            source = (wk_hbm, wv_hbm)[index - q_chunks]
        return pltpu.make_async_copy(source, w_buf.at[index], w_sems.at[index])

    for index in range(chunks):
        weight_copy(index).start()
    barrier = pltpu.get_barrier_semaphore()
    pl.semaphore_signal(barrier, inc=1, device_id={"mx": peer}, device_id_type=MESH)

    total = jnp.zeros((rows, HEAD), F32)
    for start in range(0, depth, HEAD):
        block = x_ref[:, start:start + HEAD].astype(F32)
        total = total + block * block
    sq_own = jnp.sum(total, axis=1, keepdims=True)
    sq_send[...] = jnp.broadcast_to(sq_own, (rows, HEAD))
    pl.semaphore_wait(barrier, 1)

    def remote(source, target, slot):
        return pltpu.make_async_remote_copy(
            src_ref=source, dst_ref=target, send_sem=send_sems.at[slot], recv_sem=recv_sems.at[slot],
            device_id={"mx": peer}, device_id_type=MESH)

    sq_copy = remote(sq_send, sq_recv, chunks)
    sq_copy.start()
    sq_copy.wait()
    scale = lax.rsqrt((sq_send[...] + sq_recv[...]) / (2 * depth) + NORM_EPS)
    for start in range(0, depth, HEAD):
        block = x_ref[:, start:start + HEAD].astype(F32)
        gain = gain_ref[:, start:start + HEAD].astype(F32)
        normed[:, start:start + HEAD] = (block * scale * gain).astype(BF16)

    own_rows = pl.ds(pl.multiple_of(me * half, half), half)
    peer_rows = pl.ds(pl.multiple_of(peer * half, half), half)
    copies = []
    for index in range(chunks):
        weight_copy(index).wait()
        weights = w_buf.at[index]
        part_send[index] = jnp.dot(normed[peer_rows, :], weights[...], preferred_element_type=F32).astype(BF16)
        part_own[index] = jnp.dot(normed[own_rows, :], weights[...], preferred_element_type=F32)
        copies.append(remote(part_send.at[index], part_recv.at[index], index))
        copies[index].start()

    cos_tab = cos_ref[...]
    sin_tab = sin_ref[...]
    for index in range(chunks):
        copies[index].wait()
        for head in range(2):
            lanes = slice(head * HEAD, (head + 1) * HEAD)
            columns = slice(index * width + head * HEAD, index * width + (head + 1) * HEAD)
            value = part_own[index][:, lanes] + part_recv[index][:, lanes].astype(F32) + bias_ref[:, columns].astype(F32)
            if index < chunks - 1:
                value = value * cos_tab + pltpu.roll(value, HEAD // 2, 1) * sin_tab
            if index < q_chunks:
                q_out[:, columns] = value.astype(BF16)
            else:
                kv_out[:, (index - q_chunks) * width + head * HEAD:(index - q_chunks) * width + (head + 1) * HEAD] = value.astype(BF16)


def project(x_in, gain, bias, cos_tab, sin_tab, w_q, w_k, w_v):
    rows, depth = x_in.shape
    half = rows // 2
    width = 2 * HEAD
    chunks = w_q.shape[1] // width + 2
    return pl.pallas_call(
        project_kernel,
        name="project",
        out_shape=(jax.ShapeDtypeStruct((half, w_q.shape[1]), BF16), jax.ShapeDtypeStruct((half, 2 * width), BF16)),
        in_specs=vmem_specs(5) + any_specs(3),
        out_specs=tuple(vmem_specs(2)),
        scratch_shapes=[
            VMEM((chunks, depth, width), BF16),
            VMEM((rows, depth), BF16),
            VMEM((rows, HEAD), F32),
            VMEM((rows, HEAD), F32),
            VMEM((chunks, half, width), BF16),
            VMEM((chunks, half, width), BF16),
            VMEM((chunks, half, width), F32),
            DMA((chunks,)),
            DMA((chunks + 1,)),
            DMA((chunks + 1,)),
        ],
        compiler_params=pltpu.CompilerParams(collective_id=0, has_side_effects=True, vmem_limit_bytes=48 << 20),
    )(x_in, gain, bias, cos_tab, sin_tab, w_q, w_k, w_v)


SLOTS = 4
ROWS_STEP = 8


def attend_kernel(lens_ref, q_ref, kv_ref, k_hbm, v_hbm, o_ref, k_out, v_out,
                  k_buf, v_buf, q_wide, q_packed, kv_wide, o_wide, parity, scores, weights, sums, in_sems, out_sems):
    batch, kv_rows, _ = k_hbm.shape
    q_heads = q_ref.shape[1] // HEAD
    group = q_heads // 2
    steps = batch // ROWS_STEP

    def load(step, kind):
        slot = lax.rem(step, SLOTS)
        source, target = ((k_hbm, k_buf), (v_hbm, v_buf))[kind]
        return pltpu.make_async_copy(source.at[pl.ds(step * ROWS_STEP, ROWS_STEP)], target.at[slot], in_sems.at[kind, slot])

    def save(step, kind):
        slot = lax.rem(step, SLOTS)
        source, target = ((k_buf, k_out), (v_buf, v_out))[kind]
        return pltpu.make_async_copy(source.at[slot], target.at[pl.ds(step * ROWS_STEP, ROWS_STEP)], out_sems.at[kind, slot])

    for step in range(2):
        for kind in range(2):
            load(step, kind).start()

    q_wide[...] = jnp.zeros_like(q_wide)
    for head in range(q_heads):
        q_wide[pl.ds(head, batch, stride=QPAD), :] = q_ref[:, head * HEAD:(head + 1) * HEAD].astype(F32)
    q_packed[...] = q_wide[...].astype(BF16)
    for kind in range(2):
        for head in range(2):
            start = (kind * 2 + head) * HEAD
            kv_wide[kind, pl.ds(head, batch, stride=2), :] = kv_ref[:, start:start + HEAD].astype(F32)
    row_head = lax.broadcasted_iota(jnp.int32, (QPAD, kv_rows), 0) >= group
    col_head = lax.rem(lax.broadcasted_iota(jnp.int32, (QPAD, kv_rows), 1), 2) == 1
    parity[...] = jnp.where(row_head == col_head, 0.0, -jnp.inf)
    columns = lax.broadcasted_iota(jnp.int32, (QPAD, kv_rows), 1)
    tile_row = lax.broadcasted_iota(jnp.int32, (16, HEAD), 0)
    tile_pos = lax.div(tile_row, 2)
    tile_odd = lax.rem(tile_row, 2) == 1

    def body(step, carry):
        slot = lax.rem(step, SLOTS)

        @pl.when(step + 2 < steps)
        def _():
            @pl.when(step >= 2)
            def _():
                for kind in range(2):
                    save(step - 2, kind).wait()
            for kind in range(2):
                load(step + 2, kind).start()

        for kind in range(2):
            load(step, kind).wait()
        for row in range(ROWS_STEP):
            index = step * ROWS_STEP + row
            position = lens_ref[index]
            base = pl.multiple_of(lax.div(position, 8) * 16, 16)
            offset = lax.rem(position, 8)
            for kind, buffer in ((0, k_buf), (1, v_buf)):
                low = kv_wide[kind, pl.ds(2 * index, 1), :]
                high = kv_wide[kind, pl.ds(2 * index + 1, 1), :]
                fresh = jnp.where(tile_odd, high, low).astype(BF16)
                tile = buffer[slot, row, pl.ds(base, 16), :]
                buffer[slot, row, pl.ds(base, 16), :] = jnp.where(tile_pos == offset, fresh, tile)
        for row in range(ROWS_STEP):
            q_start = pl.multiple_of((step * ROWS_STEP + row) * QPAD, QPAD)
            scores[row] = lax.dot_general(q_packed[pl.ds(q_start, QPAD), :], k_buf[slot, row], (((1,), (1,)), ((), ())),
                                          preferred_element_type=F32)
        for kind in range(2):
            save(step, kind).start()
        for row in range(ROWS_STEP):
            limit = 2 * lens_ref[step * ROWS_STEP + row] + 2
            masked = jnp.where(columns < limit, scores[row] * HEAD ** -0.5 + parity[...], -jnp.inf)
            weight = jnp.exp(masked - jnp.max(masked, axis=1, keepdims=True))
            sums[row] = jnp.broadcast_to(jnp.sum(weight, axis=1, keepdims=True), (QPAD, HEAD))
            weights[row] = weight.astype(BF16)
        for row in range(ROWS_STEP):
            q_start = pl.multiple_of((step * ROWS_STEP + row) * QPAD, QPAD)
            mixed = jnp.dot(weights[row], v_buf[slot, row], preferred_element_type=F32)
            o_wide[pl.ds(q_start, QPAD), :] = mixed / sums[row]
        return carry

    lax.fori_loop(0, steps, body, 0)
    for head in range(q_heads):
        o_ref[:, head * HEAD:(head + 1) * HEAD] = o_wide[pl.ds(head, batch, stride=QPAD), :].astype(BF16)
    for step in range(steps - SLOTS, steps):
        for kind in range(2):
            save(step, kind).wait()


def attend(seq_lens, q_rot, kv_new, k_cache, v_cache):
    batch, seq_len, kv_heads, _ = k_cache.shape
    rows = seq_len * kv_heads
    flat = (batch, rows, HEAD)
    out, k_out, v_out = pl.pallas_call(
        attend_kernel,
        name="attend",
        out_shape=(jax.ShapeDtypeStruct(q_rot.shape, BF16), jax.ShapeDtypeStruct(flat, BF16), jax.ShapeDtypeStruct(flat, BF16)),
        in_specs=[pl.BlockSpec(memory_space=pltpu.SMEM)] + vmem_specs(2) + any_specs(2),
        out_specs=tuple(vmem_specs(1) + any_specs(2)),
        scratch_shapes=[
            VMEM((SLOTS, ROWS_STEP, rows, HEAD), BF16),
            VMEM((SLOTS, ROWS_STEP, rows, HEAD), BF16),
            VMEM((batch * QPAD, HEAD), F32),
            VMEM((batch * QPAD, HEAD), BF16),
            VMEM((2, batch * 2, HEAD), F32),
            VMEM((batch * QPAD, HEAD), F32),
            VMEM((QPAD, rows), F32),
            VMEM((ROWS_STEP, QPAD, rows), F32),
            VMEM((ROWS_STEP, QPAD, rows), BF16),
            VMEM((ROWS_STEP, QPAD, HEAD), F32),
            DMA((2, SLOTS)),
            DMA((2, SLOTS)),
        ],
        compiler_params=pltpu.CompilerParams(vmem_limit_bytes=48 << 20),
    )(seq_lens, q_rot, kv_new, k_cache.reshape(flat), v_cache.reshape(flat))
    return out, k_out.reshape(k_cache.shape), v_out.reshape(v_cache.shape)


def rotary_tables(positions):
    half_dim = HEAD // 2
    inv_freq = ROPE_THETA ** (-2.0 * jnp.arange(half_dim, dtype=F32) / HEAD)
    angles = positions.astype(F32)[:, None] * jnp.concatenate([inv_freq, inv_freq])
    sign = jnp.where(jnp.arange(HEAD) < half_dim, -1.0, 1.0)
    return jnp.cos(angles), jnp.sin(angles) * sign


def solution(mesh):
    mx_size = mesh.shape["mx"]
    act_spec = P(None, "mx")
    cache_spec = P("mx", None, "my", None)
    in_specs = (act_spec, P("mx"), P("mx"), P("mx"), P("mx", "my"), P("my"), P("mx", "my"), P("my"), P("mx", "my"), P("my"), P("my", "mx"), P("mx", "my"), P("mx", "my"), P("my", "mx"), cache_spec, cache_spec)
    out_specs = (act_spec, cache_spec, cache_spec)

    def local_layer(x_in, seq_lens, gain_attn, gain_mlp, w_q, b_q, w_k, b_k, w_v, b_v, w_o, w_gate, w_up, w_down, k_cache, v_cache):
        hidden = x_in.shape[1] * mx_size
        x_f32 = x_in.astype(F32)
        cos_tab, sin_tab = rotary_tables(seq_lens)
        bias = jnp.concatenate([b_q, b_k, b_v])[None, :]
        q_rot, kv_new = project(x_in, gain_attn[None, :], bias, cos_tab, sin_tab, w_q, w_k, w_v)
        attn_rows, k_cache_out, v_cache_out = attend(seq_lens, q_rot, kv_new, k_cache, v_cache)
        attn_all = lax.all_gather(attn_rows, "mx", axis=0, tiled=True)
        attn_proj = lax.psum(jnp.dot(attn_all, w_o, preferred_element_type=F32).astype(BF16), "my")
        x_mid = (x_f32 + attn_proj.astype(F32)).astype(BF16)
        mid_f32 = x_mid.astype(F32)
        mlp_sq = lax.psum(jnp.sum(mid_f32 * mid_f32, axis=1, keepdims=True), "mx")
        normed_mlp = (mid_f32 * lax.rsqrt(mlp_sq / hidden + NORM_EPS) * gain_mlp.astype(F32)).astype(BF16)
        ff_cols = w_gate.shape[1]
        gate_up = lax.psum(jnp.concatenate([
            jnp.dot(normed_mlp, w_gate, preferred_element_type=F32).astype(BF16),
            jnp.dot(normed_mlp, w_up, preferred_element_type=F32).astype(BF16),
        ], axis=1), "mx").astype(F32)
        hidden_act = (jax.nn.silu(gate_up[:, :ff_cols]) * gate_up[:, ff_cols:]).astype(BF16)
        down_proj = lax.psum(jnp.dot(hidden_act, w_down, preferred_element_type=F32).astype(BF16), "my")
        x_out = (mid_f32 + down_proj.astype(F32)).astype(BF16)
        return x_out, k_cache_out, v_cache_out

    return jax.shard_map(local_layer, mesh=mesh, in_specs=in_specs, out_specs=out_specs, check_vma=False)
```

```python
import jax
import jax.numpy as jnp
from jax import lax
from jax.experimental import pallas as pl
from jax.experimental.pallas import tpu as pltpu
from jax.sharding import PartitionSpec as P

HEAD = 128
NORM_EPS = 1e-6
ROPE_THETA = 1000000.0
MESH = pl.DeviceIdType.MESH
F32 = jnp.float32
BF16 = jnp.bfloat16
QPAD = 16
VMEM = pltpu.VMEM
DMA = pltpu.SemaphoreType.DMA


def any_specs(count):
    return [pl.BlockSpec(memory_space=pl.ANY)] * count


def vmem_specs(count):
    return [pl.BlockSpec(memory_space=pltpu.VMEM)] * count


def project_kernel(x_ref, gain_ref, bias_ref, cos_ref, sin_ref, wq_hbm, wk_hbm, wv_hbm, q_out, kv_out,
                   w_buf, normed, sq_send, sq_recv, part_send, part_recv, part_own, w_sems, send_sems, recv_sems):
    me = lax.axis_index("mx")
    peer = 1 - me
    rows, depth = x_ref.shape
    half = rows // 2
    width = 2 * HEAD
    q_chunks = wq_hbm.shape[1] // width
    chunks = q_chunks + 2

    def weight_copy(index):
        if index < q_chunks:
            source = wq_hbm.at[:, pl.ds(index * width, width)]
        else:
            source = (wk_hbm, wv_hbm)[index - q_chunks]
        return pltpu.make_async_copy(source, w_buf.at[index], w_sems.at[index])

    for index in range(chunks):
        weight_copy(index).start()
    barrier = pltpu.get_barrier_semaphore()
    pl.semaphore_signal(barrier, inc=1, device_id={"mx": peer}, device_id_type=MESH)

    total = jnp.zeros((rows, HEAD), F32)
    for start in range(0, depth, HEAD):
        block = x_ref[:, start:start + HEAD].astype(F32)
        total = total + block * block
    sq_own = jnp.sum(total, axis=1, keepdims=True)
    sq_send[...] = jnp.broadcast_to(sq_own, (rows, HEAD))
    pl.semaphore_wait(barrier, 1)

    def remote(source, target, slot):
        return pltpu.make_async_remote_copy(
            src_ref=source, dst_ref=target, send_sem=send_sems.at[slot], recv_sem=recv_sems.at[slot],
            device_id={"mx": peer}, device_id_type=MESH)

    sq_copy = remote(sq_send, sq_recv, chunks)
    sq_copy.start()
    sq_copy.wait()
    scale = lax.rsqrt((sq_send[...] + sq_recv[...]) / (2 * depth) + NORM_EPS)
    for start in range(0, depth, HEAD):
        block = x_ref[:, start:start + HEAD].astype(F32)
        gain = gain_ref[:, start:start + HEAD].astype(F32)
        normed[:, start:start + HEAD] = (block * scale * gain).astype(BF16)

    own_rows = pl.ds(pl.multiple_of(me * half, half), half)
    peer_rows = pl.ds(pl.multiple_of(peer * half, half), half)
    copies = []
    for index in range(chunks):
        weight_copy(index).wait()
        weights = w_buf.at[index]
        part_send[index] = jnp.dot(normed[peer_rows, :], weights[...], preferred_element_type=F32).astype(BF16)
        part_own[index] = jnp.dot(normed[own_rows, :], weights[...], preferred_element_type=F32)
        copies.append(remote(part_send.at[index], part_recv.at[index], index))
        copies[index].start()

    cos_tab = cos_ref[...]
    sin_tab = sin_ref[...]
    for index in range(chunks):
        copies[index].wait()
        for head in range(2):
            lanes = slice(head * HEAD, (head + 1) * HEAD)
            columns = slice(index * width + head * HEAD, index * width + (head + 1) * HEAD)
            value = part_own[index][:, lanes] + part_recv[index][:, lanes].astype(F32) + bias_ref[:, columns].astype(F32)
            if index < chunks - 1:
                value = value * cos_tab + pltpu.roll(value, HEAD // 2, 1) * sin_tab
            if index < q_chunks:
                q_out[:, columns] = value.astype(BF16)
            else:
                kv_out[:, (index - q_chunks) * width + head * HEAD:(index - q_chunks) * width + (head + 1) * HEAD] = value.astype(BF16)


def project(x_in, gain, bias, cos_tab, sin_tab, w_q, w_k, w_v):
    rows, depth = x_in.shape
    half = rows // 2
    width = 2 * HEAD
    chunks = w_q.shape[1] // width + 2
    return pl.pallas_call(
        project_kernel,
        name="project",
        out_shape=(jax.ShapeDtypeStruct((half, w_q.shape[1]), BF16), jax.ShapeDtypeStruct((half, 2 * width), BF16)),
        in_specs=vmem_specs(5) + any_specs(3),
        out_specs=tuple(vmem_specs(2)),
        scratch_shapes=[
            VMEM((chunks, depth, width), BF16),
            VMEM((rows, depth), BF16),
            VMEM((rows, HEAD), F32),
            VMEM((rows, HEAD), F32),
            VMEM((chunks, half, width), BF16),
            VMEM((chunks, half, width), BF16),
            VMEM((chunks, half, width), F32),
            DMA((chunks,)),
            DMA((chunks + 1,)),
            DMA((chunks + 1,)),
        ],
        compiler_params=pltpu.CompilerParams(collective_id=0, has_side_effects=True, vmem_limit_bytes=67043328),
    )(x_in, gain, bias, cos_tab, sin_tab, w_q, w_k, w_v)


SLOTS = 4
ROWS_STEP = 8


def attend_kernel(lens_ref, q_ref, kv_ref, k_hbm, v_hbm, o_ref, k_out, v_out,
                  k_buf, v_buf, q_wide, q_packed, kv_wide, o_wide, parity, scores, weights, sums, in_sems, out_sems):
    batch, kv_rows, _ = k_hbm.shape
    q_heads = q_ref.shape[1] // HEAD
    group = q_heads // 2
    steps = batch // ROWS_STEP

    def load(step, kind):
        slot = lax.rem(step, SLOTS)
        source, target = ((k_hbm, k_buf), (v_hbm, v_buf))[kind]
        return pltpu.make_async_copy(source.at[pl.ds(step * ROWS_STEP, ROWS_STEP)], target.at[slot], in_sems.at[kind, slot])

    def save(step, kind):
        slot = lax.rem(step, SLOTS)
        source, target = ((k_buf, k_out), (v_buf, v_out))[kind]
        return pltpu.make_async_copy(source.at[slot], target.at[pl.ds(step * ROWS_STEP, ROWS_STEP)], out_sems.at[kind, slot])

    for step in range(2):
        for kind in range(2):
            load(step, kind).start()

    q_wide[...] = jnp.zeros_like(q_wide)
    for head in range(q_heads):
        q_wide[pl.ds(head, batch, stride=QPAD), :] = q_ref[:, head * HEAD:(head + 1) * HEAD].astype(F32)
    q_packed[...] = q_wide[...].astype(BF16)
    for kind in range(2):
        for head in range(2):
            start = (kind * 2 + head) * HEAD
            kv_wide[kind, pl.ds(head, batch, stride=2), :] = kv_ref[:, start:start + HEAD].astype(F32)
    row_head = lax.broadcasted_iota(jnp.int32, (QPAD, kv_rows), 0) >= group
    col_head = lax.rem(lax.broadcasted_iota(jnp.int32, (QPAD, kv_rows), 1), 2) == 1
    parity[...] = jnp.where(row_head == col_head, 0.0, -jnp.inf)
    columns = lax.broadcasted_iota(jnp.int32, (QPAD, kv_rows), 1)
    tile_row = lax.broadcasted_iota(jnp.int32, (16, HEAD), 0)
    tile_pos = lax.div(tile_row, 2)
    tile_odd = lax.rem(tile_row, 2) == 1

    def body(step, carry):
        slot = lax.rem(step, SLOTS)

        @pl.when(step + 2 < steps)
        def _():
            @pl.when(step >= 2)
            def _():
                for kind in range(2):
                    save(step - 2, kind).wait()
            for kind in range(2):
                load(step + 2, kind).start()

        for kind in range(2):
            load(step, kind).wait()
        for row in range(ROWS_STEP):
            index = step * ROWS_STEP + row
            position = lens_ref[index]
            base = pl.multiple_of(lax.div(position, 8) * 16, 16)
            offset = lax.rem(position, 8)
            for kind, buffer in ((0, k_buf), (1, v_buf)):
                low = kv_wide[kind, pl.ds(2 * index, 1), :]
                high = kv_wide[kind, pl.ds(2 * index + 1, 1), :]
                fresh = jnp.where(tile_odd, high, low).astype(BF16)
                tile = buffer[slot, row, pl.ds(base, 16), :]
                buffer[slot, row, pl.ds(base, 16), :] = jnp.where(tile_pos == offset, fresh, tile)
        for row in range(ROWS_STEP):
            q_start = pl.multiple_of((step * ROWS_STEP + row) * QPAD, QPAD)
            scores[row] = lax.dot_general(q_packed[pl.ds(q_start, QPAD), :], k_buf[slot, row], (((1,), (1,)), ((), ())),
                                          preferred_element_type=F32)
        for kind in range(2):
            save(step, kind).start()
        for row in range(ROWS_STEP):
            limit = 2 * lens_ref[step * ROWS_STEP + row] + 2
            masked = jnp.where(columns < limit, scores[row] * HEAD ** -0.5 + parity[...], -jnp.inf)
            weight = jnp.exp(masked - jnp.max(masked, axis=1, keepdims=True))
            sums[row] = jnp.broadcast_to(jnp.sum(weight, axis=1, keepdims=True), (QPAD, HEAD))
            weights[row] = weight.astype(BF16)
        for row in range(ROWS_STEP):
            q_start = pl.multiple_of((step * ROWS_STEP + row) * QPAD, QPAD)
            mixed = jnp.dot(weights[row], v_buf[slot, row], preferred_element_type=F32)
            o_wide[pl.ds(q_start, QPAD), :] = mixed / sums[row]
        return carry

    lax.fori_loop(0, steps, body, 0)
    for head in range(q_heads):
        o_ref[:, head * HEAD:(head + 1) * HEAD] = o_wide[pl.ds(head, batch, stride=QPAD), :].astype(BF16)
    for step in range(steps - SLOTS, steps):
        for kind in range(2):
            save(step, kind).wait()


def attend(seq_lens, q_rot, kv_new, k_cache, v_cache):
    batch, seq_len, kv_heads, _ = k_cache.shape
    rows = seq_len * kv_heads
    flat = (batch, rows, HEAD)
    out, k_out, v_out = pl.pallas_call(
        attend_kernel,
        name="attend",
        out_shape=(jax.ShapeDtypeStruct(q_rot.shape, BF16), jax.ShapeDtypeStruct(flat, BF16), jax.ShapeDtypeStruct(flat, BF16)),
        in_specs=[pl.BlockSpec(memory_space=pltpu.SMEM)] + vmem_specs(2) + any_specs(2),
        out_specs=tuple(vmem_specs(1) + any_specs(2)),
        scratch_shapes=[
            VMEM((SLOTS, ROWS_STEP, rows, HEAD), BF16),
            VMEM((SLOTS, ROWS_STEP, rows, HEAD), BF16),
            VMEM((batch * QPAD, HEAD), F32),
            VMEM((batch * QPAD, HEAD), BF16),
            VMEM((2, batch * 2, HEAD), F32),
            VMEM((batch * QPAD, HEAD), F32),
            VMEM((QPAD, rows), F32),
            VMEM((ROWS_STEP, QPAD, rows), F32),
            VMEM((ROWS_STEP, QPAD, rows), BF16),
            VMEM((ROWS_STEP, QPAD, HEAD), F32),
            DMA((2, SLOTS)),
            DMA((2, SLOTS)),
        ],
        compiler_params=pltpu.CompilerParams(vmem_limit_bytes=64 << 20),
    )(seq_lens, q_rot, kv_new, k_cache.reshape(flat), v_cache.reshape(flat))
    return out, k_out.reshape(k_cache.shape), v_out.reshape(v_cache.shape)


BLOCK = 256
RING = 36


def tail_kernel(attn_ref, gain_ref, x_hbm, wo_hbm, wg_hbm, wu_hbm, wd_hbm, out_ref,
                pool, full, rows_in, part, keep, recv_one, send_two, recv_two, x_own, mid, sq_send, sq_recv,
                h_rows, h_cols, gu_send, gu_recv, gu_own, act, early,
                pool_sems, x_sem, core_sems, rs_sems, ag_sems, gu_sems, act_sems):
    my = lax.axis_index("my")
    me = lax.axis_index("mx")
    peer = 1 - me
    side_x = my + 1 - 2 * lax.rem(my, 2)
    side_y = lax.rem(my + 2, 4)
    cross = 3 - my
    half, depth = attn_ref.shape
    batch = 2 * half
    quarter = batch // 4
    hidden = x_hbm.shape[1]
    ff = wg_hbm.shape[0]
    col_chunks = hidden // BLOCK
    ff_chunks = pl.cdiv(ff, BLOCK)
    ff_rest = ff - (ff_chunks - 1) * BLOCK
    chunk_ring = RING // 2
    out_blocks = depth // BLOCK
    out_slot = RING - 6

    def slot_rows(slot, count=BLOCK):
        return pl.ds(pl.multiple_of(slot * BLOCK, BLOCK), count)

    def block_copy(source, block, slot, count=BLOCK):
        return pltpu.make_async_copy(source.at[slot_rows(block, count)], pool.at[slot_rows(slot, count)], pool_sems.at[slot])

    def ff_copies(chunk, count=BLOCK):
        slot = 2 * lax.rem(chunk, chunk_ring)
        return block_copy(wg_hbm, chunk, slot, count), block_copy(wu_hbm, chunk, slot + 1, count)

    def down_copy(block, count=BLOCK):
        return block_copy(wd_hbm, block, lax.rem(2 * ff_chunks + block, RING), count)

    def out_copy(block):
        return block_copy(wo_hbm, block, out_slot + block)

    def to_core(source, target, slot):
        return pltpu.make_async_remote_copy(src_ref=source, dst_ref=target, send_sem=slot[0], recv_sem=slot[1],
                                            device_id={"mx": peer}, device_id_type=MESH)

    def to_chip(source, target, chip, send_sem, recv_sem):
        return pltpu.make_async_remote_copy(src_ref=source, dst_ref=target, send_sem=send_sem, recv_sem=recv_sem,
                                            device_id={"my": chip}, device_id_type=MESH)

    for block in range(out_blocks):
        out_copy(block).start()
    own_rows = pl.ds(pl.multiple_of(my * quarter, quarter), quarter)
    x_copy = pltpu.make_async_copy(x_hbm.at[own_rows], x_own, x_sem)
    x_copy.start()
    for chunk in range(out_slot // 2):
        for copy in ff_copies(chunk):
            copy.start()

    barrier = pltpu.get_barrier_semaphore()
    pl.semaphore_signal(barrier, inc=1, device_id={"mx": peer}, device_id_type=MESH)
    pl.semaphore_signal(barrier, inc=1, device_id={"my": side_x}, device_id_type=MESH)
    pl.semaphore_signal(barrier, inc=1, device_id={"my": side_y}, device_id_type=MESH)
    pl.semaphore_wait(barrier, 3)

    own_half = pl.ds(pl.multiple_of(me * half, half), half)
    peer_half = pl.ds(pl.multiple_of(peer * half, half), half)
    attn_copy = to_core(attn_ref, full.at[own_half], (core_sems.at[0], core_sems.at[1]))
    attn_copy.start()
    full[own_half, :] = attn_ref[...]
    attn_copy.wait()
    for place, owner in enumerate((my, side_x, cross, side_y)):
        rows_in[place * quarter:(place + 1) * quarter, :] = full[pl.ds(pl.multiple_of(owner * quarter, quarter), quarter), :]

    def columns(chunk):
        return slice(chunk * BLOCK, (chunk + 1) * BLOCK)

    def first_side(chunk):
        return (side_x, side_y)[chunk % 2]

    def second_side(chunk):
        return (side_y, side_x)[chunk % 2]

    def scatter_one(stage, chunk):
        sems = rs_sems.at[stage, 0]
        return to_chip(part.at[chunk], recv_one.at[chunk], first_side(chunk), sems.at[0, chunk], sems.at[1, chunk])

    def scatter_two(stage, chunk):
        sems = rs_sems.at[stage, 1]
        return to_chip(send_two.at[chunk], recv_two.at[chunk], second_side(chunk), sems.at[0, chunk], sems.at[1, chunk])

    def scatter_start(stage, chunk, total):
        lead = quarter * (1 + chunk % 2)
        part[chunk] = total[lead:lead + 2 * quarter].astype(BF16)
        keep[chunk, 0] = total[:quarter]
        other = 3 * quarter if chunk % 2 == 0 else quarter
        keep[chunk, 1] = total[other:other + quarter]
        scatter_one(stage, chunk).start()

    def scatter_pass(stage, chunk):
        scatter_one(stage, chunk).wait()
        mine = slice(0, quarter) if chunk % 2 == 0 else slice(quarter, 2 * quarter)
        theirs = slice(quarter, 2 * quarter) if chunk % 2 == 0 else slice(0, quarter)
        send_two[chunk] = (keep[chunk, 1] + recv_one[chunk, theirs, :].astype(F32)).astype(BF16)
        scatter_two(stage, chunk).start()
        keep[chunk, 0] = keep[chunk, 0] + recv_one[chunk, mine, :].astype(F32)

    def scatter_end(stage, chunk):
        scatter_two(stage, chunk).wait()
        return keep[chunk, 0] + recv_two[chunk].astype(F32)

    def mid_end(chunk):
        mid[:, columns(chunk)] = (x_own[:, columns(chunk)].astype(F32) + scatter_end(0, chunk)).astype(BF16).astype(F32)

    x_copy.wait()
    for block in range(out_blocks):
        out_copy(block).wait()
    for chunk in range(col_chunks):
        weights = pool[out_slot * BLOCK:out_slot * BLOCK + depth, columns(chunk)]
        scatter_start(0, chunk, jnp.dot(rows_in[...], weights, preferred_element_type=F32))
        if chunk >= 3:
            scatter_pass(0, chunk - 3)
        if chunk >= 7:
            mid_end(chunk - 7)
    for chunk in range(out_slot // 2, chunk_ring):
        for copy in ff_copies(chunk):
            copy.start()
    for chunk in range(col_chunks, col_chunks + 7):
        if chunk - 3 < col_chunks:
            scatter_pass(0, chunk - 3)
        mid_end(chunk - 7)

    square = jnp.zeros((quarter, HEAD), F32)
    for start in range(0, hidden, HEAD):
        square = square + mid[:, start:start + HEAD] * mid[:, start:start + HEAD]
    sq_send[...] = jnp.broadcast_to(jnp.sum(square, axis=1, keepdims=True), (quarter, HEAD))
    sq_copy = to_core(sq_send, sq_recv, (core_sems.at[2], core_sems.at[3]))
    sq_copy.start()
    sq_copy.wait()
    scale = lax.rsqrt((sq_send[...] + sq_recv[...]) / (2 * hidden) + NORM_EPS)

    def place_rows(place):
        return slice(place * quarter, (place + 1) * quarter)

    def gather_x(chunk):
        return to_chip(h_rows.at[place_rows(0), columns(chunk)], h_rows.at[place_rows(1), columns(chunk)], side_x,
                       ag_sems.at[0, 0, 0, chunk], ag_sems.at[0, 0, 1, chunk])

    def gather_y(chunk):
        return to_chip(h_rows.at[place_rows(0), columns(chunk)], h_rows.at[place_rows(3), columns(chunk)], side_y,
                       ag_sems.at[0, 1, 0, chunk], ag_sems.at[0, 1, 1, chunk])

    def gather_cross(chunk):
        source = 1 if chunk % 2 == 0 else 3
        return to_chip(h_rows.at[place_rows(source), columns(chunk)], h_rows.at[place_rows(2), columns(chunk)], second_side(chunk),
                       ag_sems.at[0, 2, 0, chunk], ag_sems.at[0, 2, 1, chunk])

    for chunk in range(col_chunks):
        for start in range(chunk * BLOCK, (chunk + 1) * BLOCK, HEAD):
            gain = gain_ref[:, start:start + HEAD].astype(F32)
            h_rows[:quarter, start:start + HEAD] = (mid[:, start:start + HEAD] * scale * gain).astype(BF16)
        gather_x(chunk).start()
        gather_y(chunk).start()
    for chunk in range(col_chunks):
        (gather_x if chunk % 2 == 0 else gather_y)(chunk).wait_recv()
        gather_cross(chunk).start()

    for chunk in range(col_chunks):
        (gather_y if chunk % 2 == 0 else gather_x)(chunk).wait_recv()
        gather_cross(chunk).wait_recv()
        for place, source in enumerate((own_half, peer_half)):
            h_cols[columns(chunk), place * half:(place + 1) * half] = h_rows[source, columns(chunk)].astype(F32).T.astype(BF16)

    def gu_copy(chunk):
        slot = lax.rem(chunk, 4)
        return to_core(gu_send.at[slot], gu_recv.at[slot], (gu_sems.at[0, slot], gu_sems.at[1, slot]))

    def act_copy(chunk):
        lanes = pl.ds(pl.multiple_of(chunk * BLOCK, BLOCK), BLOCK)
        return to_core(act.at[own_half, lanes], act.at[own_half, lanes], (act_sems.at[0, chunk], act_sems.at[1, chunk]))

    def ff_products(chunk):
        slot = lax.rem(chunk, 4)
        base = 2 * lax.rem(chunk, chunk_ring)
        for kind in range(2):
            product = jnp.dot(pool[slot_rows(base + kind), :], h_cols[...], preferred_element_type=F32)
            gu_own[slot, kind] = product[:, :half]
            gu_send[slot, kind] = product[:, half:].astype(BF16)

    def activate(chunk):
        slot = lax.rem(chunk, 4)
        gate = gu_own[slot, 0] + gu_recv[slot, 0].astype(F32)
        up = gu_own[slot, 1] + gu_recv[slot, 1].astype(F32)
        value = gate * jax.nn.sigmoid(gate) * up
        row = chunk * BLOCK + lax.broadcasted_iota(jnp.int32, value.shape, 0)
        value = jnp.where(row < ff, value, 0.0)
        lanes = pl.ds(pl.multiple_of(chunk * BLOCK, BLOCK), BLOCK)
        act[own_half, lanes] = value.T.astype(BF16)

    def refill(chunk):
        ahead = chunk + chunk_ring
        block = 2 * (ahead - ff_chunks)

        @pl.when(ahead < ff_chunks - 1)
        def _():
            for copy in ff_copies(ahead):
                copy.start()

        @pl.when(ahead == ff_chunks - 1)
        def _():
            for copy in ff_copies(ahead, ff_rest):
                copy.start()

        @pl.when((ahead >= ff_chunks) & (block < ff_chunks - 1))
        def _():
            down_copy(block).start()
            down_copy(block + 1).start()

        @pl.when(block == ff_chunks - 1)
        def _():
            down_copy(block, ff_rest).start()

    def ff_step(chunk, carry):
        @pl.when(chunk >= 2)
        def _():
            gu_copy(chunk - 2).wait()
        for copy in ff_copies(chunk):
            copy.wait()

        @pl.when(chunk >= 2)
        def _():
            activate(chunk - 2)
            act_copy(chunk - 2).start()
        ff_products(chunk)
        gu_copy(chunk).start()
        refill(chunk)
        return carry

    lax.fori_loop(0, ff_chunks - 1, ff_step, 0)
    last = ff_chunks - 1
    gu_copy(last - 2).wait()
    for copy in ff_copies(last, ff_rest):
        copy.wait()
    activate(last - 2)
    act_copy(last - 2).start()
    ff_products(last)
    gu_copy(last).start()

    first_slot = (2 * ff_chunks) % RING
    first_count = RING - first_slot
    for block in range(first_count):
        down_copy(block).wait()
    split = first_count * BLOCK

    def down_first(chunk):
        return jnp.dot(act[:, :split], pool[first_slot * BLOCK:, columns(chunk)], preferred_element_type=F32)

    def down_second(chunk):
        return jnp.dot(act[:, split:], pool[:ff_chunks * BLOCK - split, columns(chunk)], preferred_element_type=F32)

    for chunk in range(first_count):
        act_copy(chunk).wait_recv()
    early[0] = down_first(0)
    gu_copy(last - 1).wait()
    activate(last - 1)
    act_copy(last - 1).start()
    gu_copy(last).wait()
    activate(last)
    act_copy(last).start()
    early[1] = down_first(1)
    for block in range(first_count, ff_chunks):
        down_copy(block, ff_rest if block == last else BLOCK).wait()
    for chunk in range(first_count, ff_chunks):
        act_copy(chunk).wait_recv()

    def owner_rows(owner):
        return pl.ds(pl.multiple_of(owner * quarter, quarter), quarter)

    def final_x(chunk):
        block = out_ref.at[owner_rows(my), columns(chunk)]
        return to_chip(block, block, side_x, ag_sems.at[1, 0, 0, chunk], ag_sems.at[1, 0, 1, chunk])

    def final_y(chunk):
        block = out_ref.at[owner_rows(my), columns(chunk)]
        return to_chip(block, block, side_y, ag_sems.at[1, 1, 0, chunk], ag_sems.at[1, 1, 1, chunk])

    def final_cross(chunk):
        block = out_ref.at[owner_rows(first_side(chunk)), columns(chunk)]
        return to_chip(block, block, second_side(chunk), ag_sems.at[1, 2, 0, chunk], ag_sems.at[1, 2, 1, chunk])

    def out_end(chunk):
        out_ref[owner_rows(my), columns(chunk)] = (mid[:, columns(chunk)] + scatter_end(1, chunk)).astype(BF16)
        final_x(chunk).start()
        final_y(chunk).start()

    def out_pass(chunk):
        (final_x if chunk % 2 == 0 else final_y)(chunk).wait_recv()
        final_cross(chunk).start()

    for chunk in range(col_chunks + 9):
        if chunk < col_chunks:
            total = (early[chunk] if chunk < 2 else down_first(chunk)) + down_second(chunk)
            scatter_start(1, chunk, total)
        if 0 <= chunk - 3 < col_chunks:
            scatter_pass(1, chunk - 3)
        if 0 <= chunk - 6 < col_chunks:
            out_end(chunk - 6)
        if 0 <= chunk - 9 < col_chunks:
            out_pass(chunk - 9)
    for chunk in range(col_chunks):
        (final_y if chunk % 2 == 0 else final_x)(chunk).wait_recv()
        final_cross(chunk).wait()
        final_x(chunk).wait_send()
        final_y(chunk).wait_send()
        gather_x(chunk).wait_send()
        gather_y(chunk).wait_send()
        gather_cross(chunk).wait_send()
    for chunk in range(ff_chunks):
        act_copy(chunk).wait_send()


def tail(attn_rows, gain, x_in, w_o, wg_rows, wu_rows, w_down):
    half, depth = attn_rows.shape
    rows, hidden = x_in.shape
    quarter = rows // 4
    chunks = hidden // BLOCK
    ff_chunks = pl.cdiv(w_down.shape[0], BLOCK)
    return pl.pallas_call(
        tail_kernel,
        name="tail",
        out_shape=jax.ShapeDtypeStruct((rows, hidden), BF16),
        in_specs=vmem_specs(2) + any_specs(5),
        out_specs=vmem_specs(1)[0],
        scratch_shapes=[
            VMEM((RING * BLOCK, hidden), BF16),
            VMEM((rows, depth), BF16),
            VMEM((rows, depth), BF16),
            VMEM((chunks, 2 * quarter, BLOCK), BF16),
            VMEM((chunks, 2, quarter, BLOCK), F32),
            VMEM((chunks, 2 * quarter, BLOCK), BF16),
            VMEM((chunks, quarter, BLOCK), BF16),
            VMEM((chunks, quarter, BLOCK), BF16),
            VMEM((quarter, hidden), BF16),
            VMEM((quarter, hidden), F32),
            VMEM((quarter, HEAD), F32),
            VMEM((quarter, HEAD), F32),
            VMEM((rows, hidden), BF16),
            VMEM((hidden, rows), BF16),
            VMEM((4, 2, BLOCK, half), BF16),
            VMEM((4, 2, BLOCK, half), BF16),
            VMEM((4, 2, BLOCK, half), F32),
            VMEM((rows, ff_chunks * BLOCK), BF16),
            VMEM((2, rows, BLOCK), F32),
            DMA((RING,)),
            DMA,
            DMA((4,)),
            DMA((2, 2, 2, chunks)),
            DMA((2, 3, 2, chunks)),
            DMA((2, 4)),
            DMA((2, ff_chunks)),
        ],
        compiler_params=pltpu.CompilerParams(collective_id=1, has_side_effects=True, vmem_limit_bytes=67043328),
    )(attn_rows, gain, x_in, w_o, wg_rows, wu_rows, w_down)


def rotary_tables(positions):
    half_dim = HEAD // 2
    inv_freq = ROPE_THETA ** (-2.0 * jnp.arange(half_dim, dtype=F32) / HEAD)
    angles = positions.astype(F32)[:, None] * jnp.concatenate([inv_freq, inv_freq])
    sign = jnp.where(jnp.arange(HEAD) < half_dim, -1.0, 1.0)
    return jnp.cos(angles), jnp.sin(angles) * sign


def solution(mesh):
    act_spec = P(None, "mx")
    cache_spec = P("mx", None, "my", None)
    in_specs = (act_spec, P("mx"), P("mx"), P("mx"), P("mx", "my"), P("my"), P("mx", "my"), P("my"), P("mx", "my"), P("my"), P("my", "mx"), P("mx", "my"), P("mx", "my"), P("my", "mx"), cache_spec, cache_spec)
    out_specs = (act_spec, cache_spec, cache_spec)

    def local_layer(x_in, seq_lens, gain_attn, gain_mlp, w_q, b_q, w_k, b_k, w_v, b_v, w_o, w_gate, w_up, w_down, k_cache, v_cache):
        cos_tab, sin_tab = rotary_tables(seq_lens)
        bias = jnp.concatenate([b_q, b_k, b_v])[None, :]
        q_rot, kv_new = project(x_in, gain_attn[None, :], bias, cos_tab, sin_tab, w_q, w_k, w_v)
        attn_rows, k_cache_out, v_cache_out = attend(seq_lens, q_rot, kv_new, k_cache, v_cache)
        x_out = tail(attn_rows, gain_mlp[None, :], x_in, w_o, w_gate.T, w_up.T, w_down)
        return x_out, k_cache_out, v_cache_out

    return jax.shard_map(local_layer, mesh=mesh, in_specs=in_specs, out_specs=out_specs, check_vma=False)
```

```python
import jax
import jax.numpy as jnp
import numpy as np
from jax import lax
from jax.experimental import pallas as pl
from jax.experimental.pallas import tpu as pltpu
from jax.sharding import PartitionSpec as P

HEAD = 128
NORM_EPS = 1e-6
ROPE_THETA = 1000000.0
MESH = pl.DeviceIdType.MESH
F32 = jnp.float32
BF16 = jnp.bfloat16
QPAD = 16
VMEM = pltpu.VMEM
DMA = pltpu.SemaphoreType.DMA


def any_specs(count):
    return [pl.BlockSpec(memory_space=pl.ANY)] * count


def vmem_specs(count):
    return [pl.BlockSpec(memory_space=pltpu.VMEM)] * count


def lane_rows(vector):
    return vector.reshape(-1, HEAD)


def rotary_frequencies():
    half_dim = HEAD // 2
    inv_freq = np.float32(ROPE_THETA) ** (np.float32(-2.0) * np.arange(half_dim, dtype=np.float32) / np.float32(HEAD))
    return jnp.asarray(np.concatenate([inv_freq, inv_freq])[None, :], F32)


def project_kernel(gain_ref, bq_ref, bk_ref, bv_ref, lens_ref, freq_ref, x_hbm, wq_hbm, wk_hbm, wv_hbm, q_out, kv_out,
                   x_ref, x_sem, w_buf, normed, sq_send, sq_recv, part_send, part_recv, part_own, w_sems, send_sems, recv_sems):
    me = lax.axis_index("mx")
    peer = 1 - me
    rows, depth = x_ref.shape
    half = rows // 2
    width = 2 * HEAD
    q_chunks = wq_hbm.shape[1] // width
    chunks = q_chunks + 2

    def weight_copy(index):
        if index < q_chunks:
            source = wq_hbm.at[:, pl.ds(index * width, width)]
        else:
            source = (wk_hbm, wv_hbm)[index - q_chunks]
        return pltpu.make_async_copy(source, w_buf.at[index], w_sems.at[index])

    x_copy = pltpu.make_async_copy(x_hbm, x_ref, x_sem)
    x_copy.start()
    for index in range(chunks):
        weight_copy(index).start()
    barrier = pltpu.get_barrier_semaphore()
    pl.semaphore_signal(barrier, inc=1, device_id={"mx": peer}, device_id_type=MESH)

    positions = jnp.broadcast_to(lens_ref[...].astype(F32), (half, half)).T
    angles = positions * freq_ref[...]
    cos_tab = jnp.cos(angles)
    lane = lax.broadcasted_iota(jnp.int32, (half, HEAD), 1)
    sin_tab = jnp.where(lane < HEAD // 2, -1.0, 1.0) * jnp.sin(angles)

    x_copy.wait()
    total = jnp.zeros((rows, HEAD), F32)
    for start in range(0, depth, HEAD):
        block = x_ref[:, start:start + HEAD].astype(F32)
        total = total + block * block
    sq_own = jnp.sum(total, axis=1, keepdims=True)
    sq_send[...] = jnp.broadcast_to(sq_own, (rows, HEAD))
    pl.semaphore_wait(barrier, 1)

    def remote(source, target, slot):
        return pltpu.make_async_remote_copy(
            src_ref=source, dst_ref=target, send_sem=send_sems.at[slot], recv_sem=recv_sems.at[slot],
            device_id={"mx": peer}, device_id_type=MESH)

    sq_copy = remote(sq_send, sq_recv, chunks)
    sq_copy.start()
    sq_copy.wait()
    scale = lax.rsqrt((sq_send[...] + sq_recv[...]) / (2 * depth) + NORM_EPS)
    gains = gain_ref[...].astype(F32)
    for start in range(0, depth, HEAD):
        block = x_ref[:, start:start + HEAD].astype(F32)
        gain = gains[start // HEAD:start // HEAD + 1, :]
        normed[:, start:start + HEAD] = (block * scale * gain).astype(BF16)

    own_rows = pl.ds(pl.multiple_of(me * half, half), half)
    peer_rows = pl.ds(pl.multiple_of(peer * half, half), half)
    copies = []
    for index in range(chunks):
        weight_copy(index).wait()
        weights = w_buf.at[index]
        part_send[index] = jnp.dot(normed[peer_rows, :], weights[...], preferred_element_type=F32).astype(BF16)
        part_own[index] = jnp.dot(normed[own_rows, :], weights[...], preferred_element_type=F32)
        copies.append(remote(part_send.at[index], part_recv.at[index], index))
        copies[index].start()

    biases = [ref[...].astype(F32) for ref in (bq_ref, bk_ref, bv_ref)]
    for index in range(chunks):
        copies[index].wait()
        for head in range(2):
            lanes = slice(head * HEAD, (head + 1) * HEAD)
            columns = slice(index * width + head * HEAD, index * width + (head + 1) * HEAD)
            if index < q_chunks:
                bias = biases[0][2 * index + head:2 * index + head + 1, :]
            else:
                bias = biases[index - q_chunks + 1][head:head + 1, :]
            value = part_own[index][:, lanes] + part_recv[index][:, lanes].astype(F32) + bias
            if index < chunks - 1:
                value = value * cos_tab + pltpu.roll(value, HEAD // 2, 1) * sin_tab
            if index < q_chunks:
                q_out[:, columns] = value.astype(BF16)
            else:
                kv_out[:, (index - q_chunks) * width + head * HEAD:(index - q_chunks) * width + (head + 1) * HEAD] = value.astype(BF16)


def project(x_in, seq_lens, gain, b_q, b_k, b_v, w_q, w_k, w_v):
    rows, depth = x_in.shape
    half = rows // 2
    width = 2 * HEAD
    chunks = w_q.shape[1] // width + 2
    return pl.pallas_call(
        project_kernel,
        name="project",
        out_shape=(jax.ShapeDtypeStruct((half, w_q.shape[1]), BF16), jax.ShapeDtypeStruct((half, 2 * width), BF16)),
        in_specs=vmem_specs(6) + any_specs(4),
        out_specs=tuple(vmem_specs(2)),
        scratch_shapes=[
            VMEM((rows, depth), BF16),
            DMA,
            VMEM((chunks, depth, width), BF16),
            VMEM((rows, depth), BF16),
            VMEM((rows, HEAD), F32),
            VMEM((rows, HEAD), F32),
            VMEM((chunks, half, width), BF16),
            VMEM((chunks, half, width), BF16),
            VMEM((chunks, half, width), F32),
            DMA((chunks,)),
            DMA((chunks + 1,)),
            DMA((chunks + 1,)),
        ],
        compiler_params=pltpu.CompilerParams(collective_id=0, has_side_effects=True, vmem_limit_bytes=67043328),
    )(lane_rows(gain), lane_rows(b_q), lane_rows(b_k), lane_rows(b_v), seq_lens[None, :], rotary_frequencies(), x_in, w_q, w_k, w_v)


SLOTS = 4
ROWS_STEP = 8


def attend_kernel(lens_ref, q_ref, kv_ref, k_hbm, v_hbm, o_ref, k_out, v_out,
                  k_buf, v_buf, q_wide, q_packed, kv_wide, o_wide, parity, scores, weights, sums, in_sems, out_sems):
    batch, kv_rows, _ = k_hbm.shape
    q_heads = q_ref.shape[1] // HEAD
    group = q_heads // 2
    steps = batch // ROWS_STEP

    def load(step, kind):
        slot = lax.rem(step, SLOTS)
        source, target = ((k_hbm, k_buf), (v_hbm, v_buf))[kind]
        return pltpu.make_async_copy(source.at[pl.ds(step * ROWS_STEP, ROWS_STEP)], target.at[slot], in_sems.at[kind, slot])

    def save(step, kind):
        slot = lax.rem(step, SLOTS)
        source, target = ((k_buf, k_out), (v_buf, v_out))[kind]
        return pltpu.make_async_copy(source.at[slot], target.at[pl.ds(step * ROWS_STEP, ROWS_STEP)], out_sems.at[kind, slot])

    for step in range(2):
        for kind in range(2):
            load(step, kind).start()

    q_wide[...] = jnp.zeros_like(q_wide)
    for head in range(q_heads):
        q_wide[pl.ds(head, batch, stride=QPAD), :] = q_ref[:, head * HEAD:(head + 1) * HEAD].astype(F32)
    q_packed[...] = q_wide[...].astype(BF16)
    for kind in range(2):
        for head in range(2):
            start = (kind * 2 + head) * HEAD
            kv_wide[kind, pl.ds(head, batch, stride=2), :] = kv_ref[:, start:start + HEAD].astype(F32)
    row_head = lax.broadcasted_iota(jnp.int32, (QPAD, kv_rows), 0) >= group
    col_head = lax.rem(lax.broadcasted_iota(jnp.int32, (QPAD, kv_rows), 1), 2) == 1
    parity[...] = jnp.where(row_head == col_head, 0.0, -jnp.inf)
    columns = lax.broadcasted_iota(jnp.int32, (QPAD, kv_rows), 1)
    tile_row = lax.broadcasted_iota(jnp.int32, (16, HEAD), 0)
    tile_pos = lax.div(tile_row, 2)
    tile_odd = lax.rem(tile_row, 2) == 1

    def body(step, carry):
        slot = lax.rem(step, SLOTS)

        @pl.when(step + 2 < steps)
        def _():
            @pl.when(step >= 2)
            def _():
                for kind in range(2):
                    save(step - 2, kind).wait()
            for kind in range(2):
                load(step + 2, kind).start()

        for kind in range(2):
            load(step, kind).wait()
        for row in range(ROWS_STEP):
            index = step * ROWS_STEP + row
            position = lens_ref[index]
            base = pl.multiple_of(lax.div(position, 8) * 16, 16)
            offset = lax.rem(position, 8)
            for kind, buffer in ((0, k_buf), (1, v_buf)):
                low = kv_wide[kind, pl.ds(2 * index, 1), :]
                high = kv_wide[kind, pl.ds(2 * index + 1, 1), :]
                fresh = jnp.where(tile_odd, high, low).astype(BF16)
                tile = buffer[slot, row, pl.ds(base, 16), :]
                buffer[slot, row, pl.ds(base, 16), :] = jnp.where(tile_pos == offset, fresh, tile)
        for row in range(ROWS_STEP):
            q_start = pl.multiple_of((step * ROWS_STEP + row) * QPAD, QPAD)
            scores[row] = lax.dot_general(q_packed[pl.ds(q_start, QPAD), :], k_buf[slot, row], (((1,), (1,)), ((), ())),
                                          preferred_element_type=F32)
        for kind in range(2):
            save(step, kind).start()
        for row in range(ROWS_STEP):
            limit = 2 * lens_ref[step * ROWS_STEP + row] + 2
            masked = jnp.where(columns < limit, scores[row] * HEAD ** -0.5 + parity[...], -jnp.inf)
            weight = jnp.exp(masked - jnp.max(masked, axis=1, keepdims=True))
            sums[row] = jnp.broadcast_to(jnp.sum(weight, axis=1, keepdims=True), (QPAD, HEAD))
            weights[row] = weight.astype(BF16)
        for row in range(ROWS_STEP):
            q_start = pl.multiple_of((step * ROWS_STEP + row) * QPAD, QPAD)
            mixed = jnp.dot(weights[row], v_buf[slot, row], preferred_element_type=F32)
            o_wide[pl.ds(q_start, QPAD), :] = mixed / sums[row]
        return carry

    lax.fori_loop(0, steps, body, 0)
    for head in range(q_heads):
        o_ref[:, head * HEAD:(head + 1) * HEAD] = o_wide[pl.ds(head, batch, stride=QPAD), :].astype(BF16)
    for step in range(steps - SLOTS, steps):
        for kind in range(2):
            save(step, kind).wait()


def attend(seq_lens, q_rot, kv_new, k_cache, v_cache):
    batch, seq_len, kv_heads, _ = k_cache.shape
    rows = seq_len * kv_heads
    flat = (batch, rows, HEAD)
    out, k_out, v_out = pl.pallas_call(
        attend_kernel,
        name="attend",
        out_shape=(jax.ShapeDtypeStruct(q_rot.shape, BF16), jax.ShapeDtypeStruct(flat, BF16), jax.ShapeDtypeStruct(flat, BF16)),
        in_specs=[pl.BlockSpec(memory_space=pltpu.SMEM)] + vmem_specs(2) + any_specs(2),
        out_specs=tuple(vmem_specs(1) + any_specs(2)),
        scratch_shapes=[
            VMEM((SLOTS, ROWS_STEP, rows, HEAD), BF16),
            VMEM((SLOTS, ROWS_STEP, rows, HEAD), BF16),
            VMEM((batch * QPAD, HEAD), F32),
            VMEM((batch * QPAD, HEAD), BF16),
            VMEM((2, batch * 2, HEAD), F32),
            VMEM((batch * QPAD, HEAD), F32),
            VMEM((QPAD, rows), F32),
            VMEM((ROWS_STEP, QPAD, rows), F32),
            VMEM((ROWS_STEP, QPAD, rows), BF16),
            VMEM((ROWS_STEP, QPAD, HEAD), F32),
            DMA((2, SLOTS)),
            DMA((2, SLOTS)),
        ],
        compiler_params=pltpu.CompilerParams(vmem_limit_bytes=64 << 20),
    )(seq_lens, q_rot, kv_new, k_cache.reshape(flat), v_cache.reshape(flat))
    return out, k_out.reshape(k_cache.shape), v_out.reshape(v_cache.shape)


BLOCK = 256
RING = 36


def tail_kernel(gain_ref, attn_hbm, x_hbm, wo_hbm, wg_hbm, wu_hbm, wd_hbm, out_hbm,
                out_ref, out_sems, pool, full, rows_in, part, keep, recv_one, send_two, recv_two, x_own, mid, sq_send, sq_recv,
                h_rows, h_cols, gu_send, gu_recv, gu_own, act, early,
                pool_sems, x_sem, attn_sem, core_sems, rs_sems, ag_sems, gu_sems, act_sems):
    my = lax.axis_index("my")
    me = lax.axis_index("mx")
    peer = 1 - me
    side_x = my + 1 - 2 * lax.rem(my, 2)
    side_y = lax.rem(my + 2, 4)
    cross = 3 - my
    half, depth = attn_hbm.shape
    batch = 2 * half
    quarter = batch // 4
    hidden = x_hbm.shape[1]
    ff = wg_hbm.shape[0]
    col_chunks = hidden // BLOCK
    ff_chunks = pl.cdiv(ff, BLOCK)
    ff_rest = ff - (ff_chunks - 1) * BLOCK
    chunk_ring = RING // 2
    out_blocks = depth // BLOCK
    out_slot = RING - 6

    def slot_rows(slot, count=BLOCK):
        return pl.ds(pl.multiple_of(slot * BLOCK, BLOCK), count)

    def block_copy(source, block, slot, count=BLOCK):
        return pltpu.make_async_copy(source.at[slot_rows(block, count)], pool.at[slot_rows(slot, count)], pool_sems.at[slot])

    def ff_copies(chunk, count=BLOCK):
        slot = 2 * lax.rem(chunk, chunk_ring)
        return block_copy(wg_hbm, chunk, slot, count), block_copy(wu_hbm, chunk, slot + 1, count)

    def down_copy(block, count=BLOCK):
        return block_copy(wd_hbm, block, lax.rem(2 * ff_chunks + block, RING), count)

    def out_copy(block):
        return block_copy(wo_hbm, block, out_slot + block)

    def to_core(source, target, slot):
        return pltpu.make_async_remote_copy(src_ref=source, dst_ref=target, send_sem=slot[0], recv_sem=slot[1],
                                            device_id={"mx": peer}, device_id_type=MESH)

    def to_chip(source, target, chip, send_sem, recv_sem):
        return pltpu.make_async_remote_copy(src_ref=source, dst_ref=target, send_sem=send_sem, recv_sem=recv_sem,
                                            device_id={"my": chip}, device_id_type=MESH)

    own_half = pl.ds(pl.multiple_of(me * half, half), half)
    peer_half = pl.ds(pl.multiple_of(peer * half, half), half)
    attn_load = pltpu.make_async_copy(attn_hbm, full.at[own_half], attn_sem)
    attn_load.start()
    for block in range(out_blocks):
        out_copy(block).start()
    own_rows = pl.ds(pl.multiple_of(my * quarter, quarter), quarter)
    x_copy = pltpu.make_async_copy(x_hbm.at[own_rows], x_own, x_sem)
    x_copy.start()

    barrier = pltpu.get_barrier_semaphore()
    pl.semaphore_signal(barrier, inc=1, device_id={"mx": peer}, device_id_type=MESH)
    pl.semaphore_signal(barrier, inc=1, device_id={"my": side_x}, device_id_type=MESH)
    pl.semaphore_signal(barrier, inc=1, device_id={"my": side_y}, device_id_type=MESH)
    pl.semaphore_wait(barrier, 3)

    attn_load.wait()
    attn_copy = to_core(full.at[own_half], full.at[own_half], (core_sems.at[0], core_sems.at[1]))
    attn_copy.start()
    attn_copy.wait()
    for place, owner in enumerate((my, side_x, cross, side_y)):
        rows_in[place * quarter:(place + 1) * quarter, :] = full[pl.ds(pl.multiple_of(owner * quarter, quarter), quarter), :]

    def columns(chunk):
        return slice(chunk * BLOCK, (chunk + 1) * BLOCK)

    def first_side(chunk):
        return (side_x, side_y)[chunk % 2]

    def second_side(chunk):
        return (side_y, side_x)[chunk % 2]

    def scatter_one(stage, chunk):
        sems = rs_sems.at[stage, 0]
        return to_chip(part.at[chunk], recv_one.at[chunk], first_side(chunk), sems.at[0, chunk], sems.at[1, chunk])

    def scatter_two(stage, chunk):
        sems = rs_sems.at[stage, 1]
        return to_chip(send_two.at[chunk], recv_two.at[chunk], second_side(chunk), sems.at[0, chunk], sems.at[1, chunk])

    def scatter_start(stage, chunk, total):
        lead = quarter * (1 + chunk % 2)
        part[chunk] = total[lead:lead + 2 * quarter].astype(BF16)
        keep[chunk, 0] = total[:quarter]
        other = 3 * quarter if chunk % 2 == 0 else quarter
        keep[chunk, 1] = total[other:other + quarter]
        scatter_one(stage, chunk).start()

    def scatter_pass(stage, chunk):
        scatter_one(stage, chunk).wait()
        mine = slice(0, quarter) if chunk % 2 == 0 else slice(quarter, 2 * quarter)
        theirs = slice(quarter, 2 * quarter) if chunk % 2 == 0 else slice(0, quarter)
        send_two[chunk] = (keep[chunk, 1] + recv_one[chunk, theirs, :].astype(F32)).astype(BF16)
        scatter_two(stage, chunk).start()
        keep[chunk, 0] = keep[chunk, 0] + recv_one[chunk, mine, :].astype(F32)

    def scatter_end(stage, chunk):
        scatter_two(stage, chunk).wait()
        return keep[chunk, 0] + recv_two[chunk].astype(F32)

    def mid_end(chunk):
        mid[:, columns(chunk)] = (x_own[:, columns(chunk)].astype(F32) + scatter_end(0, chunk)).astype(BF16).astype(F32)

    x_copy.wait()
    for block in range(out_blocks):
        out_copy(block).wait()
    for chunk in range(out_slot // 2):
        for copy in ff_copies(chunk):
            copy.start()
    for chunk in range(col_chunks):
        weights = pool[out_slot * BLOCK:out_slot * BLOCK + depth, columns(chunk)]
        scatter_start(0, chunk, jnp.dot(rows_in[...], weights, preferred_element_type=F32))
        if chunk >= 3:
            scatter_pass(0, chunk - 3)
        if chunk >= 7:
            mid_end(chunk - 7)
    for chunk in range(out_slot // 2, chunk_ring):
        for copy in ff_copies(chunk):
            copy.start()
    for chunk in range(col_chunks, col_chunks + 7):
        if chunk - 3 < col_chunks:
            scatter_pass(0, chunk - 3)
        mid_end(chunk - 7)

    square = jnp.zeros((quarter, HEAD), F32)
    for start in range(0, hidden, HEAD):
        square = square + mid[:, start:start + HEAD] * mid[:, start:start + HEAD]
    sq_send[...] = jnp.broadcast_to(jnp.sum(square, axis=1, keepdims=True), (quarter, HEAD))
    sq_copy = to_core(sq_send, sq_recv, (core_sems.at[2], core_sems.at[3]))
    sq_copy.start()
    sq_copy.wait()
    scale = lax.rsqrt((sq_send[...] + sq_recv[...]) / (2 * hidden) + NORM_EPS)

    def place_rows(place):
        return slice(place * quarter, (place + 1) * quarter)

    def gather_x(chunk):
        return to_chip(h_rows.at[place_rows(0), columns(chunk)], h_rows.at[place_rows(1), columns(chunk)], side_x,
                       ag_sems.at[0, 0, 0, chunk], ag_sems.at[0, 0, 1, chunk])

    def gather_y(chunk):
        return to_chip(h_rows.at[place_rows(0), columns(chunk)], h_rows.at[place_rows(3), columns(chunk)], side_y,
                       ag_sems.at[0, 1, 0, chunk], ag_sems.at[0, 1, 1, chunk])

    def gather_cross(chunk):
        source = 1 if chunk % 2 == 0 else 3
        return to_chip(h_rows.at[place_rows(source), columns(chunk)], h_rows.at[place_rows(2), columns(chunk)], second_side(chunk),
                       ag_sems.at[0, 2, 0, chunk], ag_sems.at[0, 2, 1, chunk])

    gains = gain_ref[...].astype(F32)
    for chunk in range(col_chunks):
        for start in range(chunk * BLOCK, (chunk + 1) * BLOCK, HEAD):
            gain = gains[start // HEAD:start // HEAD + 1, :]
            h_rows[:quarter, start:start + HEAD] = (mid[:, start:start + HEAD] * scale * gain).astype(BF16)
        gather_x(chunk).start()
        gather_y(chunk).start()
    for chunk in range(col_chunks):
        (gather_x if chunk % 2 == 0 else gather_y)(chunk).wait_recv()
        gather_cross(chunk).start()

    for chunk in range(col_chunks):
        (gather_y if chunk % 2 == 0 else gather_x)(chunk).wait_recv()
        gather_cross(chunk).wait_recv()
        for place, source in enumerate((own_half, peer_half)):
            h_cols[columns(chunk), place * half:(place + 1) * half] = h_rows[source, columns(chunk)].astype(F32).T.astype(BF16)

    def gu_copy(chunk):
        slot = lax.rem(chunk, 4)
        return to_core(gu_send.at[slot], gu_recv.at[slot], (gu_sems.at[0, slot], gu_sems.at[1, slot]))

    def act_copy(chunk):
        lanes = pl.ds(pl.multiple_of(chunk * BLOCK, BLOCK), BLOCK)
        return to_core(act.at[own_half, lanes], act.at[own_half, lanes], (act_sems.at[0, chunk], act_sems.at[1, chunk]))

    def ff_products(chunk):
        slot = lax.rem(chunk, 4)
        base = 2 * lax.rem(chunk, chunk_ring)
        product = jnp.dot(pool[slot_rows(base, 2 * BLOCK), :], h_cols[...], preferred_element_type=F32)
        for kind in range(2):
            rows = slice(kind * BLOCK, (kind + 1) * BLOCK)
            gu_own[slot, kind] = product[rows, :half]
            gu_send[slot, kind] = product[rows, half:].astype(BF16)

    def activate(chunk):
        slot = lax.rem(chunk, 4)
        gate = gu_own[slot, 0] + gu_recv[slot, 0].astype(F32)
        up = gu_own[slot, 1] + gu_recv[slot, 1].astype(F32)
        value = gate * jax.nn.sigmoid(gate) * up
        row = chunk * BLOCK + lax.broadcasted_iota(jnp.int32, value.shape, 0)
        value = jnp.where(row < ff, value, 0.0)
        lanes = pl.ds(pl.multiple_of(chunk * BLOCK, BLOCK), BLOCK)
        act[own_half, lanes] = value.T.astype(BF16)

    def refill(chunk):
        ahead = chunk + chunk_ring
        block = 2 * (ahead - ff_chunks)

        @pl.when(ahead < ff_chunks - 1)
        def _():
            for copy in ff_copies(ahead):
                copy.start()

        @pl.when(ahead == ff_chunks - 1)
        def _():
            for copy in ff_copies(ahead, ff_rest):
                copy.start()

        @pl.when((ahead >= ff_chunks) & (block < ff_chunks - 1))
        def _():
            down_copy(block).start()
            down_copy(block + 1).start()

        @pl.when(block == ff_chunks - 1)
        def _():
            down_copy(block, ff_rest).start()

    def ff_step(chunk, carry):
        gu_copy(chunk - 2).wait()
        for copy in ff_copies(chunk):
            copy.wait()
        activate(chunk - 2)
        ff_products(chunk)
        gu_copy(chunk).start()
        act_copy(chunk - 2).start()
        refill(chunk)
        return carry

    for chunk in range(2):
        for copy in ff_copies(chunk):
            copy.wait()
        ff_products(chunk)
        gu_copy(chunk).start()
        refill(chunk)
    lax.fori_loop(2, ff_chunks - 1, ff_step, 0)
    last = ff_chunks - 1
    gu_copy(last - 2).wait()
    for copy in ff_copies(last, ff_rest):
        copy.wait()
    activate(last - 2)
    act_copy(last - 2).start()
    ff_products(last)
    gu_copy(last).start()

    first_slot = (2 * ff_chunks) % RING
    first_count = RING - first_slot
    for block in range(first_count):
        down_copy(block).wait()
    split = first_count * BLOCK

    def down_first(chunk):
        return jnp.dot(act[:, :split], pool[first_slot * BLOCK:, columns(chunk)], preferred_element_type=F32)

    def down_second(chunk):
        return jnp.dot(act[:, split:], pool[:ff_chunks * BLOCK - split, columns(chunk)], preferred_element_type=F32)

    for chunk in range(first_count):
        act_copy(chunk).wait_recv()
    early[0] = down_first(0)
    gu_copy(last - 1).wait()
    activate(last - 1)
    act_copy(last - 1).start()
    gu_copy(last).wait()
    activate(last)
    act_copy(last).start()
    early[1] = down_first(1)
    for block in range(first_count, ff_chunks):
        down_copy(block, ff_rest if block == last else BLOCK).wait()
    for chunk in range(first_count, ff_chunks):
        act_copy(chunk).wait_recv()

    def owner_rows(owner):
        return pl.ds(pl.multiple_of(owner * quarter, quarter), quarter)

    def final_x(chunk):
        block = out_ref.at[owner_rows(my), columns(chunk)]
        return to_chip(block, block, side_x, ag_sems.at[1, 0, 0, chunk], ag_sems.at[1, 0, 1, chunk])

    def final_y(chunk):
        block = out_ref.at[owner_rows(my), columns(chunk)]
        return to_chip(block, block, side_y, ag_sems.at[1, 1, 0, chunk], ag_sems.at[1, 1, 1, chunk])

    def final_cross(chunk):
        block = out_ref.at[owner_rows(first_side(chunk)), columns(chunk)]
        return to_chip(block, block, second_side(chunk), ag_sems.at[1, 2, 0, chunk], ag_sems.at[1, 2, 1, chunk])

    def save_out(chunk):
        return pltpu.make_async_copy(out_ref.at[:, columns(chunk)], out_hbm.at[:, columns(chunk)], out_sems.at[chunk])

    def out_end(chunk):
        out_ref[owner_rows(my), columns(chunk)] = (mid[:, columns(chunk)] + scatter_end(1, chunk)).astype(BF16)
        final_x(chunk).start()
        final_y(chunk).start()

    def out_pass(chunk):
        (final_x if chunk % 2 == 0 else final_y)(chunk).wait_recv()
        final_cross(chunk).start()

    for chunk in range(col_chunks + 9):
        if chunk < col_chunks:
            total = (early[chunk] if chunk < 2 else down_first(chunk)) + down_second(chunk)
            scatter_start(1, chunk, total)
        if 0 <= chunk - 3 < col_chunks:
            scatter_pass(1, chunk - 3)
        if 0 <= chunk - 6 < col_chunks:
            out_end(chunk - 6)
        if 0 <= chunk - 9 < col_chunks:
            out_pass(chunk - 9)
    for chunk in range(col_chunks):
        (final_y if chunk % 2 == 0 else final_x)(chunk).wait_recv()
        final_cross(chunk).wait_recv()
        save_out(chunk).start()
    for chunk in range(col_chunks):
        final_cross(chunk).wait_send()
        final_x(chunk).wait_send()
        final_y(chunk).wait_send()
        gather_x(chunk).wait_send()
        gather_y(chunk).wait_send()
        gather_cross(chunk).wait_send()
        save_out(chunk).wait()
    for chunk in range(ff_chunks):
        act_copy(chunk).wait_send()


def tail(attn_rows, gain, x_in, w_o, wg_rows, wu_rows, w_down):
    half, depth = attn_rows.shape
    rows, hidden = x_in.shape
    quarter = rows // 4
    chunks = hidden // BLOCK
    ff_chunks = pl.cdiv(w_down.shape[0], BLOCK)
    return pl.pallas_call(
        tail_kernel,
        name="tail",
        out_shape=jax.ShapeDtypeStruct((rows, hidden), BF16),
        in_specs=vmem_specs(1) + any_specs(6),
        out_specs=any_specs(1)[0],
        scratch_shapes=[
            VMEM((rows, hidden), BF16),
            DMA((chunks,)),
            VMEM((RING * BLOCK, hidden), BF16),
            VMEM((rows, depth), BF16),
            VMEM((rows, depth), BF16),
            VMEM((chunks, 2 * quarter, BLOCK), BF16),
            VMEM((chunks, 2, quarter, BLOCK), F32),
            VMEM((chunks, 2 * quarter, BLOCK), BF16),
            VMEM((chunks, quarter, BLOCK), BF16),
            VMEM((chunks, quarter, BLOCK), BF16),
            VMEM((quarter, hidden), BF16),
            VMEM((quarter, hidden), F32),
            VMEM((quarter, HEAD), F32),
            VMEM((quarter, HEAD), F32),
            VMEM((rows, hidden), BF16),
            VMEM((hidden, rows), BF16),
            VMEM((4, 2, BLOCK, half), BF16),
            VMEM((4, 2, BLOCK, half), BF16),
            VMEM((4, 2, BLOCK, half), F32),
            VMEM((rows, ff_chunks * BLOCK), BF16),
            VMEM((2, rows, BLOCK), F32),
            DMA((RING,)),
            DMA,
            DMA,
            DMA((4,)),
            DMA((2, 2, 2, chunks)),
            DMA((2, 3, 2, chunks)),
            DMA((2, 4)),
            DMA((2, ff_chunks)),
        ],
        compiler_params=pltpu.CompilerParams(collective_id=1, has_side_effects=True, vmem_limit_bytes=67043328),
    )(lane_rows(gain), attn_rows, x_in, w_o, wg_rows, wu_rows, w_down)


def solution(mesh):
    act_spec = P(None, "mx")
    cache_spec = P("mx", None, "my", None)
    in_specs = (act_spec, P("mx"), P("mx"), P("mx"), P("mx", "my"), P("my"), P("mx", "my"), P("my"), P("mx", "my"), P("my"), P("my", "mx"), P("mx", "my"), P("mx", "my"), P("my", "mx"), cache_spec, cache_spec)
    out_specs = (act_spec, cache_spec, cache_spec)

    def local_layer(x_in, seq_lens, gain_attn, gain_mlp, w_q, b_q, w_k, b_k, w_v, b_v, w_o, w_gate, w_up, w_down, k_cache, v_cache):
        q_rot, kv_new = project(x_in, seq_lens, gain_attn, b_q, b_k, b_v, w_q, w_k, w_v)
        attn_rows, k_cache_out, v_cache_out = attend(seq_lens, q_rot, kv_new, k_cache, v_cache)
        x_out = tail(attn_rows, gain_mlp, x_in, w_o, w_gate.T, w_up.T, w_down)
        return x_out, k_cache_out, v_cache_out

    return jax.shard_map(local_layer, mesh=mesh, in_specs=in_specs, out_specs=out_specs, check_vma=False)
```

```python
import jax
import jax.numpy as jnp
import numpy as np
from jax import lax
from jax.experimental import pallas as pl
from jax.experimental.pallas import tpu as pltpu
from jax.sharding import PartitionSpec as P

HEAD = 128
NORM_EPS = 1e-6
ROPE_THETA = 1000000.0
MESH = pl.DeviceIdType.MESH
F32 = jnp.float32
BF16 = jnp.bfloat16
QPAD = 16
VMEM = pltpu.VMEM
DMA = pltpu.SemaphoreType.DMA


def any_specs(count):
    return [pl.BlockSpec(memory_space=pl.ANY)] * count


def vmem_specs(count):
    return [pl.BlockSpec(memory_space=pltpu.VMEM)] * count


def lane_rows(vector):
    return vector.reshape(-1, HEAD)


def rotary_frequencies():
    half_dim = HEAD // 2
    inv_freq = np.float32(ROPE_THETA) ** (np.float32(-2.0) * np.arange(half_dim, dtype=np.float32) / np.float32(HEAD))
    return jnp.asarray(np.concatenate([inv_freq, inv_freq])[None, :], F32)


def project_kernel(gain_ref, bq_ref, bk_ref, bv_ref, lens_ref, freq_ref, x_hbm, wq_hbm, wk_hbm, wv_hbm, q_out, kv_out,
                   x_ref, x_sem, w_buf, normed, sq_send, sq_recv, part_send, part_recv, part_own, w_sems, send_sems, recv_sems):
    me = lax.axis_index("mx")
    peer = 1 - me
    rows, depth = x_ref.shape
    half = rows // 2
    width = 2 * HEAD
    q_chunks = wq_hbm.shape[1] // width
    chunks = q_chunks + 2

    def weight_copy(index):
        if index < q_chunks:
            source = wq_hbm.at[:, pl.ds(index * width, width)]
        else:
            source = (wk_hbm, wv_hbm)[index - q_chunks]
        return pltpu.make_async_copy(source, w_buf.at[index], w_sems.at[index])

    def weight_wait(index):
        pltpu.make_async_copy(wk_hbm, w_buf.at[index], w_sems.at[index]).wait()

    x_copy = pltpu.make_async_copy(x_hbm, x_ref, x_sem)
    x_copy.start()
    barrier = pltpu.get_barrier_semaphore()
    pl.semaphore_signal(barrier, inc=1, device_id={"mx": peer}, device_id_type=MESH)

    positions = jnp.broadcast_to(lens_ref[...].astype(F32), (half, half)).T
    angles = positions * freq_ref[...]
    cos_tab = jnp.cos(angles)
    lane = lax.broadcasted_iota(jnp.int32, (half, HEAD), 1)
    sin_tab = jnp.where(lane < HEAD // 2, -1.0, 1.0) * jnp.sin(angles)

    x_copy.wait()
    for index in range(chunks):
        weight_copy(index).start()
    total = jnp.zeros((rows, HEAD), F32)
    for start in range(0, depth, HEAD):
        block = x_ref[:, start:start + HEAD].astype(F32)
        total = total + block * block
    sq_own = jnp.sum(total, axis=1, keepdims=True)
    sq_send[...] = jnp.broadcast_to(sq_own, (rows, HEAD))
    pl.semaphore_wait(barrier, 1)

    def remote(source, target, slot):
        return pltpu.make_async_remote_copy(
            src_ref=source, dst_ref=target, send_sem=send_sems.at[slot], recv_sem=recv_sems.at[slot],
            device_id={"mx": peer}, device_id_type=MESH)

    sq_copy = remote(sq_send, sq_recv, chunks)
    sq_copy.start()
    sq_copy.wait()
    own_rows = pl.ds(pl.multiple_of(me * half, half), half)
    peer_rows = pl.ds(pl.multiple_of(peer * half, half), half)
    scale = lax.rsqrt((sq_send[...] + sq_recv[...]) / (2 * depth) + NORM_EPS)
    gains = gain_ref[...].astype(F32)
    for start in range(0, depth, HEAD):
        block = x_ref[:, start:start + HEAD].astype(F32)
        gain = gains[start // HEAD:start // HEAD + 1, :]
        value = (block * scale * gain).astype(BF16)
        normed[own_rows, start:start + HEAD] = value[:half]
        normed[peer_rows, start:start + HEAD] = value[half:]

    def part_copy(index):
        return remote(part_send.at[index], part_recv.at[index], index)

    def multiply(index, carry):
        weight_wait(index)
        product = jnp.dot(normed[...], w_buf[index], preferred_element_type=F32)
        part_own[index] = product[:half]
        part_send[index] = product[half:].astype(BF16)
        part_copy(index).start()
        return carry

    lax.fori_loop(0, chunks, multiply, 0)
    biases = [ref[...].astype(F32) for ref in (bq_ref, bk_ref, bv_ref)]
    for index in range(chunks):
        part_copy(index).wait()
        for head in range(2):
            lanes = slice(head * HEAD, (head + 1) * HEAD)
            columns = slice(index * width + head * HEAD, index * width + (head + 1) * HEAD)
            if index < q_chunks:
                bias = biases[0][2 * index + head:2 * index + head + 1, :]
            else:
                bias = biases[index - q_chunks + 1][head:head + 1, :]
            value = part_own[index][:, lanes] + part_recv[index][:, lanes].astype(F32) + bias
            if index < chunks - 1:
                value = value * cos_tab + pltpu.roll(value, HEAD // 2, 1) * sin_tab
            if index < q_chunks:
                q_out[:, columns] = value.astype(BF16)
            else:
                kv_out[:, (index - q_chunks) * width + head * HEAD:(index - q_chunks) * width + (head + 1) * HEAD] = value.astype(BF16)


def project(x_in, seq_lens, gain, b_q, b_k, b_v, w_q, w_k, w_v):
    rows, depth = x_in.shape
    half = rows // 2
    width = 2 * HEAD
    chunks = w_q.shape[1] // width + 2
    return pl.pallas_call(
        project_kernel,
        name="project",
        out_shape=(jax.ShapeDtypeStruct((half, w_q.shape[1]), BF16), jax.ShapeDtypeStruct((half, 2 * width), BF16)),
        in_specs=vmem_specs(6) + any_specs(4),
        out_specs=tuple(vmem_specs(2)),
        scratch_shapes=[
            VMEM((rows, depth), BF16),
            DMA,
            VMEM((chunks, depth, width), BF16),
            VMEM((rows, depth), BF16),
            VMEM((rows, HEAD), F32),
            VMEM((rows, HEAD), F32),
            VMEM((chunks, half, width), BF16),
            VMEM((chunks, half, width), BF16),
            VMEM((chunks, half, width), F32),
            DMA((chunks,)),
            DMA((chunks + 1,)),
            DMA((chunks + 1,)),
        ],
        compiler_params=pltpu.CompilerParams(collective_id=0, has_side_effects=True, vmem_limit_bytes=67043328),
    )(lane_rows(gain), lane_rows(b_q), lane_rows(b_k), lane_rows(b_v), seq_lens[None, :], rotary_frequencies(), x_in, w_q, w_k, w_v)


SLOTS = 4
ROWS_STEP = 8


def attend_kernel(lens_ref, q_ref, kv_ref, k_hbm, v_hbm, o_ref, k_out, v_out,
                  k_buf, v_buf, q_wide, q_packed, kv_wide, o_wide, parity, scores, weights, sums, in_sems, out_sems):
    batch, kv_rows, _ = k_hbm.shape
    q_heads = q_ref.shape[1] // HEAD
    group = q_heads // 2
    steps = batch // ROWS_STEP

    def load(step, kind):
        slot = lax.rem(step, SLOTS)
        source, target = ((k_hbm, k_buf), (v_hbm, v_buf))[kind]
        return pltpu.make_async_copy(source.at[pl.ds(step * ROWS_STEP, ROWS_STEP)], target.at[slot], in_sems.at[kind, slot])

    def save(step, kind):
        slot = lax.rem(step, SLOTS)
        source, target = ((k_buf, k_out), (v_buf, v_out))[kind]
        return pltpu.make_async_copy(source.at[slot], target.at[pl.ds(step * ROWS_STEP, ROWS_STEP)], out_sems.at[kind, slot])

    for step in range(2):
        for kind in range(2):
            load(step, kind).start()

    q_wide[...] = jnp.zeros_like(q_wide)
    for head in range(q_heads):
        q_wide[pl.ds(head, batch, stride=QPAD), :] = q_ref[:, head * HEAD:(head + 1) * HEAD].astype(F32)
    q_packed[...] = q_wide[...].astype(BF16)
    for kind in range(2):
        for head in range(2):
            start = (kind * 2 + head) * HEAD
            kv_wide[kind, pl.ds(head, batch, stride=2), :] = kv_ref[:, start:start + HEAD].astype(F32)
    row_head = lax.broadcasted_iota(jnp.int32, (QPAD, kv_rows), 0) >= group
    col_head = lax.rem(lax.broadcasted_iota(jnp.int32, (QPAD, kv_rows), 1), 2) == 1
    parity[...] = jnp.where(row_head == col_head, 0.0, -jnp.inf)
    columns = lax.broadcasted_iota(jnp.int32, (QPAD, kv_rows), 1)
    tile_row = lax.broadcasted_iota(jnp.int32, (16, HEAD), 0)
    tile_pos = lax.div(tile_row, 2)
    tile_odd = lax.rem(tile_row, 2) == 1

    def body(step, carry):
        slot = lax.rem(step, SLOTS)

        @pl.when(step + 2 < steps)
        def _():
            @pl.when(step >= 2)
            def _():
                for kind in range(2):
                    save(step - 2, kind).wait()
            for kind in range(2):
                load(step + 2, kind).start()

        for kind in range(2):
            load(step, kind).wait()
        for row in range(ROWS_STEP):
            index = step * ROWS_STEP + row
            position = lens_ref[index]
            base = pl.multiple_of(lax.div(position, 8) * 16, 16)
            offset = lax.rem(position, 8)
            for kind, buffer in ((0, k_buf), (1, v_buf)):
                low = kv_wide[kind, pl.ds(2 * index, 1), :]
                high = kv_wide[kind, pl.ds(2 * index + 1, 1), :]
                fresh = jnp.where(tile_odd, high, low).astype(BF16)
                tile = buffer[slot, row, pl.ds(base, 16), :]
                buffer[slot, row, pl.ds(base, 16), :] = jnp.where(tile_pos == offset, fresh, tile)
        for row in range(ROWS_STEP):
            q_start = pl.multiple_of((step * ROWS_STEP + row) * QPAD, QPAD)
            scores[row] = lax.dot_general(q_packed[pl.ds(q_start, QPAD), :], k_buf[slot, row], (((1,), (1,)), ((), ())),
                                          preferred_element_type=F32)
        for kind in range(2):
            save(step, kind).start()
        for row in range(ROWS_STEP):
            limit = 2 * lens_ref[step * ROWS_STEP + row] + 2
            masked = jnp.where(columns < limit, scores[row] * HEAD ** -0.5 + parity[...], -jnp.inf)
            weight = jnp.exp(masked - jnp.max(masked, axis=1, keepdims=True))
            sums[row] = jnp.broadcast_to(jnp.sum(weight, axis=1, keepdims=True), (QPAD, HEAD))
            weights[row] = weight.astype(BF16)
        for row in range(ROWS_STEP):
            q_start = pl.multiple_of((step * ROWS_STEP + row) * QPAD, QPAD)
            mixed = jnp.dot(weights[row], v_buf[slot, row], preferred_element_type=F32)
            o_wide[pl.ds(q_start, QPAD), :] = mixed / sums[row]
        return carry

    lax.fori_loop(0, steps, body, 0)
    for head in range(q_heads):
        o_ref[:, head * HEAD:(head + 1) * HEAD] = o_wide[pl.ds(head, batch, stride=QPAD), :].astype(BF16)
    for step in range(steps - SLOTS, steps):
        for kind in range(2):
            save(step, kind).wait()


def attend(seq_lens, q_rot, kv_new, k_cache, v_cache):
    batch, seq_len, kv_heads, _ = k_cache.shape
    rows = seq_len * kv_heads
    flat = (batch, rows, HEAD)
    out, k_out, v_out = pl.pallas_call(
        attend_kernel,
        name="attend",
        out_shape=(jax.ShapeDtypeStruct(q_rot.shape, BF16), jax.ShapeDtypeStruct(flat, BF16), jax.ShapeDtypeStruct(flat, BF16)),
        in_specs=[pl.BlockSpec(memory_space=pltpu.SMEM)] + vmem_specs(2) + any_specs(2),
        out_specs=tuple(vmem_specs(1) + any_specs(2)),
        scratch_shapes=[
            VMEM((SLOTS, ROWS_STEP, rows, HEAD), BF16),
            VMEM((SLOTS, ROWS_STEP, rows, HEAD), BF16),
            VMEM((batch * QPAD, HEAD), F32),
            VMEM((batch * QPAD, HEAD), BF16),
            VMEM((2, batch * 2, HEAD), F32),
            VMEM((batch * QPAD, HEAD), F32),
            VMEM((QPAD, rows), F32),
            VMEM((ROWS_STEP, QPAD, rows), F32),
            VMEM((ROWS_STEP, QPAD, rows), BF16),
            VMEM((ROWS_STEP, QPAD, HEAD), F32),
            DMA((2, SLOTS)),
            DMA((2, SLOTS)),
        ],
        compiler_params=pltpu.CompilerParams(vmem_limit_bytes=64 << 20),
    )(seq_lens, q_rot, kv_new, k_cache.reshape(flat), v_cache.reshape(flat))
    return out, k_out.reshape(k_cache.shape), v_out.reshape(v_cache.shape)


BLOCK = 256
RING = 36


def tail_kernel(gain_ref, attn_hbm, x_hbm, wo_hbm, wg_hbm, wu_hbm, wd_hbm, out_hbm,
                out_ref, pool, full, rows_in, part, keep, recv_one, send_two, recv_two, x_own, mid, sq_send, sq_recv,
                h_rows, h_cols, gu_send, gu_recv, gu_own, act, early,
                pool_sems, x_sem, attn_sem, core_sems, rs_sems, ag_sems, gu_sems, act_sems):
    my = lax.axis_index("my")
    me = lax.axis_index("mx")
    peer = 1 - me
    side_x = my + 1 - 2 * lax.rem(my, 2)
    side_y = lax.rem(my + 2, 4)
    cross = 3 - my
    half, depth = attn_hbm.shape
    batch = 2 * half
    quarter = batch // 4
    hidden = x_hbm.shape[1]
    ff = wg_hbm.shape[0]
    col_chunks = hidden // BLOCK
    ff_chunks = pl.cdiv(ff, BLOCK)
    ff_rest = ff - (ff_chunks - 1) * BLOCK
    chunk_ring = RING // 2
    out_blocks = depth // BLOCK
    out_slot = RING - 6
    down_slot = RING - ff_chunks
    early_blocks = chunk_ring
    late_chunk = chunk_ring + chunk_ring // 2 - (down_slot // 2)
    late_count = ff_chunks - late_chunk

    def slot_rows(slot, count=BLOCK):
        return pl.ds(pl.multiple_of(slot * BLOCK, BLOCK), count)

    def block_copy(source, block, slot, count=BLOCK):
        return pltpu.make_async_copy(source.at[slot_rows(block, count)], pool.at[slot_rows(slot, count)], pool_sems.at[slot])

    def ff_slot(chunk):
        return 2 * jnp.where(chunk < chunk_ring, chunk, jnp.where(chunk < late_chunk, chunk - late_chunk + chunk_ring // 2, chunk - late_chunk))

    def ff_copies(chunk, count=BLOCK):
        slot = ff_slot(chunk)
        return block_copy(wg_hbm, chunk, slot, count), block_copy(wu_hbm, chunk, slot + 1, count)

    def down_copy(block, count=BLOCK):
        slot = down_slot + jnp.where(block < early_blocks, block + ff_chunks - early_blocks, block - early_blocks)
        return block_copy(wd_hbm, block, slot, count)

    def out_copy(block):
        return block_copy(wo_hbm, block, out_slot + block)

    def to_core(source, target, slot):
        return pltpu.make_async_remote_copy(src_ref=source, dst_ref=target, send_sem=slot[0], recv_sem=slot[1],
                                            device_id={"mx": peer}, device_id_type=MESH)

    def to_chip(source, target, chip, send_sem, recv_sem):
        return pltpu.make_async_remote_copy(src_ref=source, dst_ref=target, send_sem=send_sem, recv_sem=recv_sem,
                                            device_id={"my": chip}, device_id_type=MESH)

    own_half = pl.ds(pl.multiple_of(me * half, half), half)
    peer_half = pl.ds(pl.multiple_of(peer * half, half), half)
    attn_load = pltpu.make_async_copy(attn_hbm, full.at[own_half], attn_sem)
    attn_load.start()
    own_rows = pl.ds(pl.multiple_of(my * quarter, quarter), quarter)
    x_copy = pltpu.make_async_copy(x_hbm.at[own_rows], x_own, x_sem)
    x_copy.start()

    barrier = pltpu.get_barrier_semaphore()
    pl.semaphore_signal(barrier, inc=1, device_id={"mx": peer}, device_id_type=MESH)
    pl.semaphore_signal(barrier, inc=1, device_id={"my": side_x}, device_id_type=MESH)
    pl.semaphore_signal(barrier, inc=1, device_id={"my": side_y}, device_id_type=MESH)
    attn_load.wait()
    for block in range(out_blocks):
        out_copy(block).start()
    pl.semaphore_wait(barrier, 3)
    attn_copy = to_core(full.at[own_half], full.at[own_half], (core_sems.at[0], core_sems.at[1]))
    attn_copy.start()
    attn_copy.wait()
    for place, owner in enumerate((my, side_x, cross, side_y)):
        rows_in[place * quarter:(place + 1) * quarter, :] = full[pl.ds(pl.multiple_of(owner * quarter, quarter), quarter), :]

    def columns(chunk):
        if isinstance(chunk, int):
            return slice(chunk * BLOCK, (chunk + 1) * BLOCK)
        return pl.ds(pl.multiple_of(chunk * BLOCK, BLOCK), BLOCK)

    def first_side(parity):
        return (side_x, side_y)[parity]

    def second_side(parity):
        return (side_y, side_x)[parity]

    def scatter_one(chunk, parity):
        return to_chip(part.at[chunk], recv_one.at[chunk], first_side(parity), rs_sems.at[0, 0, chunk], rs_sems.at[0, 1, chunk])

    def scatter_two(chunk, parity):
        return to_chip(send_two.at[chunk], recv_two.at[chunk], second_side(parity), rs_sems.at[1, 0, chunk], rs_sems.at[1, 1, chunk])

    def scatter_start(pair, total):
        for parity in range(2):
            chunk = 2 * pair + parity
            value = total[:, parity * BLOCK:(parity + 1) * BLOCK]
            lead = quarter * (1 + parity)
            part[chunk] = value[lead:lead + 2 * quarter].astype(BF16)
            keep[chunk, 0] = value[:quarter]
            other = 3 * quarter if parity == 0 else quarter
            keep[chunk, 1] = value[other:other + quarter]
        for parity in range(2):
            scatter_one(2 * pair + parity, parity).start()

    def scatter_pass(chunk, parity):
        scatter_one(chunk, parity).wait()
        mine = slice(0, quarter) if parity == 0 else slice(quarter, 2 * quarter)
        theirs = slice(quarter, 2 * quarter) if parity == 0 else slice(0, quarter)
        send_two[chunk] = (keep[chunk, 1] + recv_one[chunk, theirs, :].astype(F32)).astype(BF16)
        scatter_two(chunk, parity).start()
        keep[chunk, 0] = keep[chunk, 0] + recv_one[chunk, mine, :].astype(F32)

    def scatter_end(chunk, parity):
        scatter_two(chunk, parity).wait()
        return keep[chunk, 0] + recv_two[chunk].astype(F32)

    def mid_end(chunk):
        mid[:, columns(chunk)] = (x_own[:, columns(chunk)].astype(F32) + scatter_end(chunk, chunk % 2)).astype(BF16).astype(F32)

    x_copy.wait()
    for block in range(out_blocks):
        out_copy(block).wait()
    for chunk in range(out_slot // 2):
        for copy in ff_copies(chunk):
            copy.start()
    def out_product(pair, carry):
        lanes = pl.ds(pl.multiple_of(pair * 2 * BLOCK, 2 * BLOCK), 2 * BLOCK)
        weights = pool[out_slot * BLOCK:out_slot * BLOCK + depth, lanes]
        scatter_start(pair, jnp.dot(rows_in[...], weights, preferred_element_type=F32))
        return carry

    lax.fori_loop(0, col_chunks // 2, out_product, 0)
    for chunk in range(out_slot // 2, chunk_ring):
        for copy in ff_copies(chunk):
            copy.start()
    for chunk in range(col_chunks + 3):
        if chunk < col_chunks:
            scatter_pass(chunk, chunk % 2)
        if chunk >= 3:
            mid_end(chunk - 3)

    square = jnp.zeros((quarter, HEAD), F32)
    for start in range(0, hidden, HEAD):
        square = square + mid[:, start:start + HEAD] * mid[:, start:start + HEAD]
    sq_send[...] = jnp.broadcast_to(jnp.sum(square, axis=1, keepdims=True), (quarter, HEAD))
    sq_copy = to_core(sq_send, sq_recv, (core_sems.at[2], core_sems.at[3]))
    sq_copy.start()
    sq_copy.wait()
    scale = lax.rsqrt((sq_send[...] + sq_recv[...]) / (2 * hidden) + NORM_EPS)

    def place_rows(place):
        return slice(place * quarter, (place + 1) * quarter)

    def gather_x(chunk):
        return to_chip(h_rows.at[place_rows(0), columns(chunk)], h_rows.at[place_rows(1), columns(chunk)], side_x,
                       ag_sems.at[0, 0, chunk], ag_sems.at[0, 1, chunk])

    def gather_y(chunk):
        return to_chip(h_rows.at[place_rows(0), columns(chunk)], h_rows.at[place_rows(3), columns(chunk)], side_y,
                       ag_sems.at[1, 0, chunk], ag_sems.at[1, 1, chunk])

    def gather_cross(chunk):
        source = 1 if chunk % 2 == 0 else 3
        return to_chip(h_rows.at[place_rows(source), columns(chunk)], h_rows.at[place_rows(2), columns(chunk)], second_side(chunk % 2),
                       ag_sems.at[2, 0, chunk], ag_sems.at[2, 1, chunk])

    gains = gain_ref[...].astype(F32)
    for chunk in range(col_chunks):
        for start in range(chunk * BLOCK, (chunk + 1) * BLOCK, HEAD):
            gain = gains[start // HEAD:start // HEAD + 1, :]
            h_rows[:quarter, start:start + HEAD] = (mid[:, start:start + HEAD] * scale * gain).astype(BF16)
        gather_x(chunk).start()
        gather_y(chunk).start()
    for chunk in range(col_chunks):
        (gather_x if chunk % 2 == 0 else gather_y)(chunk).wait_recv()
        gather_cross(chunk).start()

    for chunk in range(col_chunks):
        (gather_y if chunk % 2 == 0 else gather_x)(chunk).wait_recv()
        gather_cross(chunk).wait_recv()
        for place, source in enumerate((own_half, peer_half)):
            h_cols[columns(chunk), place * half:(place + 1) * half] = h_rows[source, columns(chunk)].astype(F32).T.astype(BF16)
        gather_x(chunk).wait_send()
        gather_y(chunk).wait_send()
        gather_cross(chunk).wait_send()

    def gu_copy(chunk):
        slot = lax.rem(chunk, 4)
        return to_core(gu_send.at[slot], gu_recv.at[slot], (gu_sems.at[0, slot], gu_sems.at[1, slot]))

    def act_lanes(chunk):
        place = jnp.where(chunk < early_blocks, chunk + ff_chunks - early_blocks, chunk - early_blocks)
        return pl.ds(pl.multiple_of(place * BLOCK, BLOCK), BLOCK)

    def act_copy(chunk):
        lanes = act_lanes(chunk)
        return to_core(act.at[own_half, lanes], act.at[own_half, lanes], (act_sems.at[0, lax.rem(chunk, 8)], act_sems.at[1, lax.rem(chunk, 8)]))

    def ff_products(chunk):
        slot = lax.rem(chunk, 4)
        base = ff_slot(chunk)
        product = jnp.dot(pool[slot_rows(base, 2 * BLOCK), :], h_cols[...], preferred_element_type=F32)
        for kind in range(2):
            rows = slice(kind * BLOCK, (kind + 1) * BLOCK)
            gu_own[slot, kind] = product[rows, :half]
            gu_send[slot, kind] = product[rows, half:].astype(BF16)

    def activate(chunk):
        slot = lax.rem(chunk, 4)
        gate = gu_own[slot, 0] + gu_recv[slot, 0].astype(F32)
        up = gu_own[slot, 1] + gu_recv[slot, 1].astype(F32)
        value = gate * jax.nn.sigmoid(gate) * up
        row = chunk * BLOCK + lax.broadcasted_iota(jnp.int32, value.shape, 0)
        value = jnp.where(row < ff, value, 0.0)
        lanes = act_lanes(chunk)
        act[own_half, lanes] = value.T.astype(BF16)

    def refill(chunk):
        half_ring = chunk_ring // 2

        @pl.when(chunk < late_count - 1)
        def _():
            for copy in ff_copies(late_chunk + chunk):
                copy.start()

        @pl.when(chunk == late_count - 1)
        def _():
            for copy in ff_copies(ff_chunks - 1, ff_rest):
                copy.start()

        @pl.when((chunk >= late_count) & (chunk < half_ring))
        def _():
            for copy in ff_copies(chunk - late_count + chunk_ring):
                copy.start()

        @pl.when((chunk >= half_ring) & (chunk < chunk_ring))
        def _():
            down_copy(2 * (chunk - half_ring)).start()
            down_copy(2 * (chunk - half_ring) + 1).start()

        free = 2 * (chunk - chunk_ring + late_count) - down_slot + early_blocks

        @pl.when((chunk >= chunk_ring) & (chunk < late_chunk) & (free >= early_blocks))
        def _():
            down_copy(free).start()

        @pl.when((chunk >= chunk_ring) & (chunk < late_chunk - 1))
        def _():
            down_copy(free + 1).start()

        @pl.when(chunk == late_chunk - 1)
        def _():
            down_copy(ff_chunks - 1, ff_rest).start()

    def ff_step(chunk, carry):
        @pl.when(chunk >= 7)
        def _():
            act_copy(chunk - 7).wait()
        gu_copy(chunk - 2).wait()
        for copy in ff_copies(chunk):
            copy.wait()
        activate(chunk - 2)
        ff_products(chunk)
        gu_copy(chunk).start()
        act_copy(chunk - 2).start()
        refill(chunk)
        return carry

    def ff_first(chunk, carry):
        for copy in ff_copies(chunk):
            copy.wait()
        ff_products(chunk)
        gu_copy(chunk).start()
        refill(chunk)
        return carry

    lax.fori_loop(0, 2, ff_first, 0)
    lax.fori_loop(2, ff_chunks - 1, ff_step, 0)
    last = ff_chunks - 1
    act_copy(last - 7).wait()
    gu_copy(last - 2).wait()
    for copy in ff_copies(last, ff_rest):
        copy.wait()
    activate(last - 2)
    ff_products(last)
    gu_copy(last).start()
    act_copy(last - 2).start()

    for block in range(early_blocks):
        down_copy(block).wait()
    late_lanes = (ff_chunks - early_blocks) * BLOCK
    late_row = down_slot * BLOCK + late_lanes

    def pair_lanes(pair):
        return pl.ds(pl.multiple_of(pair * 2 * BLOCK, 2 * BLOCK), 2 * BLOCK)

    for chunk in range(last - 6, last - 3):
        act_copy(chunk).wait()

    def down_early(pair, carry):
        early[...] = jnp.dot(act[:, late_lanes:], pool[late_row:, pair_lanes(pair)], preferred_element_type=F32)
        return carry

    lax.fori_loop(0, 1, down_early, 0)
    gu_copy(last - 1).wait()
    activate(last - 1)
    act_copy(last - 1).start()
    gu_copy(last).wait()
    activate(last)
    act_copy(last).start()
    for block in range(early_blocks, ff_chunks):
        down_copy(block, ff_rest if block == last else BLOCK).wait()
    for chunk in range(last - 3, ff_chunks):
        act_copy(chunk).wait()

    def owner_rows(owner):
        return pl.ds(pl.multiple_of(owner * quarter, quarter), quarter)

    def final_x(chunk):
        block = out_ref.at[owner_rows(my), columns(chunk)]
        return to_chip(block, block, side_x, ag_sems.at[0, 0, chunk], ag_sems.at[0, 1, chunk])

    def final_y(chunk):
        block = out_ref.at[owner_rows(my), columns(chunk)]
        return to_chip(block, block, side_y, ag_sems.at[1, 0, chunk], ag_sems.at[1, 1, chunk])

    def final_cross(chunk):
        block = out_ref.at[owner_rows(first_side(chunk % 2)), columns(chunk)]
        return to_chip(block, block, second_side(chunk % 2), ag_sems.at[2, 0, chunk], ag_sems.at[2, 1, chunk])

    def save_out(chunk):
        return pltpu.make_async_copy(out_ref.at[:, columns(chunk)], out_hbm.at[:, columns(chunk)], pool_sems.at[chunk])

    def out_end(chunk):
        out_ref[owner_rows(my), columns(chunk)] = (mid[:, columns(chunk)] + scatter_end(chunk, chunk % 2)).astype(BF16)
        final_x(chunk).start()
        final_y(chunk).start()

    def out_pass(chunk):
        (final_x if chunk % 2 == 0 else final_y)(chunk).wait_recv()
        final_cross(chunk).start()

    def down_rest(pair, carry):
        total = jnp.dot(act[:, :late_lanes], pool[down_slot * BLOCK:late_row, pair_lanes(pair)], preferred_element_type=F32)
        scatter_start(pair, early[...] + total)
        return carry

    def down_pair(pair, carry):
        scatter_start(pair, jnp.dot(act[...], pool[down_slot * BLOCK:, pair_lanes(pair)], preferred_element_type=F32))

        @pl.when(pair >= 2)
        def _():
            for parity in range(2):
                scatter_pass(2 * (pair - 2) + parity, parity)
        return carry

    pairs = col_chunks // 2
    lax.fori_loop(0, 1, down_rest, 0)
    lax.fori_loop(1, pairs, down_pair, 0)
    passed = 2 * (pairs - 2)
    for step in range(passed, col_chunks + 6):
        if step < col_chunks:
            scatter_pass(step, step % 2)
        if step == passed:
            for chunk in range(passed - 2):
                out_end(chunk)
        if 0 <= step - 2 < col_chunks and step - 2 >= passed - 2:
            out_end(step - 2)
        if step == passed:
            for chunk in range(passed - 4):
                out_pass(chunk)
        if 0 <= step - 4 < col_chunks and step - 4 >= passed - 4:
            out_pass(step - 4)
    for chunk in range(col_chunks):
        (final_y if chunk % 2 == 0 else final_x)(chunk).wait_recv()
        final_cross(chunk).wait_recv()
        save_out(chunk).start()
    for chunk in range(col_chunks):
        final_cross(chunk).wait_send()
        final_x(chunk).wait_send()
        final_y(chunk).wait_send()
        save_out(chunk).wait()


def tail(attn_rows, gain, x_in, w_o, wg_rows, wu_rows, w_down):
    half, depth = attn_rows.shape
    rows, hidden = x_in.shape
    quarter = rows // 4
    chunks = hidden // BLOCK
    ff_chunks = pl.cdiv(w_down.shape[0], BLOCK)
    return pl.pallas_call(
        tail_kernel,
        name="tail",
        out_shape=jax.ShapeDtypeStruct((rows, hidden), BF16),
        in_specs=vmem_specs(1) + any_specs(6),
        out_specs=any_specs(1)[0],
        scratch_shapes=[
            VMEM((rows, hidden), BF16),
            VMEM((RING * BLOCK, hidden), BF16),
            VMEM((rows, depth), BF16),
            VMEM((rows, depth), BF16),
            VMEM((chunks, 2 * quarter, BLOCK), BF16),
            VMEM((chunks, 2, quarter, BLOCK), F32),
            VMEM((chunks, 2 * quarter, BLOCK), BF16),
            VMEM((chunks, quarter, BLOCK), BF16),
            VMEM((chunks, quarter, BLOCK), BF16),
            VMEM((quarter, hidden), BF16),
            VMEM((quarter, hidden), F32),
            VMEM((quarter, HEAD), F32),
            VMEM((quarter, HEAD), F32),
            VMEM((rows, hidden), BF16),
            VMEM((hidden, rows), BF16),
            VMEM((4, 2, BLOCK, half), BF16),
            VMEM((4, 2, BLOCK, half), BF16),
            VMEM((4, 2, BLOCK, half), F32),
            VMEM((rows, ff_chunks * BLOCK), BF16),
            VMEM((rows, 2 * BLOCK), F32),
            DMA((RING,)),
            DMA,
            DMA,
            DMA((4,)),
            DMA((2, 2, chunks)),
            DMA((3, 2, chunks)),
            DMA((2, 4)),
            DMA((2, 8)),
        ],
        compiler_params=pltpu.CompilerParams(collective_id=1, has_side_effects=True, vmem_limit_bytes=67043328),
    )(lane_rows(gain), attn_rows, x_in, w_o, wg_rows, wu_rows, w_down)


def solution(mesh):
    act_spec = P(None, "mx")
    cache_spec = P("mx", None, "my", None)
    in_specs = (act_spec, P("mx"), P("mx"), P("mx"), P("mx", "my"), P("my"), P("mx", "my"), P("my"), P("mx", "my"), P("my"), P("my", "mx"), P("mx", "my"), P("mx", "my"), P("my", "mx"), cache_spec, cache_spec)
    out_specs = (act_spec, cache_spec, cache_spec)

    def local_layer(x_in, seq_lens, gain_attn, gain_mlp, w_q, b_q, w_k, b_k, w_v, b_v, w_o, w_gate, w_up, w_down, k_cache, v_cache):
        q_rot, kv_new = project(x_in, seq_lens, gain_attn, b_q, b_k, b_v, w_q, w_k, w_v)
        attn_rows, k_cache_out, v_cache_out = attend(seq_lens, q_rot, kv_new, k_cache, v_cache)
        x_out = tail(attn_rows, gain_mlp, x_in, w_o, w_gate.T, w_up.T, w_down)
        return x_out, k_cache_out, v_cache_out

    return jax.shard_map(local_layer, mesh=mesh, in_specs=in_specs, out_specs=out_specs, check_vma=False)
```

```python
import jax
import jax.numpy as jnp
import numpy as np
from jax import lax
from jax.experimental import pallas as pl
from jax.experimental.pallas import tpu as pltpu
from jax.sharding import PartitionSpec as P

HEAD = 128
NORM_EPS = 1e-6
ROPE_THETA = 1000000.0
MESH = pl.DeviceIdType.MESH
F32 = jnp.float32
BF16 = jnp.bfloat16
QPAD = 16
VMEM = pltpu.VMEM
DMA = pltpu.SemaphoreType.DMA


def any_specs(count):
    return [pl.BlockSpec(memory_space=pl.ANY)] * count


def vmem_specs(count):
    return [pl.BlockSpec(memory_space=pltpu.VMEM)] * count


def lane_rows(vector):
    return vector.reshape(-1, HEAD)


def rotary_frequencies():
    half_dim = HEAD // 2
    inv_freq = np.float32(ROPE_THETA) ** (np.float32(-2.0) * np.arange(half_dim, dtype=np.float32) / np.float32(HEAD))
    return jnp.asarray(np.concatenate([inv_freq, inv_freq])[None, :], F32)


def project_kernel(gain_hbm, bq_hbm, bk_hbm, bv_hbm, lens_hbm, freq_hbm, x_hbm, wq_hbm, wk_hbm, wv_hbm, q_out, kv_out,
                   gain_ref, bq_ref, bk_ref, bv_ref, lens_ref, freq_ref, small_sems, x_ref, x_sem, w_buf, normed, sq_send, sq_recv, part_send, part_recv, part_own, w_sems, send_sems, recv_sems):
    me = lax.axis_index("mx")
    peer = 1 - me
    rows, depth = x_hbm.shape
    half = rows // 2
    width = 2 * HEAD
    q_chunks = wq_hbm.shape[1] // width
    chunks = q_chunks + 2

    def weight_copy(index):
        if index < q_chunks:
            source = wq_hbm.at[:, pl.ds(index * width, width)]
        else:
            source = (wk_hbm, wv_hbm)[index - q_chunks]
        return pltpu.make_async_copy(source, w_buf.at[index], w_sems.at[index])

    def weight_wait(index):
        pltpu.make_async_copy(wk_hbm, w_buf.at[index], w_sems.at[index]).wait()

    smalls = [pltpu.make_async_copy(source, target, small_sems.at[slot]) for slot, (source, target) in enumerate((
        (lens_hbm, lens_ref), (freq_hbm, freq_ref), (gain_hbm, gain_ref), (bq_hbm, bq_ref), (bk_hbm, bk_ref), (bv_hbm, bv_ref)))]
    for copy in smalls:
        copy.start()
    x_copy = pltpu.make_async_copy(x_hbm, x_ref, x_sem)
    x_copy.start()
    barrier = pltpu.get_barrier_semaphore()
    pl.semaphore_signal(barrier, inc=1, device_id={"mx": peer}, device_id_type=MESH)

    for copy in smalls:
        copy.wait()
    positions = jnp.broadcast_to(lens_ref[...].astype(F32), (half, half)).T
    angles = positions * freq_ref[...]
    cos_tab = jnp.cos(angles)
    lane = lax.broadcasted_iota(jnp.int32, (half, HEAD), 1)
    sin_tab = jnp.where(lane < HEAD // 2, -1.0, 1.0) * jnp.sin(angles)

    x_copy.wait()
    for index in range(chunks):
        weight_copy(index).start()
    total = jnp.zeros((rows, HEAD), F32)
    for start in range(0, depth, HEAD):
        block = x_ref[:, start:start + HEAD].astype(F32)
        total = total + block * block
    sq_own = jnp.sum(total, axis=1, keepdims=True)
    sq_send[...] = jnp.broadcast_to(sq_own, (rows, HEAD))
    pl.semaphore_wait(barrier, 1)

    def remote(source, target, slot):
        return pltpu.make_async_remote_copy(
            src_ref=source, dst_ref=target, send_sem=send_sems.at[slot], recv_sem=recv_sems.at[slot],
            device_id={"mx": peer}, device_id_type=MESH)

    sq_copy = remote(sq_send, sq_recv, chunks)
    sq_copy.start()
    sq_copy.wait()
    own_rows = pl.ds(pl.multiple_of(me * half, half), half)
    peer_rows = pl.ds(pl.multiple_of(peer * half, half), half)
    scale = lax.rsqrt((sq_send[...] + sq_recv[...]) / (2 * depth) + NORM_EPS)
    gains = gain_ref[...].astype(F32)
    for start in range(0, depth, HEAD):
        block = x_ref[:, start:start + HEAD].astype(F32)
        gain = gains[start // HEAD:start // HEAD + 1, :]
        value = (block * scale * gain).astype(BF16)
        normed[own_rows, start:start + HEAD] = value[:half]
        normed[peer_rows, start:start + HEAD] = value[half:]

    def part_copy(index):
        return remote(part_send.at[index], part_recv.at[index], index)

    def multiply(index, carry):
        weight_wait(index)
        product = jnp.dot(normed[...], w_buf[index], preferred_element_type=F32)
        part_own[index] = product[:half]
        part_send[index] = product[half:].astype(BF16)
        part_copy(index).start()
        return carry

    lax.fori_loop(0, chunks, multiply, 0)
    biases = [ref[...].astype(F32) for ref in (bq_ref, bk_ref, bv_ref)]
    for index in range(chunks):
        part_copy(index).wait()
        for head in range(2):
            lanes = slice(head * HEAD, (head + 1) * HEAD)
            columns = slice(index * width + head * HEAD, index * width + (head + 1) * HEAD)
            if index < q_chunks:
                bias = biases[0][2 * index + head:2 * index + head + 1, :]
            else:
                bias = biases[index - q_chunks + 1][head:head + 1, :]
            value = part_own[index][:, lanes] + part_recv[index][:, lanes].astype(F32) + bias
            if index < chunks - 1:
                value = value * cos_tab + pltpu.roll(value, HEAD // 2, 1) * sin_tab
            if index < q_chunks:
                q_out[:, columns] = value.astype(BF16)
            else:
                kv_out[:, (index - q_chunks) * width + head * HEAD:(index - q_chunks) * width + (head + 1) * HEAD] = value.astype(BF16)


def project(x_in, seq_lens, gain, b_q, b_k, b_v, w_q, w_k, w_v):
    rows, depth = x_in.shape
    half = rows // 2
    width = 2 * HEAD
    chunks = w_q.shape[1] // width + 2
    return pl.pallas_call(
        project_kernel,
        name="project",
        out_shape=(jax.ShapeDtypeStruct((half, w_q.shape[1]), BF16), jax.ShapeDtypeStruct((half, 2 * width), BF16)),
        in_specs=any_specs(10),
        out_specs=tuple(vmem_specs(2)),
        scratch_shapes=[
            VMEM((depth // HEAD, HEAD), BF16),
            VMEM((w_q.shape[1] // HEAD, HEAD), BF16),
            VMEM((2, HEAD), BF16),
            VMEM((2, HEAD), BF16),
            VMEM((1, half), jnp.int32),
            VMEM((1, HEAD), F32),
            DMA((6,)),
            VMEM((rows, depth), BF16),
            DMA,
            VMEM((chunks, depth, width), BF16),
            VMEM((rows, depth), BF16),
            VMEM((rows, HEAD), F32),
            VMEM((rows, HEAD), F32),
            VMEM((chunks, half, width), BF16),
            VMEM((chunks, half, width), BF16),
            VMEM((chunks, half, width), F32),
            DMA((chunks,)),
            DMA((chunks + 1,)),
            DMA((chunks + 1,)),
        ],
        compiler_params=pltpu.CompilerParams(collective_id=0, has_side_effects=True, vmem_limit_bytes=67043328),
    )(lane_rows(gain), lane_rows(b_q), lane_rows(b_k), lane_rows(b_v), seq_lens[None, :], rotary_frequencies(), x_in, w_q, w_k, w_v)


SLOTS = 6
ROWS_STEP = 8


def attend_kernel(lens_ref, q_hbm, kv_hbm, k_hbm, v_hbm, o_ref, k_out, v_out,
                  q_ref, kv_ref, small_sems, k_buf, v_buf, q_wide, q_packed, kv_wide, o_wide, parity, scores, weights, sums, in_sems, out_sems):
    batch, kv_rows, _ = k_hbm.shape
    q_heads = q_hbm.shape[1] // HEAD
    group = q_heads // 2
    steps = batch // ROWS_STEP

    def load(step, kind):
        slot = lax.rem(step, SLOTS)
        source, target = ((k_hbm, k_buf), (v_hbm, v_buf))[kind]
        return pltpu.make_async_copy(source.at[pl.ds(step * ROWS_STEP, ROWS_STEP)], target.at[slot], in_sems.at[kind, slot])

    def save(step, kind):
        slot = lax.rem(step, SLOTS)
        source, target = ((k_buf, k_out), (v_buf, v_out))[kind]
        return pltpu.make_async_copy(source.at[slot], target.at[pl.ds(step * ROWS_STEP, ROWS_STEP)], out_sems.at[kind, slot])

    q_copy = pltpu.make_async_copy(q_hbm, q_ref, small_sems.at[0])
    kv_copy = pltpu.make_async_copy(kv_hbm, kv_ref, small_sems.at[1])
    q_copy.start()
    kv_copy.start()
    for step in range(3):
        for kind in range(2):
            load(step, kind).start()

    q_wide[...] = jnp.zeros_like(q_wide)
    q_copy.wait()
    kv_copy.wait()
    for head in range(q_heads):
        q_wide[pl.ds(head, batch, stride=QPAD), :] = q_ref[:, head * HEAD:(head + 1) * HEAD].astype(F32)
    q_packed[...] = q_wide[...].astype(BF16)
    for kind in range(2):
        for head in range(2):
            start = (kind * 2 + head) * HEAD
            kv_wide[kind, pl.ds(head, batch, stride=2), :] = kv_ref[:, start:start + HEAD].astype(F32)
    row_head = lax.broadcasted_iota(jnp.int32, (QPAD, kv_rows), 0) >= group
    col_head = lax.rem(lax.broadcasted_iota(jnp.int32, (QPAD, kv_rows), 1), 2) == 1
    parity[...] = jnp.where(row_head == col_head, 0.0, -jnp.inf)
    columns = lax.broadcasted_iota(jnp.int32, (QPAD, kv_rows), 1)
    tile_row = lax.broadcasted_iota(jnp.int32, (16, HEAD), 0)
    tile_pos = lax.div(tile_row, 2)
    tile_odd = lax.rem(tile_row, 2) == 1

    def body(step, carry):
        slot = lax.rem(step, SLOTS)

        @pl.when(step + 3 < steps)
        def _():
            @pl.when(step >= 3)
            def _():
                for kind in range(2):
                    save(step - 3, kind).wait()
            for kind in range(2):
                load(step + 3, kind).start()

        for kind in range(2):
            load(step, kind).wait()
        for row in range(ROWS_STEP):
            index = step * ROWS_STEP + row
            position = lens_ref[index]
            base = pl.multiple_of(lax.div(position, 8) * 16, 16)
            offset = lax.rem(position, 8)
            for kind, buffer in ((0, k_buf), (1, v_buf)):
                low = kv_wide[kind, pl.ds(2 * index, 1), :]
                high = kv_wide[kind, pl.ds(2 * index + 1, 1), :]
                fresh = jnp.where(tile_odd, high, low).astype(BF16)
                tile = buffer[slot, row, pl.ds(base, 16), :]
                buffer[slot, row, pl.ds(base, 16), :] = jnp.where(tile_pos == offset, fresh, tile)
        for row in range(ROWS_STEP):
            q_start = pl.multiple_of((step * ROWS_STEP + row) * QPAD, QPAD)
            scores[row] = lax.dot_general(q_packed[pl.ds(q_start, QPAD), :], k_buf[slot, row], (((1,), (1,)), ((), ())),
                                          preferred_element_type=F32)
        for kind in range(2):
            save(step, kind).start()
        for row in range(ROWS_STEP):
            limit = 2 * lens_ref[step * ROWS_STEP + row] + 2
            masked = jnp.where(columns < limit, scores[row] * HEAD ** -0.5 + parity[...], -jnp.inf)
            weight = jnp.exp(masked - jnp.max(masked, axis=1, keepdims=True))
            sums[row] = jnp.broadcast_to(jnp.sum(weight, axis=1, keepdims=True), (QPAD, HEAD))
            weights[row] = weight.astype(BF16)
        for row in range(ROWS_STEP):
            q_start = pl.multiple_of((step * ROWS_STEP + row) * QPAD, QPAD)
            mixed = jnp.dot(weights[row], v_buf[slot, row], preferred_element_type=F32)
            o_wide[pl.ds(q_start, QPAD), :] = mixed / sums[row]
        return carry

    lax.fori_loop(0, steps, body, 0)
    for head in range(q_heads):
        o_ref[:, head * HEAD:(head + 1) * HEAD] = o_wide[pl.ds(head, batch, stride=QPAD), :].astype(BF16)
    for step in range(steps - SLOTS, steps):
        for kind in range(2):
            save(step, kind).wait()


def attend(seq_lens, q_rot, kv_new, k_cache, v_cache):
    batch, seq_len, kv_heads, _ = k_cache.shape
    rows = seq_len * kv_heads
    flat = (batch, rows, HEAD)
    out, k_out, v_out = pl.pallas_call(
        attend_kernel,
        name="attend",
        out_shape=(jax.ShapeDtypeStruct(q_rot.shape, BF16), jax.ShapeDtypeStruct(flat, BF16), jax.ShapeDtypeStruct(flat, BF16)),
        in_specs=[pl.BlockSpec(memory_space=pltpu.SMEM)] + any_specs(4),
        out_specs=tuple(vmem_specs(1) + any_specs(2)),
        scratch_shapes=[
            VMEM(q_rot.shape, BF16),
            VMEM(kv_new.shape, BF16),
            DMA((2,)),
            VMEM((SLOTS, ROWS_STEP, rows, HEAD), BF16),
            VMEM((SLOTS, ROWS_STEP, rows, HEAD), BF16),
            VMEM((batch * QPAD, HEAD), F32),
            VMEM((batch * QPAD, HEAD), BF16),
            VMEM((2, batch * 2, HEAD), F32),
            VMEM((batch * QPAD, HEAD), F32),
            VMEM((QPAD, rows), F32),
            VMEM((ROWS_STEP, QPAD, rows), F32),
            VMEM((ROWS_STEP, QPAD, rows), BF16),
            VMEM((ROWS_STEP, QPAD, HEAD), F32),
            DMA((2, SLOTS)),
            DMA((2, SLOTS)),
        ],
        compiler_params=pltpu.CompilerParams(vmem_limit_bytes=64 << 20),
    )(seq_lens, q_rot, kv_new, k_cache.reshape(flat), v_cache.reshape(flat))
    return out, k_out.reshape(k_cache.shape), v_out.reshape(v_cache.shape)


BLOCK = 256
RING = 36


def tail_kernel(gain_hbm, attn_hbm, x_hbm, wo_hbm, wg_hbm, wu_hbm, wd_hbm, out_hbm,
                out_ref, gain_ref, gain_sem, pool, full, rows_in, part, keep, recv_one, send_two, recv_two, x_own, mid, sq_send, sq_recv,
                h_rows, h_cols, gu_send, gu_recv, gu_own, act, early,
                pool_sems, x_sem, attn_sem, core_sems, rs_sems, ag_sems, gu_sems, act_sems):
    my = lax.axis_index("my")
    me = lax.axis_index("mx")
    peer = 1 - me
    side_x = my + 1 - 2 * lax.rem(my, 2)
    side_y = lax.rem(my + 2, 4)
    cross = 3 - my
    half, depth = attn_hbm.shape
    batch = 2 * half
    quarter = batch // 4
    hidden = x_hbm.shape[1]
    ff = wg_hbm.shape[0]
    col_chunks = hidden // BLOCK
    ff_chunks = pl.cdiv(ff, BLOCK)
    ff_rest = ff - (ff_chunks - 1) * BLOCK
    chunk_ring = RING // 2
    out_blocks = depth // BLOCK
    out_slot = RING - 6
    down_slot = RING - ff_chunks
    early_blocks = chunk_ring
    late_chunk = chunk_ring + chunk_ring // 2 - (down_slot // 2)
    late_count = ff_chunks - late_chunk

    def slot_rows(slot, count=BLOCK):
        return pl.ds(pl.multiple_of(slot * BLOCK, BLOCK), count)

    def block_copy(source, block, slot, count=BLOCK):
        return pltpu.make_async_copy(source.at[slot_rows(block, count)], pool.at[slot_rows(slot, count)], pool_sems.at[slot])

    def ff_slot(chunk):
        return 2 * jnp.where(chunk < chunk_ring, chunk, jnp.where(chunk < late_chunk, chunk - late_chunk + chunk_ring // 2, chunk - late_chunk))

    def ff_copies(chunk, count=BLOCK):
        slot = ff_slot(chunk)
        return block_copy(wg_hbm, chunk, slot, count), block_copy(wu_hbm, chunk, slot + 1, count)

    def down_copy(block, count=BLOCK):
        slot = down_slot + jnp.where(block < early_blocks, block + ff_chunks - early_blocks, block - early_blocks)
        return block_copy(wd_hbm, block, slot, count)

    def out_copy(block):
        return block_copy(wo_hbm, block, out_slot + block)

    def to_core(source, target, slot):
        return pltpu.make_async_remote_copy(src_ref=source, dst_ref=target, send_sem=slot[0], recv_sem=slot[1],
                                            device_id={"mx": peer}, device_id_type=MESH)

    def to_chip(source, target, chip, send_sem, recv_sem):
        return pltpu.make_async_remote_copy(src_ref=source, dst_ref=target, send_sem=send_sem, recv_sem=recv_sem,
                                            device_id={"my": chip}, device_id_type=MESH)

    own_half = pl.ds(pl.multiple_of(me * half, half), half)
    peer_half = pl.ds(pl.multiple_of(peer * half, half), half)
    attn_load = pltpu.make_async_copy(attn_hbm, full.at[own_half], attn_sem)
    attn_load.start()
    own_rows = pl.ds(pl.multiple_of(my * quarter, quarter), quarter)
    x_copy = pltpu.make_async_copy(x_hbm.at[own_rows], x_own, x_sem)
    x_copy.start()
    gain_copy = pltpu.make_async_copy(gain_hbm, gain_ref, gain_sem)
    gain_copy.start()

    barrier = pltpu.get_barrier_semaphore()
    pl.semaphore_signal(barrier, inc=1, device_id={"mx": peer}, device_id_type=MESH)
    pl.semaphore_signal(barrier, inc=1, device_id={"my": side_x}, device_id_type=MESH)
    pl.semaphore_signal(barrier, inc=1, device_id={"my": side_y}, device_id_type=MESH)
    attn_load.wait()
    for block in range(out_blocks):
        out_copy(block).start()
    pl.semaphore_wait(barrier, 3)
    attn_copy = to_core(full.at[own_half], full.at[own_half], (core_sems.at[0], core_sems.at[1]))
    attn_copy.start()
    attn_copy.wait()
    for place, owner in enumerate((my, side_x, cross, side_y)):
        rows_in[place * quarter:(place + 1) * quarter, :] = full[pl.ds(pl.multiple_of(owner * quarter, quarter), quarter), :]

    def columns(chunk):
        if isinstance(chunk, int):
            return slice(chunk * BLOCK, (chunk + 1) * BLOCK)
        return pl.ds(pl.multiple_of(chunk * BLOCK, BLOCK), BLOCK)

    def first_side(parity):
        return (side_x, side_y)[parity]

    def second_side(parity):
        return (side_y, side_x)[parity]

    def scatter_one(chunk, parity):
        return to_chip(part.at[chunk], recv_one.at[chunk], first_side(parity), rs_sems.at[0, 0, chunk], rs_sems.at[0, 1, chunk])

    def scatter_two(chunk, parity):
        return to_chip(send_two.at[chunk], recv_two.at[chunk], second_side(parity), rs_sems.at[1, 0, chunk], rs_sems.at[1, 1, chunk])

    def scatter_start(pair, total):
        for parity in range(2):
            chunk = 2 * pair + parity
            value = total[:, parity * BLOCK:(parity + 1) * BLOCK]
            lead = quarter * (1 + parity)
            part[chunk] = value[lead:lead + 2 * quarter].astype(BF16)
            keep[chunk, 0] = value[:quarter]
            other = 3 * quarter if parity == 0 else quarter
            keep[chunk, 1] = value[other:other + quarter]
        for parity in range(2):
            scatter_one(2 * pair + parity, parity).start()

    def scatter_pass(chunk, parity):
        scatter_one(chunk, parity).wait()
        mine = slice(0, quarter) if parity == 0 else slice(quarter, 2 * quarter)
        theirs = slice(quarter, 2 * quarter) if parity == 0 else slice(0, quarter)
        send_two[chunk] = (keep[chunk, 1] + recv_one[chunk, theirs, :].astype(F32)).astype(BF16)
        scatter_two(chunk, parity).start()
        keep[chunk, 0] = keep[chunk, 0] + recv_one[chunk, mine, :].astype(F32)

    def scatter_end(chunk, parity):
        scatter_two(chunk, parity).wait()
        return keep[chunk, 0] + recv_two[chunk].astype(F32)

    def mid_end(chunk):
        mid[:, columns(chunk)] = (x_own[:, columns(chunk)].astype(F32) + scatter_end(chunk, chunk % 2)).astype(BF16).astype(F32)

    x_copy.wait()
    gain_copy.wait()
    for block in range(out_blocks):
        out_copy(block).wait()
    for chunk in range(out_slot // 2):
        for copy in ff_copies(chunk):
            copy.start()
    def out_product(pair, carry):
        lanes = pl.ds(pl.multiple_of(pair * 2 * BLOCK, 2 * BLOCK), 2 * BLOCK)
        weights = pool[out_slot * BLOCK:out_slot * BLOCK + depth, lanes]
        scatter_start(pair, jnp.dot(rows_in[...], weights, preferred_element_type=F32))
        return carry

    lax.fori_loop(0, col_chunks // 2, out_product, 0)
    for chunk in range(out_slot // 2, chunk_ring):
        for copy in ff_copies(chunk):
            copy.start()
    for chunk in range(col_chunks + 3):
        if chunk < col_chunks:
            scatter_pass(chunk, chunk % 2)
        if chunk >= 3:
            mid_end(chunk - 3)

    square = jnp.zeros((quarter, HEAD), F32)
    for start in range(0, hidden, HEAD):
        square = square + mid[:, start:start + HEAD] * mid[:, start:start + HEAD]
    sq_send[...] = jnp.broadcast_to(jnp.sum(square, axis=1, keepdims=True), (quarter, HEAD))
    sq_copy = to_core(sq_send, sq_recv, (core_sems.at[2], core_sems.at[3]))
    sq_copy.start()
    sq_copy.wait()
    scale = lax.rsqrt((sq_send[...] + sq_recv[...]) / (2 * hidden) + NORM_EPS)

    def place_rows(place):
        return slice(place * quarter, (place + 1) * quarter)

    def gather_x(chunk):
        return to_chip(h_rows.at[place_rows(0), columns(chunk)], h_rows.at[place_rows(1), columns(chunk)], side_x,
                       ag_sems.at[0, 0, chunk], ag_sems.at[0, 1, chunk])

    def gather_y(chunk):
        return to_chip(h_rows.at[place_rows(0), columns(chunk)], h_rows.at[place_rows(3), columns(chunk)], side_y,
                       ag_sems.at[1, 0, chunk], ag_sems.at[1, 1, chunk])

    def gather_cross(chunk):
        source = 1 if chunk % 2 == 0 else 3
        return to_chip(h_rows.at[place_rows(source), columns(chunk)], h_rows.at[place_rows(2), columns(chunk)], second_side(chunk % 2),
                       ag_sems.at[2, 0, chunk], ag_sems.at[2, 1, chunk])

    gains = gain_ref[...].astype(F32)
    for chunk in range(col_chunks):
        for start in range(chunk * BLOCK, (chunk + 1) * BLOCK, HEAD):
            gain = gains[start // HEAD:start // HEAD + 1, :]
            h_rows[:quarter, start:start + HEAD] = (mid[:, start:start + HEAD] * scale * gain).astype(BF16)
        gather_x(chunk).start()
        gather_y(chunk).start()
    for chunk in range(col_chunks):
        (gather_x if chunk % 2 == 0 else gather_y)(chunk).wait_recv()
        gather_cross(chunk).start()

    for chunk in range(col_chunks):
        (gather_y if chunk % 2 == 0 else gather_x)(chunk).wait_recv()
        gather_cross(chunk).wait_recv()
        for place, source in enumerate((own_half, peer_half)):
            h_cols[columns(chunk), place * half:(place + 1) * half] = h_rows[source, columns(chunk)].astype(F32).T.astype(BF16)
        gather_x(chunk).wait_send()
        gather_y(chunk).wait_send()
        gather_cross(chunk).wait_send()

    def gu_copy(chunk):
        slot = lax.rem(chunk, 8)
        return to_core(gu_send.at[slot], gu_recv.at[slot], (gu_sems.at[0, slot], gu_sems.at[1, slot]))

    def act_lanes(chunk):
        place = jnp.where(chunk < early_blocks, chunk + ff_chunks - early_blocks, chunk - early_blocks)
        return pl.ds(pl.multiple_of(place * BLOCK, BLOCK), BLOCK)

    def act_copy(chunk):
        lanes = act_lanes(chunk)
        return to_core(act.at[own_half, lanes], act.at[own_half, lanes], (act_sems.at[0, lax.rem(chunk, 8)], act_sems.at[1, lax.rem(chunk, 8)]))

    def ff_products(chunk):
        slot = lax.rem(chunk, 8)
        base = ff_slot(chunk)
        product = jnp.dot(pool[slot_rows(base, 2 * BLOCK), :], h_cols[...], preferred_element_type=F32)
        for kind in range(2):
            rows = slice(kind * BLOCK, (kind + 1) * BLOCK)
            gu_own[slot, kind] = product[rows, :half]
            gu_send[slot, kind] = product[rows, half:].astype(BF16)

    def activate(chunk):
        slot = lax.rem(chunk, 8)
        gate = gu_own[slot, 0] + gu_recv[slot, 0].astype(F32)
        up = gu_own[slot, 1] + gu_recv[slot, 1].astype(F32)
        value = gate * jax.nn.sigmoid(gate) * up
        row = chunk * BLOCK + lax.broadcasted_iota(jnp.int32, value.shape, 0)
        value = jnp.where(row < ff, value, 0.0)
        lanes = act_lanes(chunk)
        act[own_half, lanes] = value.T.astype(BF16)

    def refill(chunk):
        half_ring = chunk_ring // 2

        @pl.when(chunk < late_count - 1)
        def _():
            for copy in ff_copies(late_chunk + chunk):
                copy.start()

        @pl.when(chunk == late_count - 1)
        def _():
            for copy in ff_copies(ff_chunks - 1, ff_rest):
                copy.start()

        @pl.when((chunk >= late_count) & (chunk < half_ring))
        def _():
            for copy in ff_copies(chunk - late_count + chunk_ring):
                copy.start()

        @pl.when((chunk >= half_ring) & (chunk < chunk_ring))
        def _():
            down_copy(2 * (chunk - half_ring)).start()
            down_copy(2 * (chunk - half_ring) + 1).start()

        free = 2 * (chunk - chunk_ring + late_count) - down_slot + early_blocks

        @pl.when((chunk >= chunk_ring) & (chunk < late_chunk) & (free >= early_blocks))
        def _():
            down_copy(free).start()

        @pl.when((chunk >= chunk_ring) & (chunk < late_chunk - 1))
        def _():
            down_copy(free + 1).start()

        @pl.when(chunk == late_chunk - 1)
        def _():
            down_copy(ff_chunks - 1, ff_rest).start()

    def ff_pair(pair, active):
        chunks = (2 * pair, 2 * pair + 1)
        if active:
            for chunk in chunks:
                gu_copy(chunk - 4).wait()
        for chunk in chunks:
            for copy in ff_copies(chunk):
                copy.wait()
        if active:
            for chunk in chunks:
                activate(chunk - 4)
        for chunk in chunks:
            ff_products(chunk)
        for chunk in chunks:
            gu_copy(chunk).start()
        if active:
            for chunk in chunks:
                act_copy(chunk - 4).start()
        for chunk in chunks:
            refill(chunk)

    def ff_first(pair, carry):
        ff_pair(pair, False)
        return carry

    def ff_step(pair, carry):
        @pl.when(pair >= 4)
        def _():
            for parity in range(2):
                act_copy(2 * (pair - 4) + parity).wait()
        ff_pair(pair, True)
        return carry

    last = ff_chunks - 1
    ff_pairs = last // 2
    lax.fori_loop(0, 2, ff_first, 0)
    lax.fori_loop(2, ff_pairs, ff_step, 0)

    def finish(chunk):
        gu_copy(chunk).wait()
        activate(chunk)
        act_copy(chunk).start()

    for chunk in range(2 * ff_pairs - 8, 2 * ff_pairs - 6):
        act_copy(chunk).wait()

    def ff_last(chunk, carry):
        for copy in ff_copies(chunk, ff_rest):
            copy.wait()
        ff_products(chunk)
        gu_copy(chunk).start()
        return carry

    lax.fori_loop(last, last + 1, ff_last, 0)
    for chunk in range(last - 4, last - 2):
        finish(chunk)
    for block in range(early_blocks):
        down_copy(block).wait()
    late_lanes = (ff_chunks - early_blocks) * BLOCK
    late_row = down_slot * BLOCK + late_lanes

    def pair_lanes(pair):
        return pl.ds(pl.multiple_of(pair * 2 * BLOCK, 2 * BLOCK), 2 * BLOCK)

    def down_early(pair, carry):
        early[pair] = jnp.dot(act[:, late_lanes:], pool[late_row:, pair_lanes(pair)], preferred_element_type=F32)
        return carry

    lax.fori_loop(0, 1, down_early, 0)
    for chunk in range(last - 2, ff_chunks):
        finish(chunk)
    lax.fori_loop(1, 2, down_early, 0)
    for block in range(early_blocks, ff_chunks):
        down_copy(block, ff_rest if block == last else BLOCK).wait()
    for chunk in range(2 * ff_pairs - 6, ff_chunks):
        act_copy(chunk).wait()

    def owner_rows(owner):
        return pl.ds(pl.multiple_of(owner * quarter, quarter), quarter)

    def final_x(chunk):
        block = out_ref.at[owner_rows(my), columns(chunk)]
        return to_chip(block, block, side_x, ag_sems.at[0, 0, chunk], ag_sems.at[0, 1, chunk])

    def final_y(chunk):
        block = out_ref.at[owner_rows(my), columns(chunk)]
        return to_chip(block, block, side_y, ag_sems.at[1, 0, chunk], ag_sems.at[1, 1, chunk])

    def final_cross(chunk):
        block = out_ref.at[owner_rows(first_side(chunk % 2)), columns(chunk)]
        return to_chip(block, block, second_side(chunk % 2), ag_sems.at[2, 0, chunk], ag_sems.at[2, 1, chunk])

    def save_out(chunk):
        return pltpu.make_async_copy(out_ref.at[:, columns(chunk)], out_hbm.at[:, columns(chunk)], pool_sems.at[chunk])

    def out_end(chunk):
        out_ref[owner_rows(my), columns(chunk)] = (mid[:, columns(chunk)] + scatter_end(chunk, chunk % 2)).astype(BF16)
        final_x(chunk).start()
        final_y(chunk).start()

    def out_pass(chunk):
        (final_x if chunk % 2 == 0 else final_y)(chunk).wait_recv()
        final_cross(chunk).start()

    def down_rest(pair, carry):
        total = jnp.dot(act[:, :late_lanes], pool[down_slot * BLOCK:late_row, pair_lanes(pair)], preferred_element_type=F32)
        scatter_start(pair, early[pair] + total)
        return carry

    def down_pair(pair, carry):
        scatter_start(pair, jnp.dot(act[...], pool[down_slot * BLOCK:, pair_lanes(pair)], preferred_element_type=F32))

        @pl.when(pair >= 2)
        def _():
            for parity in range(2):
                scatter_pass(2 * (pair - 2) + parity, parity)
        return carry

    pairs = col_chunks // 2
    lax.fori_loop(0, 2, down_rest, 0)
    lax.fori_loop(2, pairs, down_pair, 0)

    def each(step, pair):
        for chunk in (2 * pair, 2 * pair + 1):
            if step is scatter_pass:
                step(chunk, chunk % 2)
            else:
                step(chunk)

    each(out_end, 0)
    for pair in range(pairs - 2, pairs):
        each(scatter_pass, pair)
        each(out_end, pair - pairs + 3)
    each(out_pass, 0)
    for pair in range(3, pairs):
        each(out_end, pair)
        each(out_pass, pair - 2)
    for pair in range(pairs - 2, pairs):
        each(out_pass, pair)
    for chunk in range(col_chunks):
        (final_y if chunk % 2 == 0 else final_x)(chunk).wait_recv()
        final_cross(chunk).wait_recv()
        save_out(chunk).start()
    for chunk in range(col_chunks):
        final_cross(chunk).wait_send()
        final_x(chunk).wait_send()
        final_y(chunk).wait_send()
        save_out(chunk).wait()


def tail(attn_rows, gain, x_in, w_o, wg_rows, wu_rows, w_down):
    half, depth = attn_rows.shape
    rows, hidden = x_in.shape
    quarter = rows // 4
    chunks = hidden // BLOCK
    ff_chunks = pl.cdiv(w_down.shape[0], BLOCK)
    return pl.pallas_call(
        tail_kernel,
        name="tail",
        out_shape=jax.ShapeDtypeStruct((rows, hidden), BF16),
        in_specs=any_specs(7),
        out_specs=any_specs(1)[0],
        scratch_shapes=[
            VMEM((rows, hidden), BF16),
            VMEM((hidden // HEAD, HEAD), BF16),
            DMA,
            VMEM((RING * BLOCK, hidden), BF16),
            VMEM((rows, depth), BF16),
            VMEM((rows, depth), BF16),
            VMEM((chunks, 2 * quarter, BLOCK), BF16),
            VMEM((chunks, 2, quarter, BLOCK), F32),
            VMEM((chunks, 2 * quarter, BLOCK), BF16),
            VMEM((chunks, quarter, BLOCK), BF16),
            VMEM((chunks, quarter, BLOCK), BF16),
            VMEM((quarter, hidden), BF16),
            VMEM((quarter, hidden), F32),
            VMEM((quarter, HEAD), F32),
            VMEM((quarter, HEAD), F32),
            VMEM((rows, hidden), BF16),
            VMEM((hidden, rows), BF16),
            VMEM((8, 2, BLOCK, half), BF16),
            VMEM((8, 2, BLOCK, half), BF16),
            VMEM((8, 2, BLOCK, half), F32),
            VMEM((rows, ff_chunks * BLOCK), BF16),
            VMEM((2, rows, 2 * BLOCK), F32),
            DMA((RING,)),
            DMA,
            DMA,
            DMA((4,)),
            DMA((2, 2, chunks)),
            DMA((3, 2, chunks)),
            DMA((2, 8)),
            DMA((2, 8)),
        ],
        compiler_params=pltpu.CompilerParams(collective_id=1, has_side_effects=True, vmem_limit_bytes=67043328),
    )(lane_rows(gain), attn_rows, x_in, w_o, wg_rows, wu_rows, w_down)


def solution(mesh):
    act_spec = P(None, "mx")
    cache_spec = P("mx", None, "my", None)
    in_specs = (act_spec, P("mx"), P("mx"), P("mx"), P("mx", "my"), P("my"), P("mx", "my"), P("my"), P("mx", "my"), P("my"), P("my", "mx"), P("mx", "my"), P("mx", "my"), P("my", "mx"), cache_spec, cache_spec)
    out_specs = (act_spec, cache_spec, cache_spec)

    def local_layer(x_in, seq_lens, gain_attn, gain_mlp, w_q, b_q, w_k, b_k, w_v, b_v, w_o, w_gate, w_up, w_down, k_cache, v_cache):
        q_rot, kv_new = project(x_in, seq_lens, gain_attn, b_q, b_k, b_v, w_q, w_k, w_v)
        attn_rows, k_cache_out, v_cache_out = attend(seq_lens, q_rot, kv_new, k_cache, v_cache)
        x_out = tail(attn_rows, gain_mlp, x_in, w_o, w_gate.T, w_up.T, w_down)
        return x_out, k_cache_out, v_cache_out

    return jax.shard_map(local_layer, mesh=mesh, in_specs=in_specs, out_specs=out_specs, check_vma=False)
```

```python
import jax
import jax.numpy as jnp
import numpy as np
from jax import lax
from jax.experimental import pallas as pl
from jax.experimental.pallas import tpu as pltpu
from jax.sharding import PartitionSpec as P

HEAD = 128
NORM_EPS = 1e-6
ROPE_THETA = 1000000.0
MESH = pl.DeviceIdType.MESH
F32 = jnp.float32
BF16 = jnp.bfloat16
QPAD = 16
VMEM = pltpu.VMEM
DMA = pltpu.SemaphoreType.DMA


def any_specs(count):
    return [pl.BlockSpec(memory_space=pl.ANY)] * count


def vmem_specs(count):
    return [pl.BlockSpec(memory_space=pltpu.VMEM)] * count


def lane_rows(vector):
    return vector.reshape(-1, HEAD)


def rotary_frequencies():
    half_dim = HEAD // 2
    inv_freq = np.float32(ROPE_THETA) ** (np.float32(-2.0) * np.arange(half_dim, dtype=np.float32) / np.float32(HEAD))
    return jnp.asarray(np.concatenate([inv_freq, inv_freq])[None, :], F32)


def project_kernel(gain_hbm, bq_hbm, bk_hbm, bv_hbm, lens_hbm, freq_hbm, x_hbm, wq_hbm, wk_hbm, wv_hbm, q_out, kv_out,
                   gain_ref, bq_ref, bk_ref, bv_ref, lens_ref, freq_ref, small_sems, x_ref, x_sem, w_buf, normed, sq_send, sq_recv, part_send, part_recv, part_own, w_sems, send_sems, recv_sems):
    me = lax.axis_index("mx")
    peer = 1 - me
    rows, depth = x_hbm.shape
    half = rows // 2
    width = 2 * HEAD
    q_chunks = wq_hbm.shape[1] // width
    chunks = q_chunks + 2

    def weight_copy(index):
        if index < q_chunks:
            source = wq_hbm.at[:, pl.ds(index * width, width)]
        else:
            source = (wk_hbm, wv_hbm)[index - q_chunks]
        return pltpu.make_async_copy(source, w_buf.at[:, pl.ds(index * width, width)], w_sems.at[index])

    def weight_wait(index):
        lanes = pl.ds(pl.multiple_of(index * width, width), width)
        pltpu.make_async_copy(wk_hbm, w_buf.at[:, lanes], w_sems.at[index]).wait()

    smalls = [pltpu.make_async_copy(source, target, small_sems.at[slot]) for slot, (source, target) in enumerate((
        (lens_hbm, lens_ref), (freq_hbm, freq_ref), (gain_hbm, gain_ref), (bq_hbm, bq_ref), (bk_hbm, bk_ref), (bv_hbm, bv_ref)))]
    for copy in smalls:
        copy.start()
    x_copy = pltpu.make_async_copy(x_hbm, x_ref, x_sem)
    x_copy.start()
    barrier = pltpu.get_barrier_semaphore()
    pl.semaphore_signal(barrier, inc=1, device_id={"mx": peer}, device_id_type=MESH)

    for copy in smalls:
        copy.wait()
    positions = jnp.broadcast_to(lens_ref[...].astype(F32), (half, half)).T
    angles = positions * freq_ref[...]
    cos_tab = jnp.cos(angles)
    lane = lax.broadcasted_iota(jnp.int32, (half, HEAD), 1)
    sin_tab = jnp.where(lane < HEAD // 2, -1.0, 1.0) * jnp.sin(angles)

    x_copy.wait()
    for index in range(chunks):
        weight_copy(index).start()
    total = jnp.zeros((rows, HEAD), F32)
    for start in range(0, depth, HEAD):
        block = x_ref[:, start:start + HEAD].astype(F32)
        total = total + block * block
    sq_own = jnp.sum(total, axis=1, keepdims=True)
    sq_send[...] = jnp.broadcast_to(sq_own, (rows, HEAD))
    pl.semaphore_wait(barrier, 1)

    def remote(source, target, slot):
        return pltpu.make_async_remote_copy(
            src_ref=source, dst_ref=target, send_sem=send_sems.at[slot], recv_sem=recv_sems.at[slot],
            device_id={"mx": peer}, device_id_type=MESH)

    sq_copy = remote(sq_send, sq_recv, chunks)
    sq_copy.start()
    sq_copy.wait()
    own_rows = pl.ds(pl.multiple_of(me * half, half), half)
    peer_rows = pl.ds(pl.multiple_of(peer * half, half), half)
    scale = lax.rsqrt((sq_send[...] + sq_recv[...]) / (2 * depth) + NORM_EPS)
    gains = gain_ref[...].astype(F32)
    for start in range(0, depth, HEAD):
        block = x_ref[:, start:start + HEAD].astype(F32)
        gain = gains[start // HEAD:start // HEAD + 1, :]
        value = (block * scale * gain).astype(BF16)
        normed[own_rows, start:start + HEAD] = value[:half]
        normed[peer_rows, start:start + HEAD] = value[half:]

    def part_copy(index):
        return remote(part_send.at[index], part_recv.at[index], index)

    def multiply(first, count):
        for index in range(count):
            weight_wait(first + index)
        lanes = pl.ds(pl.multiple_of(first * width, width), count * width)
        product = jnp.dot(normed[...], w_buf[:, lanes], preferred_element_type=F32)
        for index in range(count):
            value = product[:, index * width:(index + 1) * width]
            part_own[first + index] = value[:half]
            part_send[first + index] = value[half:].astype(BF16)
        for index in range(count):
            part_copy(first + index).start()

    def multiply_pair(pair, carry):
        multiply(2 * pair, 2)
        return carry

    def multiply_last(index, carry):
        multiply(index, 1)
        return carry

    lax.fori_loop(0, chunks // 2, multiply_pair, 0)
    lax.fori_loop(chunks - chunks % 2, chunks, multiply_last, 0)
    biases = [ref[...].astype(F32) for ref in (bq_ref, bk_ref, bv_ref)]
    for index in range(chunks):
        part_copy(index).wait()
        for head in range(2):
            lanes = slice(head * HEAD, (head + 1) * HEAD)
            columns = slice(index * width + head * HEAD, index * width + (head + 1) * HEAD)
            if index < q_chunks:
                bias = biases[0][2 * index + head:2 * index + head + 1, :]
            else:
                bias = biases[index - q_chunks + 1][head:head + 1, :]
            value = part_own[index][:, lanes] + part_recv[index][:, lanes].astype(F32) + bias
            if index < chunks - 1:
                value = value * cos_tab + pltpu.roll(value, HEAD // 2, 1) * sin_tab
            if index < q_chunks:
                q_out[:, columns] = value.astype(BF16)
            else:
                kv_out[:, (index - q_chunks) * width + head * HEAD:(index - q_chunks) * width + (head + 1) * HEAD] = value.astype(BF16)


def project(x_in, seq_lens, gain, b_q, b_k, b_v, w_q, w_k, w_v):
    rows, depth = x_in.shape
    half = rows // 2
    width = 2 * HEAD
    chunks = w_q.shape[1] // width + 2
    return pl.pallas_call(
        project_kernel,
        name="project",
        out_shape=(jax.ShapeDtypeStruct((half, w_q.shape[1]), BF16), jax.ShapeDtypeStruct((half, 2 * width), BF16)),
        in_specs=any_specs(10),
        out_specs=tuple(vmem_specs(2)),
        scratch_shapes=[
            VMEM((depth // HEAD, HEAD), BF16),
            VMEM((w_q.shape[1] // HEAD, HEAD), BF16),
            VMEM((2, HEAD), BF16),
            VMEM((2, HEAD), BF16),
            VMEM((1, half), jnp.int32),
            VMEM((1, HEAD), F32),
            DMA((6,)),
            VMEM((rows, depth), BF16),
            DMA,
            VMEM((depth, chunks * width), BF16),
            VMEM((rows, depth), BF16),
            VMEM((rows, HEAD), F32),
            VMEM((rows, HEAD), F32),
            VMEM((chunks, half, width), BF16),
            VMEM((chunks, half, width), BF16),
            VMEM((chunks, half, width), F32),
            DMA((chunks,)),
            DMA((chunks + 1,)),
            DMA((chunks + 1,)),
        ],
        compiler_params=pltpu.CompilerParams(collective_id=0, has_side_effects=True, vmem_limit_bytes=67043328),
    )(lane_rows(gain), lane_rows(b_q), lane_rows(b_k), lane_rows(b_v), seq_lens[None, :], rotary_frequencies(), x_in, w_q, w_k, w_v)


SLOTS = 6
ROWS_STEP = 8


def attend_kernel(lens_ref, q_hbm, kv_hbm, k_hbm, v_hbm, o_ref, k_out, v_out,
                  q_ref, kv_ref, small_sems, k_buf, v_buf, q_wide, q_packed, kv_wide, o_wide, parity, scores, weights, sums, in_sems, out_sems):
    batch, kv_rows, _ = k_hbm.shape
    q_heads = q_hbm.shape[1] // HEAD
    group = q_heads // 2
    steps = batch // ROWS_STEP

    def load(step, kind):
        slot = lax.rem(step, SLOTS)
        source, target = ((k_hbm, k_buf), (v_hbm, v_buf))[kind]
        return pltpu.make_async_copy(source.at[pl.ds(step * ROWS_STEP, ROWS_STEP)], target.at[slot], in_sems.at[kind, slot])

    def save(step, kind):
        slot = lax.rem(step, SLOTS)
        source, target = ((k_buf, k_out), (v_buf, v_out))[kind]
        return pltpu.make_async_copy(source.at[slot], target.at[pl.ds(step * ROWS_STEP, ROWS_STEP)], out_sems.at[kind, slot])

    q_copy = pltpu.make_async_copy(q_hbm, q_ref, small_sems.at[0])
    kv_copy = pltpu.make_async_copy(kv_hbm, kv_ref, small_sems.at[1])
    q_copy.start()
    kv_copy.start()
    for kind in range(2):
        load(0, kind).start()

    q_wide[...] = jnp.zeros_like(q_wide)
    q_copy.wait()
    kv_copy.wait()
    for step in range(1, 3):
        for kind in range(2):
            load(step, kind).start()
    for head in range(q_heads):
        q_wide[pl.ds(head, batch, stride=QPAD), :] = q_ref[:, head * HEAD:(head + 1) * HEAD].astype(F32)
    q_packed[...] = q_wide[...].astype(BF16)
    for kind in range(2):
        for head in range(2):
            start = (kind * 2 + head) * HEAD
            kv_wide[kind, pl.ds(head, batch, stride=2), :] = kv_ref[:, start:start + HEAD].astype(F32)
    row_head = lax.broadcasted_iota(jnp.int32, (QPAD, kv_rows), 0) >= group
    col_head = lax.rem(lax.broadcasted_iota(jnp.int32, (QPAD, kv_rows), 1), 2) == 1
    parity[...] = jnp.where(row_head == col_head, 0.0, -jnp.inf)
    columns = lax.broadcasted_iota(jnp.int32, (QPAD, kv_rows), 1)
    tile_row = lax.broadcasted_iota(jnp.int32, (16, HEAD), 0)
    tile_pos = lax.div(tile_row, 2)
    tile_odd = lax.rem(tile_row, 2) == 1

    def body(step, carry):
        slot = lax.rem(step, SLOTS)

        @pl.when(step + 3 < steps)
        def _():
            @pl.when(step >= 3)
            def _():
                for kind in range(2):
                    save(step - 3, kind).wait()
            for kind in range(2):
                load(step + 3, kind).start()

        for kind in range(2):
            load(step, kind).wait()
        for row in range(ROWS_STEP):
            index = step * ROWS_STEP + row
            position = lens_ref[index]
            base = pl.multiple_of(lax.div(position, 8) * 16, 16)
            offset = lax.rem(position, 8)
            for kind, buffer in ((0, k_buf), (1, v_buf)):
                low = kv_wide[kind, pl.ds(2 * index, 1), :]
                high = kv_wide[kind, pl.ds(2 * index + 1, 1), :]
                fresh = jnp.where(tile_odd, high, low).astype(BF16)
                tile = buffer[slot, row, pl.ds(base, 16), :]
                buffer[slot, row, pl.ds(base, 16), :] = jnp.where(tile_pos == offset, fresh, tile)
        for row in range(ROWS_STEP):
            q_start = pl.multiple_of((step * ROWS_STEP + row) * QPAD, QPAD)
            scores[row] = lax.dot_general(q_packed[pl.ds(q_start, QPAD), :], k_buf[slot, row], (((1,), (1,)), ((), ())),
                                          preferred_element_type=F32)
        for kind in range(2):
            save(step, kind).start()
        for row in range(ROWS_STEP):
            limit = 2 * lens_ref[step * ROWS_STEP + row] + 2
            masked = jnp.where(columns < limit, scores[row] * HEAD ** -0.5 + parity[...], -jnp.inf)
            weight = jnp.exp(masked - jnp.max(masked, axis=1, keepdims=True))
            sums[row] = jnp.broadcast_to(jnp.sum(weight, axis=1, keepdims=True), (QPAD, HEAD))
            weights[row] = weight.astype(BF16)
        for row in range(ROWS_STEP):
            q_start = pl.multiple_of((step * ROWS_STEP + row) * QPAD, QPAD)
            mixed = jnp.dot(weights[row], v_buf[slot, row], preferred_element_type=F32)
            o_wide[pl.ds(q_start, QPAD), :] = mixed / sums[row]
        return carry

    lax.fori_loop(0, steps, body, 0)
    for head in range(q_heads):
        o_ref[:, head * HEAD:(head + 1) * HEAD] = o_wide[pl.ds(head, batch, stride=QPAD), :].astype(BF16)
    for step in range(steps - SLOTS, steps):
        for kind in range(2):
            save(step, kind).wait()


def attend(seq_lens, q_rot, kv_new, k_cache, v_cache):
    batch, seq_len, kv_heads, _ = k_cache.shape
    rows = seq_len * kv_heads
    flat = (batch, rows, HEAD)
    out, k_out, v_out = pl.pallas_call(
        attend_kernel,
        name="attend",
        out_shape=(jax.ShapeDtypeStruct(q_rot.shape, BF16), jax.ShapeDtypeStruct(flat, BF16), jax.ShapeDtypeStruct(flat, BF16)),
        in_specs=[pl.BlockSpec(memory_space=pltpu.SMEM)] + any_specs(4),
        out_specs=tuple(vmem_specs(1) + any_specs(2)),
        scratch_shapes=[
            VMEM(q_rot.shape, BF16),
            VMEM(kv_new.shape, BF16),
            DMA((2,)),
            VMEM((SLOTS, ROWS_STEP, rows, HEAD), BF16),
            VMEM((SLOTS, ROWS_STEP, rows, HEAD), BF16),
            VMEM((batch * QPAD, HEAD), F32),
            VMEM((batch * QPAD, HEAD), BF16),
            VMEM((2, batch * 2, HEAD), F32),
            VMEM((batch * QPAD, HEAD), F32),
            VMEM((QPAD, rows), F32),
            VMEM((ROWS_STEP, QPAD, rows), F32),
            VMEM((ROWS_STEP, QPAD, rows), BF16),
            VMEM((ROWS_STEP, QPAD, HEAD), F32),
            DMA((2, SLOTS)),
            DMA((2, SLOTS)),
        ],
        compiler_params=pltpu.CompilerParams(vmem_limit_bytes=64 << 20),
    )(seq_lens, q_rot, kv_new, k_cache.reshape(flat), v_cache.reshape(flat))
    return out, k_out.reshape(k_cache.shape), v_out.reshape(v_cache.shape)


BLOCK = 256
RING = 36


def tail_kernel(gain_hbm, attn_hbm, x_hbm, wo_hbm, wg_hbm, wu_hbm, wd_hbm, out_ref,
                gain_ref, gain_sem, pool, part, keep, recv_one, send_two, recv_two, x_own, mid, sq_send, sq_recv,
                h_rows, h_cols, gu_send, gu_recv, gu_own, act,
                pool_sems, x_sem, attn_sem, core_sems, rs_sems, ag_sems, gu_sems, act_sems):
    my = lax.axis_index("my")
    me = lax.axis_index("mx")
    peer = 1 - me
    side_x = my + 1 - 2 * lax.rem(my, 2)
    side_y = lax.rem(my + 2, 4)
    cross = 3 - my
    half, depth = attn_hbm.shape
    batch = 2 * half
    quarter = batch // 4
    hidden = x_hbm.shape[1]
    ff = wg_hbm.shape[0]
    col_chunks = hidden // BLOCK
    ff_chunks = pl.cdiv(ff, BLOCK)
    ff_rest = ff - (ff_chunks - 1) * BLOCK
    chunk_ring = RING // 2
    out_blocks = depth // BLOCK
    out_slot = RING - 6
    down_slot = RING - ff_chunks
    early_blocks = chunk_ring
    late_chunk = chunk_ring + chunk_ring // 2 - (down_slot // 2)
    late_count = ff_chunks - late_chunk

    def slot_rows(slot, count=BLOCK):
        return pl.ds(pl.multiple_of(slot * BLOCK, BLOCK), count)

    def block_copy(source, block, slot, count=BLOCK):
        return pltpu.make_async_copy(source.at[slot_rows(block, count)], pool.at[slot_rows(slot, count)], pool_sems.at[slot])

    def ff_slot(chunk):
        return 2 * jnp.where(chunk < chunk_ring, chunk, jnp.where(chunk < late_chunk, chunk - late_chunk + chunk_ring // 2, chunk - late_chunk))

    def ff_copies(chunk, count=BLOCK):
        slot = ff_slot(chunk)
        return block_copy(wg_hbm, chunk, slot, count), block_copy(wu_hbm, chunk, slot + 1, count)

    def down_copy(block, count=BLOCK):
        slot = down_slot + jnp.where(block < early_blocks, block + ff_chunks - early_blocks, block - early_blocks)
        return block_copy(wd_hbm, block, slot, count)

    def out_copy(block):
        return block_copy(wo_hbm, block, out_slot + block)

    def to_core(source, target, slot):
        return pltpu.make_async_remote_copy(src_ref=source, dst_ref=target, send_sem=slot[0], recv_sem=slot[1],
                                            device_id={"mx": peer}, device_id_type=MESH)

    def to_chip(source, target, chip, send_sem, recv_sem):
        return pltpu.make_async_remote_copy(src_ref=source, dst_ref=target, send_sem=send_sem, recv_sem=recv_sem,
                                            device_id={"my": chip}, device_id_type=MESH)

    own_half = pl.ds(pl.multiple_of(me * half, half), half)
    peer_half = pl.ds(pl.multiple_of(peer * half, half), half)
    rows_in = h_rows.at[:, pl.ds(0, depth)]
    full = h_rows.at[:, pl.ds(depth, depth)]
    attn_load = pltpu.make_async_copy(attn_hbm, full.at[own_half], attn_sem)
    attn_load.start()
    own_rows = pl.ds(pl.multiple_of(my * quarter, quarter), quarter)
    x_copy = pltpu.make_async_copy(x_hbm.at[own_rows], x_own, x_sem)
    x_copy.start()
    gain_copy = pltpu.make_async_copy(gain_hbm, gain_ref, gain_sem)
    gain_copy.start()

    barrier = pltpu.get_barrier_semaphore()
    pl.semaphore_signal(barrier, inc=1, device_id={"mx": peer}, device_id_type=MESH)
    pl.semaphore_signal(barrier, inc=1, device_id={"my": side_x}, device_id_type=MESH)
    pl.semaphore_signal(barrier, inc=1, device_id={"my": side_y}, device_id_type=MESH)
    attn_load.wait()
    for block in range(out_blocks):
        out_copy(block).start()
    pl.semaphore_wait(barrier, 3)
    attn_copy = to_core(full.at[own_half], full.at[own_half], (core_sems.at[0], core_sems.at[1]))
    attn_copy.start()
    attn_copy.wait()
    for place, owner in enumerate((my, side_x, cross, side_y)):
        rows_in[place * quarter:(place + 1) * quarter, :] = full[pl.ds(pl.multiple_of(owner * quarter, quarter), quarter), :]

    def columns(chunk):
        if isinstance(chunk, int):
            return slice(chunk * BLOCK, (chunk + 1) * BLOCK)
        return pl.ds(pl.multiple_of(chunk * BLOCK, BLOCK), BLOCK)

    def first_side(parity):
        return (side_x, side_y)[parity]

    def second_side(parity):
        return (side_y, side_x)[parity]

    def scatter_one(chunk, parity):
        return to_chip(part.at[chunk], recv_one.at[chunk], first_side(parity), rs_sems.at[0, 0, chunk], rs_sems.at[0, 1, chunk])

    def scatter_two(chunk, parity):
        return to_chip(send_two.at[chunk], recv_two.at[chunk], second_side(parity), rs_sems.at[1, 0, chunk], rs_sems.at[1, 1, chunk])

    def scatter_start(pair, total):
        for parity in range(2):
            chunk = 2 * pair + parity
            value = total[:, parity * BLOCK:(parity + 1) * BLOCK]
            lead = quarter * (1 + parity)
            part[chunk] = value[lead:lead + 2 * quarter].astype(BF16)
            keep[chunk, 0] = value[:quarter]
            other = 3 * quarter if parity == 0 else quarter
            keep[chunk, 1] = value[other:other + quarter]
        for parity in range(2):
            scatter_one(2 * pair + parity, parity).start()

    def scatter_pass(chunk, parity):
        scatter_one(chunk, parity).wait()
        mine = slice(0, quarter) if parity == 0 else slice(quarter, 2 * quarter)
        theirs = slice(quarter, 2 * quarter) if parity == 0 else slice(0, quarter)
        send_two[chunk] = (keep[chunk, 1] + recv_one[chunk, theirs, :].astype(F32)).astype(BF16)
        scatter_two(chunk, parity).start()
        keep[chunk, 0] = keep[chunk, 0] + recv_one[chunk, mine, :].astype(F32)

    def scatter_end(chunk, parity):
        scatter_two(chunk, parity).wait()
        return keep[chunk, 0] + recv_two[chunk].astype(F32)

    def mid_end(chunk):
        mid[:, columns(chunk)] = (x_own[:, columns(chunk)].astype(F32) + scatter_end(chunk, chunk % 2)).astype(BF16).astype(F32)

    x_copy.wait()
    gain_copy.wait()
    for block in range(out_blocks):
        out_copy(block).wait()
    for chunk in range(out_slot // 2):
        for copy in ff_copies(chunk):
            copy.start()
    def out_product(pair, carry):
        lanes = pl.ds(pl.multiple_of(pair * 2 * BLOCK, 2 * BLOCK), 2 * BLOCK)
        weights = pool[out_slot * BLOCK:out_slot * BLOCK + depth, lanes]
        scatter_start(pair, jnp.dot(rows_in[...], weights, preferred_element_type=F32))
        return carry

    lax.fori_loop(0, col_chunks // 2, out_product, 0)
    for chunk in range(out_slot // 2, chunk_ring):
        for copy in ff_copies(chunk):
            copy.start()
    for chunk in range(col_chunks + 3):
        if chunk < col_chunks:
            scatter_pass(chunk, chunk % 2)
        if chunk >= 3:
            mid_end(chunk - 3)

    square = jnp.zeros((quarter, HEAD), F32)
    for start in range(0, hidden, HEAD):
        square = square + mid[:, start:start + HEAD] * mid[:, start:start + HEAD]
    sq_send[...] = jnp.broadcast_to(jnp.sum(square, axis=1, keepdims=True), (quarter, HEAD))
    sq_copy = to_core(sq_send, sq_recv, (core_sems.at[2], core_sems.at[3]))
    sq_copy.start()
    sq_copy.wait()
    scale = lax.rsqrt((sq_send[...] + sq_recv[...]) / (2 * hidden) + NORM_EPS)

    def place_rows(place):
        return slice(place * quarter, (place + 1) * quarter)

    def gather_x(chunk):
        return to_chip(h_rows.at[place_rows(0), columns(chunk)], h_rows.at[place_rows(1), columns(chunk)], side_x,
                       ag_sems.at[0, 0, chunk], ag_sems.at[0, 1, chunk])

    def gather_y(chunk):
        return to_chip(h_rows.at[place_rows(0), columns(chunk)], h_rows.at[place_rows(3), columns(chunk)], side_y,
                       ag_sems.at[1, 0, chunk], ag_sems.at[1, 1, chunk])

    def gather_cross(chunk):
        source = 1 if chunk % 2 == 0 else 3
        return to_chip(h_rows.at[place_rows(source), columns(chunk)], h_rows.at[place_rows(2), columns(chunk)], second_side(chunk % 2),
                       ag_sems.at[2, 0, chunk], ag_sems.at[2, 1, chunk])

    gains = gain_ref[...].astype(F32)
    for chunk in range(col_chunks):
        for start in range(chunk * BLOCK, (chunk + 1) * BLOCK, HEAD):
            gain = gains[start // HEAD:start // HEAD + 1, :]
            h_rows[:quarter, start:start + HEAD] = (mid[:, start:start + HEAD] * scale * gain).astype(BF16)
        gather_x(chunk).start()
        gather_y(chunk).start()
    for chunk in range(col_chunks):
        (gather_x if chunk % 2 == 0 else gather_y)(chunk).wait_recv()
        gather_cross(chunk).start()

    for chunk in range(col_chunks):
        (gather_y if chunk % 2 == 0 else gather_x)(chunk).wait_recv()
        gather_cross(chunk).wait_recv()
        for place, source in enumerate((own_half, peer_half)):
            h_cols[columns(chunk), place * half:(place + 1) * half] = h_rows[source, columns(chunk)].astype(F32).T.astype(BF16)
        gather_x(chunk).wait_send()
        gather_y(chunk).wait_send()
        gather_cross(chunk).wait_send()

    def gu_copy(chunk):
        slot = lax.rem(chunk, 8)
        return to_core(gu_send.at[slot], gu_recv.at[slot], (gu_sems.at[0, slot], gu_sems.at[1, slot]))

    def act_lanes(chunk):
        place = jnp.where(chunk < early_blocks, chunk + ff_chunks - early_blocks, chunk - early_blocks)
        return pl.ds(pl.multiple_of(place * BLOCK, BLOCK), BLOCK)

    def act_copy(chunk):
        lanes = act_lanes(chunk)
        return to_core(act.at[own_half, lanes], act.at[own_half, lanes], (act_sems.at[0, lax.rem(chunk, 8)], act_sems.at[1, lax.rem(chunk, 8)]))

    def ff_products(chunk):
        slot = lax.rem(chunk, 8)
        base = ff_slot(chunk)
        product = jnp.dot(pool[slot_rows(base, 2 * BLOCK), :], h_cols[...], preferred_element_type=F32)
        for kind in range(2):
            rows = slice(kind * BLOCK, (kind + 1) * BLOCK)
            gu_own[slot, kind] = product[rows, :half]
            gu_send[slot, kind] = product[rows, half:].astype(BF16)

    def activate(chunk):
        slot = lax.rem(chunk, 8)
        gate = gu_own[slot, 0] + gu_recv[slot, 0].astype(F32)
        up = gu_own[slot, 1] + gu_recv[slot, 1].astype(F32)
        value = gate * jax.nn.sigmoid(gate) * up
        row = chunk * BLOCK + lax.broadcasted_iota(jnp.int32, value.shape, 0)
        value = jnp.where(row < ff, value, 0.0)
        lanes = act_lanes(chunk)
        act[own_half, lanes] = value.T.astype(BF16)

    def refill(chunk):
        half_ring = chunk_ring // 2

        @pl.when(chunk < late_count - 1)
        def _():
            for copy in ff_copies(late_chunk + chunk):
                copy.start()

        @pl.when(chunk == late_count - 1)
        def _():
            for copy in ff_copies(ff_chunks - 1, ff_rest):
                copy.start()

        @pl.when((chunk >= late_count) & (chunk < half_ring))
        def _():
            for copy in ff_copies(chunk - late_count + chunk_ring):
                copy.start()

        @pl.when((chunk >= half_ring) & (chunk < chunk_ring))
        def _():
            down_copy(2 * (chunk - half_ring)).start()
            down_copy(2 * (chunk - half_ring) + 1).start()

        free = 2 * (chunk - chunk_ring + late_count) - down_slot + early_blocks

        @pl.when((chunk >= chunk_ring) & (chunk < late_chunk) & (free >= early_blocks))
        def _():
            down_copy(free).start()

        @pl.when((chunk >= chunk_ring) & (chunk < late_chunk - 1))
        def _():
            down_copy(free + 1).start()

        @pl.when(chunk == late_chunk - 1)
        def _():
            down_copy(ff_chunks - 1, ff_rest).start()

    def ff_pair(pair, active):
        chunks = (2 * pair, 2 * pair + 1)
        if active:
            for chunk in chunks:
                gu_copy(chunk - 4).wait()
        for chunk in chunks:
            for copy in ff_copies(chunk):
                copy.wait()
        if active:
            for chunk in chunks:
                activate(chunk - 4)
        for chunk in chunks:
            ff_products(chunk)
        for chunk in chunks:
            gu_copy(chunk).start()
        if active:
            for chunk in chunks:
                act_copy(chunk - 4).start()
        for chunk in chunks:
            refill(chunk)

    def ff_first(pair, carry):
        ff_pair(pair, False)
        return carry

    def ff_step(pair, carry):
        @pl.when(pair >= 4)
        def _():
            for parity in range(2):
                act_copy(2 * (pair - 4) + parity).wait()
        ff_pair(pair, True)
        return carry

    last = ff_chunks - 1
    ff_pairs = last // 2
    lax.fori_loop(0, 2, ff_first, 0)
    lax.fori_loop(2, ff_pairs, ff_step, 0)

    def finish(chunk):
        gu_copy(chunk).wait()
        activate(chunk)
        act_copy(chunk).start()

    for chunk in range(2 * ff_pairs - 8, 2 * ff_pairs - 6):
        act_copy(chunk).wait()

    def ff_last(chunk, carry):
        for copy in ff_copies(chunk, ff_rest):
            copy.wait()
        ff_products(chunk)
        gu_copy(chunk).start()
        return carry

    lax.fori_loop(last, last + 1, ff_last, 0)
    for chunk in range(last - 4, last - 2):
        finish(chunk)
    for block in range(early_blocks):
        down_copy(block).wait()
    late_lanes = (ff_chunks - early_blocks) * BLOCK
    late_row = down_slot * BLOCK + late_lanes

    def pair_lanes(pair):
        return pl.ds(pl.multiple_of(pair * 2 * BLOCK, 2 * BLOCK), 2 * BLOCK)

    early_slot = 3

    def down_early(pair, carry):
        value = jnp.dot(act[:, late_lanes:], pool[late_row:, pair_lanes(pair)], preferred_element_type=F32)
        for piece in range(4):
            gu_own[early_slot + 2 * pair + piece // 2, piece % 2] = value[:, piece * half:(piece + 1) * half]
        return carry

    lax.fori_loop(0, 1, down_early, 0)
    for chunk in range(last - 2, ff_chunks):
        finish(chunk)
    lax.fori_loop(1, 2, down_early, 0)
    for block in range(early_blocks, ff_chunks):
        down_copy(block, ff_rest if block == last else BLOCK).wait()
    for chunk in range(2 * ff_pairs - 6, ff_chunks):
        act_copy(chunk).wait()

    def owner_rows(owner):
        return pl.ds(pl.multiple_of(owner * quarter, quarter), quarter)

    def final_x(chunk):
        block = out_ref.at[owner_rows(my), columns(chunk)]
        return to_chip(block, block, side_x, ag_sems.at[0, 0, chunk], ag_sems.at[0, 1, chunk])

    def final_y(chunk):
        block = out_ref.at[owner_rows(my), columns(chunk)]
        return to_chip(block, block, side_y, ag_sems.at[1, 0, chunk], ag_sems.at[1, 1, chunk])

    def final_cross(chunk):
        block = out_ref.at[owner_rows(first_side(chunk % 2)), columns(chunk)]
        return to_chip(block, block, second_side(chunk % 2), ag_sems.at[2, 0, chunk], ag_sems.at[2, 1, chunk])

    def out_end(chunk):
        out_ref[owner_rows(my), columns(chunk)] = (mid[:, columns(chunk)] + scatter_end(chunk, chunk % 2)).astype(BF16)
        final_x(chunk).start()
        final_y(chunk).start()

    def out_pass(chunk):
        (final_x if chunk % 2 == 0 else final_y)(chunk).wait_recv()
        final_cross(chunk).start()

    def down_rest(pair, carry):
        total = jnp.dot(act[:, :late_lanes], pool[down_slot * BLOCK:late_row, pair_lanes(pair)], preferred_element_type=F32)
        pieces = [gu_own[early_slot + 2 * pair + piece // 2, piece % 2] for piece in range(4)]
        scatter_start(pair, jnp.concatenate(pieces, axis=1) + total)
        return carry

    def down_pair(pair, carry):
        scatter_start(pair, jnp.dot(act[...], pool[down_slot * BLOCK:, pair_lanes(pair)], preferred_element_type=F32))

        @pl.when(pair >= 2)
        def _():
            for parity in range(2):
                scatter_pass(2 * (pair - 2) + parity, parity)
        return carry

    pairs = col_chunks // 2
    lax.fori_loop(0, 2, down_rest, 0)
    lax.fori_loop(2, pairs, down_pair, 0)

    def each(step, pair):
        for chunk in (2 * pair, 2 * pair + 1):
            if step is scatter_pass:
                step(chunk, chunk % 2)
            else:
                step(chunk)

    each(out_end, 0)
    for pair in range(pairs - 2, pairs):
        each(scatter_pass, pair)
        each(out_end, pair - pairs + 3)
    each(out_pass, 0)
    for pair in range(3, pairs):
        each(out_end, pair)
        each(out_pass, pair - 2)
    for pair in range(pairs - 2, pairs):
        each(out_pass, pair)
    for chunk in range(col_chunks):
        (final_y if chunk % 2 == 0 else final_x)(chunk).wait_recv()
        final_cross(chunk).wait_recv()
    for chunk in range(col_chunks):
        final_cross(chunk).wait_send()
        final_x(chunk).wait_send()
        final_y(chunk).wait_send()


def tail(attn_rows, gain, x_in, w_o, wg_rows, wu_rows, w_down):
    half, depth = attn_rows.shape
    rows, hidden = x_in.shape
    quarter = rows // 4
    chunks = hidden // BLOCK
    ff_chunks = pl.cdiv(w_down.shape[0], BLOCK)
    return pl.pallas_call(
        tail_kernel,
        name="tail",
        out_shape=jax.ShapeDtypeStruct((rows, hidden), BF16),
        in_specs=any_specs(7),
        out_specs=vmem_specs(1)[0],
        scratch_shapes=[
            VMEM((hidden // HEAD, HEAD), BF16),
            DMA,
            VMEM((RING * BLOCK, hidden), BF16),
            VMEM((chunks, 2 * quarter, BLOCK), BF16),
            VMEM((chunks, 2, quarter, BLOCK), F32),
            VMEM((chunks, 2 * quarter, BLOCK), BF16),
            VMEM((chunks, quarter, BLOCK), BF16),
            VMEM((chunks, quarter, BLOCK), BF16),
            VMEM((quarter, hidden), BF16),
            VMEM((quarter, hidden), F32),
            VMEM((quarter, HEAD), F32),
            VMEM((quarter, HEAD), F32),
            VMEM((rows, hidden), BF16),
            VMEM((hidden, rows), BF16),
            VMEM((8, 2, BLOCK, half), BF16),
            VMEM((8, 2, BLOCK, half), BF16),
            VMEM((8, 2, BLOCK, half), F32),
            VMEM((rows, ff_chunks * BLOCK), BF16),
            DMA((RING,)),
            DMA,
            DMA,
            DMA((4,)),
            DMA((2, 2, chunks)),
            DMA((3, 2, chunks)),
            DMA((2, 8)),
            DMA((2, 8)),
        ],
        compiler_params=pltpu.CompilerParams(collective_id=1, has_side_effects=True, vmem_limit_bytes=67043328),
    )(lane_rows(gain), attn_rows, x_in, w_o, wg_rows, wu_rows, w_down)


def solution(mesh):
    act_spec = P(None, "mx")
    cache_spec = P("mx", None, "my", None)
    in_specs = (act_spec, P("mx"), P("mx"), P("mx"), P("mx", "my"), P("my"), P("mx", "my"), P("my"), P("mx", "my"), P("my"), P("my", "mx"), P("mx", "my"), P("mx", "my"), P("my", "mx"), cache_spec, cache_spec)
    out_specs = (act_spec, cache_spec, cache_spec)

    def local_layer(x_in, seq_lens, gain_attn, gain_mlp, w_q, b_q, w_k, b_k, w_v, b_v, w_o, w_gate, w_up, w_down, k_cache, v_cache):
        q_rot, kv_new = project(x_in, seq_lens, gain_attn, b_q, b_k, b_v, w_q, w_k, w_v)
        attn_rows, k_cache_out, v_cache_out = attend(seq_lens, q_rot, kv_new, k_cache, v_cache)
        x_out = tail(attn_rows, gain_mlp, x_in, w_o, w_gate.T, w_up.T, w_down)
        return x_out, k_cache_out, v_cache_out

    return jax.shard_map(local_layer, mesh=mesh, in_specs=in_specs, out_specs=out_specs, check_vma=False)
```

```python
import jax
import jax.numpy as jnp
import numpy as np
from jax import lax
from jax.experimental import pallas as pl
from jax.experimental.pallas import tpu as pltpu
from jax.sharding import PartitionSpec as P

HEAD = 128
NORM_EPS = 1e-6
ROPE_THETA = 1000000.0
MESH = pl.DeviceIdType.MESH
F32 = jnp.float32
BF16 = jnp.bfloat16
QPAD = 16
VMEM = pltpu.VMEM
DMA = pltpu.SemaphoreType.DMA


def any_specs(count):
    return [pl.BlockSpec(memory_space=pl.ANY)] * count


def vmem_specs(count):
    return [pl.BlockSpec(memory_space=pltpu.VMEM)] * count


def lane_rows(vector):
    return vector.reshape(-1, HEAD)


def rotary_frequencies():
    half_dim = HEAD // 2
    inv_freq = np.float32(ROPE_THETA) ** (np.float32(-2.0) * np.arange(half_dim, dtype=np.float32) / np.float32(HEAD))
    return jnp.asarray(np.concatenate([inv_freq, inv_freq])[None, :], F32)


def project_kernel(gain_hbm, bq_hbm, bk_hbm, bv_hbm, lens_hbm, freq_hbm, x_hbm, wq_hbm, wk_hbm, wv_hbm, q_out, kv_out,
                   gain_ref, bq_ref, bk_ref, bv_ref, lens_ref, freq_ref, small_sems, x_ref, x_sem, w_buf, normed, sq_send, sq_recv, part_send, part_recv, part_own, w_sems, send_sems, recv_sems):
    me = lax.axis_index("mx")
    peer = 1 - me
    rows, depth = x_hbm.shape
    half = rows // 2
    width = 2 * HEAD
    q_chunks = wq_hbm.shape[1] // width
    chunks = q_chunks + 2

    def weight_copy(index):
        if index < q_chunks:
            source = wq_hbm.at[:, pl.ds(index * width, width)]
        else:
            source = (wk_hbm, wv_hbm)[index - q_chunks]
        return pltpu.make_async_copy(source, w_buf.at[:, pl.ds(index * width, width)], w_sems.at[index])

    def weight_wait(index):
        lanes = pl.ds(pl.multiple_of(index * width, width), width)
        pltpu.make_async_copy(wk_hbm, w_buf.at[:, lanes], w_sems.at[index]).wait()

    smalls = [pltpu.make_async_copy(source, target, small_sems.at[slot]) for slot, (source, target) in enumerate((
        (lens_hbm, lens_ref), (freq_hbm, freq_ref), (gain_hbm, gain_ref), (bq_hbm, bq_ref), (bk_hbm, bk_ref), (bv_hbm, bv_ref)))]
    for copy in smalls:
        copy.start()
    x_copy = pltpu.make_async_copy(x_hbm, x_ref, x_sem)
    x_copy.start()
    barrier = pltpu.get_barrier_semaphore()
    pl.semaphore_signal(barrier, inc=1, device_id={"mx": peer}, device_id_type=MESH)

    for copy in smalls:
        copy.wait()
    positions = jnp.broadcast_to(lens_ref[...].astype(F32), (half, half)).T
    angles = positions * freq_ref[...]
    cos_tab = jnp.cos(angles)
    lane = lax.broadcasted_iota(jnp.int32, (half, HEAD), 1)
    sin_tab = jnp.where(lane < HEAD // 2, -1.0, 1.0) * jnp.sin(angles)

    x_copy.wait()
    for index in range(chunks):
        weight_copy(index).start()
    total = jnp.zeros((rows, HEAD), F32)
    for start in range(0, depth, HEAD):
        block = x_ref[:, start:start + HEAD].astype(F32)
        total = total + block * block
    sq_own = jnp.sum(total, axis=1, keepdims=True)
    sq_send[...] = jnp.broadcast_to(sq_own, (rows, HEAD))
    pl.semaphore_wait(barrier, 1)

    def remote(source, target, slot):
        return pltpu.make_async_remote_copy(
            src_ref=source, dst_ref=target, send_sem=send_sems.at[slot], recv_sem=recv_sems.at[slot],
            device_id={"mx": peer}, device_id_type=MESH)

    sq_copy = remote(sq_send, sq_recv, chunks)
    sq_copy.start()
    sq_copy.wait()
    own_rows = pl.ds(pl.multiple_of(me * half, half), half)
    peer_rows = pl.ds(pl.multiple_of(peer * half, half), half)
    scale = lax.rsqrt((sq_send[...] + sq_recv[...]) / (2 * depth) + NORM_EPS)
    gains = gain_ref[...].astype(F32)
    for start in range(0, depth, HEAD):
        block = x_ref[:, start:start + HEAD].astype(F32)
        gain = gains[start // HEAD:start // HEAD + 1, :]
        value = (block * scale * gain).astype(BF16)
        normed[own_rows, start:start + HEAD] = value[:half]
        normed[peer_rows, start:start + HEAD] = value[half:]

    def part_copy(index):
        return remote(part_send.at[index], part_recv.at[index], index)

    def multiply(first, count):
        for index in range(count):
            weight_wait(first + index)
        lanes = pl.ds(pl.multiple_of(first * width, width), count * width)
        product = jnp.dot(normed[...], w_buf[:, lanes], preferred_element_type=F32)
        for index in range(count):
            value = product[:, index * width:(index + 1) * width]
            part_own[first + index] = value[:half]
            part_send[first + index] = value[half:].astype(BF16)
        for index in range(count):
            part_copy(first + index).start()

    def multiply_pair(pair, carry):
        multiply(2 * pair, 2)
        return carry

    def multiply_last(index, carry):
        multiply(index, 1)
        return carry

    lax.fori_loop(0, chunks // 2, multiply_pair, 0)
    lax.fori_loop(chunks - chunks % 2, chunks, multiply_last, 0)
    biases = [ref[...].astype(F32) for ref in (bq_ref, bk_ref, bv_ref)]
    for index in range(chunks):
        part_copy(index).wait()
        for head in range(2):
            lanes = slice(head * HEAD, (head + 1) * HEAD)
            columns = slice(index * width + head * HEAD, index * width + (head + 1) * HEAD)
            if index < q_chunks:
                bias = biases[0][2 * index + head:2 * index + head + 1, :]
            else:
                bias = biases[index - q_chunks + 1][head:head + 1, :]
            value = part_own[index][:, lanes] + part_recv[index][:, lanes].astype(F32) + bias
            if index < chunks - 1:
                value = value * cos_tab + pltpu.roll(value, HEAD // 2, 1) * sin_tab
            if index < q_chunks:
                q_out[:, columns] = value.astype(BF16)
            else:
                kv_out[:, (index - q_chunks) * width + head * HEAD:(index - q_chunks) * width + (head + 1) * HEAD] = value.astype(BF16)


def project(x_in, seq_lens, gain, b_q, b_k, b_v, w_q, w_k, w_v):
    rows, depth = x_in.shape
    half = rows // 2
    width = 2 * HEAD
    chunks = w_q.shape[1] // width + 2
    return pl.pallas_call(
        project_kernel,
        name="project",
        out_shape=(jax.ShapeDtypeStruct((half, w_q.shape[1]), BF16), jax.ShapeDtypeStruct((half, 2 * width), BF16)),
        in_specs=any_specs(10),
        out_specs=tuple(vmem_specs(2)),
        scratch_shapes=[
            VMEM((depth // HEAD, HEAD), BF16),
            VMEM((w_q.shape[1] // HEAD, HEAD), BF16),
            VMEM((2, HEAD), BF16),
            VMEM((2, HEAD), BF16),
            VMEM((1, half), jnp.int32),
            VMEM((1, HEAD), F32),
            DMA((6,)),
            VMEM((rows, depth), BF16),
            DMA,
            VMEM((depth, chunks * width), BF16),
            VMEM((rows, depth), BF16),
            VMEM((rows, HEAD), F32),
            VMEM((rows, HEAD), F32),
            VMEM((chunks, half, width), BF16),
            VMEM((chunks, half, width), BF16),
            VMEM((chunks, half, width), F32),
            DMA((chunks,)),
            DMA((chunks + 1,)),
            DMA((chunks + 1,)),
        ],
        compiler_params=pltpu.CompilerParams(collective_id=0, has_side_effects=True, vmem_limit_bytes=67043328),
    )(lane_rows(gain), lane_rows(b_q), lane_rows(b_k), lane_rows(b_v), seq_lens[None, :], rotary_frequencies(), x_in, w_q, w_k, w_v)


SLOTS = 6
ROWS_STEP = 8


def attend_kernel(lens_ref, q_hbm, kv_hbm, k_hbm, v_hbm, o_ref, k_out, v_out,
                  q_ref, kv_ref, small_sems, k_buf, v_buf, q_wide, q_packed, kv_wide, o_wide, parity, scores, weights, sums, in_sems, out_sems):
    batch, kv_rows, _ = k_hbm.shape
    q_heads = q_hbm.shape[1] // HEAD
    group = q_heads // 2
    steps = batch // ROWS_STEP

    def load(step, kind):
        slot = lax.rem(step, SLOTS)
        source, target = ((k_hbm, k_buf), (v_hbm, v_buf))[kind]
        return pltpu.make_async_copy(source.at[pl.ds(step * ROWS_STEP, ROWS_STEP)], target.at[slot], in_sems.at[kind, slot])

    def save(step, kind):
        slot = lax.rem(step, SLOTS)
        source, target = ((k_buf, k_out), (v_buf, v_out))[kind]
        return pltpu.make_async_copy(source.at[slot], target.at[pl.ds(step * ROWS_STEP, ROWS_STEP)], out_sems.at[kind, slot])

    q_copy = pltpu.make_async_copy(q_hbm, q_ref, small_sems.at[0])
    kv_copy = pltpu.make_async_copy(kv_hbm, kv_ref, small_sems.at[1])
    q_copy.start()
    kv_copy.start()
    for kind in range(2):
        load(0, kind).start()

    q_wide[...] = jnp.zeros_like(q_wide)
    q_copy.wait()
    kv_copy.wait()
    for step in range(1, 3):
        for kind in range(2):
            load(step, kind).start()
    for head in range(q_heads):
        q_wide[pl.ds(head, batch, stride=QPAD), :] = q_ref[:, head * HEAD:(head + 1) * HEAD].astype(F32)
    q_packed[...] = q_wide[...].astype(BF16)
    for kind in range(2):
        for head in range(2):
            start = (kind * 2 + head) * HEAD
            kv_wide[kind, pl.ds(head, batch, stride=2), :] = kv_ref[:, start:start + HEAD].astype(F32)
    row_head = lax.broadcasted_iota(jnp.int32, (QPAD, kv_rows), 0) >= group
    col_head = lax.rem(lax.broadcasted_iota(jnp.int32, (QPAD, kv_rows), 1), 2) == 1
    parity[...] = jnp.where(row_head == col_head, 0.0, -jnp.inf)
    columns = lax.broadcasted_iota(jnp.int32, (QPAD, kv_rows), 1)
    tile_row = lax.broadcasted_iota(jnp.int32, (16, HEAD), 0)
    tile_pos = lax.div(tile_row, 2)
    tile_odd = lax.rem(tile_row, 2) == 1

    def body(step, carry):
        slot = lax.rem(step, SLOTS)

        @pl.when(step + 3 < steps)
        def _():
            @pl.when(step >= 3)
            def _():
                for kind in range(2):
                    save(step - 3, kind).wait()
            for kind in range(2):
                load(step + 3, kind).start()

        for kind in range(2):
            load(step, kind).wait()
        for row in range(ROWS_STEP):
            index = step * ROWS_STEP + row
            position = lens_ref[index]
            base = pl.multiple_of(lax.div(position, 8) * 16, 16)
            offset = lax.rem(position, 8)
            for kind, buffer in ((0, k_buf), (1, v_buf)):
                low = kv_wide[kind, pl.ds(2 * index, 1), :]
                high = kv_wide[kind, pl.ds(2 * index + 1, 1), :]
                fresh = jnp.where(tile_odd, high, low).astype(BF16)
                tile = buffer[slot, row, pl.ds(base, 16), :]
                buffer[slot, row, pl.ds(base, 16), :] = jnp.where(tile_pos == offset, fresh, tile)
        for row in range(ROWS_STEP):
            q_start = pl.multiple_of((step * ROWS_STEP + row) * QPAD, QPAD)
            scores[row] = lax.dot_general(q_packed[pl.ds(q_start, QPAD), :], k_buf[slot, row], (((1,), (1,)), ((), ())),
                                          preferred_element_type=F32)
        for kind in range(2):
            save(step, kind).start()
        for row in range(ROWS_STEP):
            limit = 2 * lens_ref[step * ROWS_STEP + row] + 2
            masked = jnp.where(columns < limit, scores[row] * HEAD ** -0.5 + parity[...], -jnp.inf)
            weight = jnp.exp(masked - jnp.max(masked, axis=1, keepdims=True))
            sums[row] = jnp.broadcast_to(jnp.sum(weight, axis=1, keepdims=True), (QPAD, HEAD))
            weights[row] = weight.astype(BF16)
        for row in range(ROWS_STEP):
            q_start = pl.multiple_of((step * ROWS_STEP + row) * QPAD, QPAD)
            mixed = jnp.dot(weights[row], v_buf[slot, row], preferred_element_type=F32)
            o_wide[pl.ds(q_start, QPAD), :] = mixed / sums[row]
        return carry

    lax.fori_loop(0, steps, body, 0)
    for head in range(q_heads):
        o_ref[:, head * HEAD:(head + 1) * HEAD] = o_wide[pl.ds(head, batch, stride=QPAD), :].astype(BF16)
    for step in range(steps - SLOTS, steps):
        for kind in range(2):
            save(step, kind).wait()


def attend(seq_lens, q_rot, kv_new, k_cache, v_cache):
    batch, seq_len, kv_heads, _ = k_cache.shape
    rows = seq_len * kv_heads
    flat = (batch, rows, HEAD)
    out, k_out, v_out = pl.pallas_call(
        attend_kernel,
        name="attend",
        out_shape=(jax.ShapeDtypeStruct(q_rot.shape, BF16), jax.ShapeDtypeStruct(flat, BF16), jax.ShapeDtypeStruct(flat, BF16)),
        in_specs=[pl.BlockSpec(memory_space=pltpu.SMEM)] + any_specs(4),
        out_specs=tuple(vmem_specs(1) + any_specs(2)),
        scratch_shapes=[
            VMEM(q_rot.shape, BF16),
            VMEM(kv_new.shape, BF16),
            DMA((2,)),
            VMEM((SLOTS, ROWS_STEP, rows, HEAD), BF16),
            VMEM((SLOTS, ROWS_STEP, rows, HEAD), BF16),
            VMEM((batch * QPAD, HEAD), F32),
            VMEM((batch * QPAD, HEAD), BF16),
            VMEM((2, batch * 2, HEAD), F32),
            VMEM((batch * QPAD, HEAD), F32),
            VMEM((QPAD, rows), F32),
            VMEM((ROWS_STEP, QPAD, rows), F32),
            VMEM((ROWS_STEP, QPAD, rows), BF16),
            VMEM((ROWS_STEP, QPAD, HEAD), F32),
            DMA((2, SLOTS)),
            DMA((2, SLOTS)),
        ],
        compiler_params=pltpu.CompilerParams(vmem_limit_bytes=64 << 20),
    )(seq_lens, q_rot, kv_new, k_cache.reshape(flat), v_cache.reshape(flat))
    return out, k_out.reshape(k_cache.shape), v_out.reshape(v_cache.shape)


BLOCK = 256
RING = 36


def tail_kernel(gain_hbm, attn_hbm, x_hbm, wo_hbm, wg_hbm, wu_hbm, wd_hbm, out_ref,
                gain_ref, gain_sem, pool, part, keep, recv_one, send_two, recv_two, x_own, mid, sq_send, sq_recv,
                h_rows, h_cols, gu_send, gu_recv, gu_own, act,
                pool_sems, x_sem, attn_sem, core_sems, rs_sems, ag_sems, gu_sems, act_sems):
    my = lax.axis_index("my")
    me = lax.axis_index("mx")
    peer = 1 - me
    side_x = my + 1 - 2 * lax.rem(my, 2)
    side_y = lax.rem(my + 2, 4)
    cross = 3 - my
    half, depth = attn_hbm.shape
    batch = 2 * half
    quarter = batch // 4
    hidden = x_hbm.shape[1]
    ff = wg_hbm.shape[0]
    col_chunks = hidden // BLOCK
    ff_chunks = pl.cdiv(ff, BLOCK)
    ff_rest = ff - (ff_chunks - 1) * BLOCK
    chunk_ring = RING // 2
    out_blocks = depth // BLOCK
    out_slot = RING - 6
    down_slot = RING - ff_chunks
    early_blocks = chunk_ring
    late_chunk = chunk_ring + chunk_ring // 2 - (down_slot // 2)
    late_count = ff_chunks - late_chunk

    def slot_rows(slot, count=BLOCK):
        return pl.ds(pl.multiple_of(slot * BLOCK, BLOCK), count)

    def block_copy(source, block, slot, count=BLOCK):
        return pltpu.make_async_copy(source.at[slot_rows(block, count)], pool.at[slot_rows(slot, count)], pool_sems.at[slot])

    def ff_slot(chunk):
        return 2 * jnp.where(chunk < chunk_ring, chunk, jnp.where(chunk < late_chunk, chunk - late_chunk + chunk_ring // 2, chunk - late_chunk))

    def ff_copies(chunk, count=BLOCK):
        slot = ff_slot(chunk)
        return block_copy(wg_hbm, chunk, slot, count), block_copy(wu_hbm, chunk, slot + 1, count)

    def down_copy(block, count=BLOCK):
        slot = down_slot + jnp.where(block < early_blocks, block + ff_chunks - early_blocks, block - early_blocks)
        return block_copy(wd_hbm, block, slot, count)

    def out_copy(block):
        return block_copy(wo_hbm, block, out_slot + block)

    def to_core(source, target, slot):
        return pltpu.make_async_remote_copy(src_ref=source, dst_ref=target, send_sem=slot[0], recv_sem=slot[1],
                                            device_id={"mx": peer}, device_id_type=MESH)

    def to_chip(source, target, chip, send_sem, recv_sem):
        return pltpu.make_async_remote_copy(src_ref=source, dst_ref=target, send_sem=send_sem, recv_sem=recv_sem,
                                            device_id={"my": chip}, device_id_type=MESH)

    own_half = pl.ds(pl.multiple_of(me * half, half), half)
    peer_half = pl.ds(pl.multiple_of(peer * half, half), half)
    rows_in = h_rows.at[:, pl.ds(0, depth)]
    full = h_rows.at[:, pl.ds(depth, depth)]
    attn_load = pltpu.make_async_copy(attn_hbm, full.at[own_half], attn_sem)
    attn_load.start()
    own_rows = pl.ds(pl.multiple_of(my * quarter, quarter), quarter)
    x_copy = pltpu.make_async_copy(x_hbm.at[own_rows], x_own, x_sem)
    x_copy.start()
    gain_copy = pltpu.make_async_copy(gain_hbm, gain_ref, gain_sem)
    gain_copy.start()

    barrier = pltpu.get_barrier_semaphore()
    pl.semaphore_signal(barrier, inc=1, device_id={"mx": peer}, device_id_type=MESH)
    pl.semaphore_signal(barrier, inc=1, device_id={"my": side_x}, device_id_type=MESH)
    pl.semaphore_signal(barrier, inc=1, device_id={"my": side_y}, device_id_type=MESH)
    attn_load.wait()
    for block in range(out_blocks):
        out_copy(block).start()
    pl.semaphore_wait(barrier, 3)
    attn_copy = to_core(full.at[own_half], full.at[own_half], (core_sems.at[0], core_sems.at[1]))
    attn_copy.start()
    attn_copy.wait()
    for place, owner in enumerate((my, side_x, cross, side_y)):
        rows_in[place * quarter:(place + 1) * quarter, :] = full[pl.ds(pl.multiple_of(owner * quarter, quarter), quarter), :]

    sub = quarter // 2
    wide = 2 * BLOCK
    pairs = hidden // wide

    def wide_cols(pair):
        if isinstance(pair, int):
            return slice(pair * wide, (pair + 1) * wide)
        return pl.ds(pl.multiple_of(pair * wide, wide), wide)

    def first_side(parity):
        return side_x + parity * (side_y - side_x)

    def second_side(parity):
        return side_y + parity * (side_x - side_y)

    def sub_rows(index):
        if isinstance(index, int):
            return slice(index * sub, (index + 1) * sub)
        return pl.ds(pl.multiple_of(index * sub, sub), sub)

    def scatter_one(chunk, parity):
        lead = pl.ds(pl.multiple_of(sub * (1 + parity), sub), 2 * sub)
        return to_chip(part.at[chunk, lead], recv_one.at[chunk], first_side(parity), rs_sems.at[0, 0, chunk], rs_sems.at[0, 1, chunk])

    def scatter_two(chunk, parity):
        return to_chip(send_two.at[chunk], recv_two.at[chunk], second_side(parity), rs_sems.at[1, 0, chunk], rs_sems.at[1, 1, chunk])

    def scatter_store(pair, total):
        for block in range(2):
            chunk = 2 * pair + block
            pieces = [total[place * quarter + block * sub:place * quarter + (block + 1) * sub] for place in range(4)]
            for place in range(1, 4):
                part[chunk, sub_rows(place), :] = pieces[place].astype(BF16)
            keep[chunk, 0] = pieces[0]
            keep[chunk, 1] = pieces[1]
            keep[chunk, 2] = pieces[3]

    def scatter_pass(chunk, parity):
        scatter_one(chunk, parity).wait()
        send_two[chunk] = (keep[chunk, 2 - parity] + recv_one[chunk, sub_rows(1 - parity), :].astype(F32)).astype(BF16)
        scatter_two(chunk, parity).start()
        keep[chunk, 0] = keep[chunk, 0] + recv_one[chunk, sub_rows(parity), :].astype(F32)

    def scatter_end(chunk, parity):
        scatter_two(chunk, parity).wait()
        return keep[chunk, 0] + recv_two[chunk].astype(F32)

    def turn(pair, block):
        return (pair + block) % 2

    def mid_end(pair, block):
        before = x_own[sub_rows(block), wide_cols(pair)].astype(F32)
        mid[sub_rows(block), wide_cols(pair)] = (before + scatter_end(2 * pair + block, turn(pair, block))).astype(BF16).astype(F32)

    x_copy.wait()
    gain_copy.wait()
    for block in range(out_blocks):
        out_copy(block).wait()
    for chunk in range(out_slot // 2):
        for copy in ff_copies(chunk):
            copy.start()
    def out_product(pair, carry):
        weights = pool[out_slot * BLOCK:out_slot * BLOCK + depth, wide_cols(pair)]
        scatter_store(pair, jnp.dot(rows_in[...], weights, preferred_element_type=F32))
        scatter_one(2 * pair, lax.rem(pair, 2)).start()
        return carry

    lax.fori_loop(0, pairs, out_product, 0)
    gains = gain_ref[...].astype(F32)

    def square_copy(block):
        return to_core(sq_send.at[sub_rows(block)], sq_recv.at[sub_rows(block)], (core_sems.at[2 + 2 * block], core_sems.at[3 + 2 * block]))

    def square_start(block):
        square = jnp.zeros((sub, HEAD), F32)
        for start in range(0, hidden, HEAD):
            value = mid[sub_rows(block), start:start + HEAD]
            square = square + value * value
        sq_send[sub_rows(block), :] = jnp.broadcast_to(jnp.sum(square, axis=1, keepdims=True), (sub, HEAD))
        square_copy(block).start()

    def norm_rows(block):
        square_copy(block).wait()
        scale = lax.rsqrt((sq_send[sub_rows(block), :] + sq_recv[sub_rows(block), :]) / (2 * hidden) + NORM_EPS)
        for start in range(0, hidden, HEAD):
            gain = gains[start // HEAD:start // HEAD + 1, :]
            h_rows[sub_rows(block), start:start + HEAD] = (mid[sub_rows(block), start:start + HEAD] * scale * gain).astype(BF16)

    def h_block(place, pair, block):
        return h_rows.at[sub_rows(2 * place + block), wide_cols(pair)]

    def gather_x(pair, block):
        chunk = 2 * pair + block
        return to_chip(h_block(0, pair, block), h_block(1, pair, block), side_x, ag_sems.at[0, 0, chunk], ag_sems.at[0, 1, chunk])

    def gather_y(pair, block):
        chunk = 2 * pair + block
        return to_chip(h_block(0, pair, block), h_block(3, pair, block), side_y, ag_sems.at[1, 0, chunk], ag_sems.at[1, 1, chunk])

    def gather_cross(pair, block):
        chunk = 2 * pair + block
        source = 1 if turn(pair, block) == 0 else 3
        return to_chip(h_block(source, pair, block), h_block(2, pair, block), second_side(turn(pair, block)),
                       ag_sems.at[2, 0, chunk], ag_sems.at[2, 1, chunk])

    def gather_send(pair, block):
        gather_x(pair, block).start()
        gather_y(pair, block).start()

    def gather_pass(pair, block):
        (gather_y if turn(pair, block) else gather_x)(pair, block).wait_recv()
        gather_cross(pair, block).start()

    def start_late(pair):
        scatter_one(2 * pair + 1, turn(pair, 1)).start()

    def pass_late(pair):
        scatter_pass(2 * pair + 1, turn(pair, 1))

    for pair in range(2):
        start_late(pair)
    for chunk in range(out_slot // 2, chunk_ring):
        for copy in ff_copies(chunk):
            copy.start()
    for pair in range(pairs):
        scatter_pass(2 * pair, turn(pair, 0))
    for pair in range(2, pairs):
        start_late(pair)
    for pair in range(2):
        pass_late(pair)
    for pair in range(pairs):
        mid_end(pair, 0)
    square_start(0)
    norm_rows(0)
    for pair in range(2):
        gather_send(pair, 0)
    for pair in range(2, pairs):
        pass_late(pair)
    for pair in range(2, pairs):
        gather_send(pair, 0)
    for pair in range(pairs):
        mid_end(pair, 1)
    square_start(1)
    for pair in range(2):
        gather_pass(pair, 0)
    norm_rows(1)
    for pair in range(pairs):
        gather_send(pair, 1)
    for pair in range(2, pairs):
        gather_pass(pair, 0)
    for pair in range(pairs):
        gather_pass(pair, 1)
    for pair in range(pairs):
        for block in range(2):
            (gather_x if turn(pair, block) else gather_y)(pair, block).wait_recv()
            gather_cross(pair, block).wait_recv()
        for place, source in enumerate((own_half, peer_half)):
            h_cols[wide_cols(pair), place * half:(place + 1) * half] = h_rows[source, wide_cols(pair)].astype(F32).T.astype(BF16)
        for block in range(2):
            gather_x(pair, block).wait_send()
            gather_y(pair, block).wait_send()
            gather_cross(pair, block).wait_send()

    def gu_copy(chunk):
        slot = lax.rem(chunk, 8)
        return to_core(gu_send.at[slot], gu_recv.at[slot], (gu_sems.at[0, slot], gu_sems.at[1, slot]))

    def act_lanes(chunk):
        place = jnp.where(chunk < early_blocks, chunk + ff_chunks - early_blocks, chunk - early_blocks)
        return pl.ds(pl.multiple_of(place * BLOCK, BLOCK), BLOCK)

    def act_copy(chunk):
        lanes = act_lanes(chunk)
        return to_core(act.at[own_half, lanes], act.at[own_half, lanes], (act_sems.at[0, lax.rem(chunk, 8)], act_sems.at[1, lax.rem(chunk, 8)]))

    def ff_products(chunk):
        slot = lax.rem(chunk, 8)
        base = ff_slot(chunk)
        product = jnp.dot(pool[slot_rows(base, 2 * BLOCK), :], h_cols[...], preferred_element_type=F32)
        for kind in range(2):
            rows = slice(kind * BLOCK, (kind + 1) * BLOCK)
            gu_own[slot, kind] = product[rows, :half]
            gu_send[slot, kind] = product[rows, half:].astype(BF16)

    def activate(chunk):
        slot = lax.rem(chunk, 8)
        gate = gu_own[slot, 0] + gu_recv[slot, 0].astype(F32)
        up = gu_own[slot, 1] + gu_recv[slot, 1].astype(F32)
        value = gate * jax.nn.sigmoid(gate) * up
        row = chunk * BLOCK + lax.broadcasted_iota(jnp.int32, value.shape, 0)
        value = jnp.where(row < ff, value, 0.0)
        lanes = act_lanes(chunk)
        act[own_half, lanes] = value.T.astype(BF16)

    def refill(chunk):
        half_ring = chunk_ring // 2

        @pl.when(chunk < late_count - 1)
        def _():
            for copy in ff_copies(late_chunk + chunk):
                copy.start()

        @pl.when(chunk == late_count - 1)
        def _():
            for copy in ff_copies(ff_chunks - 1, ff_rest):
                copy.start()

        @pl.when((chunk >= late_count) & (chunk < half_ring))
        def _():
            for copy in ff_copies(chunk - late_count + chunk_ring):
                copy.start()

        @pl.when((chunk >= half_ring) & (chunk < chunk_ring))
        def _():
            down_copy(2 * (chunk - half_ring)).start()
            down_copy(2 * (chunk - half_ring) + 1).start()

        free = 2 * (chunk - chunk_ring + late_count) - down_slot + early_blocks

        @pl.when((chunk >= chunk_ring) & (chunk < late_chunk) & (free >= early_blocks))
        def _():
            down_copy(free).start()

        @pl.when((chunk >= chunk_ring) & (chunk < late_chunk - 1))
        def _():
            down_copy(free + 1).start()

        @pl.when(chunk == late_chunk - 1)
        def _():
            down_copy(ff_chunks - 1, ff_rest).start()

    def ff_pair(pair, active):
        chunks = (2 * pair, 2 * pair + 1)
        if active:
            for chunk in chunks:
                gu_copy(chunk - 4).wait()
        for chunk in chunks:
            for copy in ff_copies(chunk):
                copy.wait()
        if active:
            for chunk in chunks:
                activate(chunk - 4)
        for chunk in chunks:
            ff_products(chunk)
        for chunk in chunks:
            gu_copy(chunk).start()
        if active:
            for chunk in chunks:
                act_copy(chunk - 4).start()
        for chunk in chunks:
            refill(chunk)

    def ff_first(pair, carry):
        ff_pair(pair, False)
        return carry

    def ff_step(pair, carry):
        @pl.when(pair >= 4)
        def _():
            for parity in range(2):
                act_copy(2 * (pair - 4) + parity).wait()
        ff_pair(pair, True)
        return carry

    last = ff_chunks - 1
    ff_pairs = last // 2
    lax.fori_loop(0, 2, ff_first, 0)
    lax.fori_loop(2, ff_pairs, ff_step, 0)

    def finish(chunk):
        gu_copy(chunk).wait()
        activate(chunk)
        act_copy(chunk).start()

    for chunk in range(2 * ff_pairs - 8, 2 * ff_pairs - 6):
        act_copy(chunk).wait()

    def ff_last(chunk, carry):
        for copy in ff_copies(chunk, ff_rest):
            copy.wait()
        ff_products(chunk)
        gu_copy(chunk).start()
        return carry

    lax.fori_loop(last, last + 1, ff_last, 0)
    for chunk in range(last - 4, last - 2):
        finish(chunk)
    for block in range(early_blocks):
        down_copy(block).wait()
    late_lanes = (ff_chunks - early_blocks) * BLOCK
    late_row = down_slot * BLOCK + late_lanes

    early_slot = 3

    def down_early(pair, carry):
        value = jnp.dot(act[:, late_lanes:], pool[late_row:, wide_cols(pair)], preferred_element_type=F32)
        for piece in range(4):
            gu_own[early_slot + 2 * pair + piece // 2, piece % 2] = value[:, piece * half:(piece + 1) * half]
        return carry

    lax.fori_loop(0, 1, down_early, 0)
    for chunk in range(last - 2, ff_chunks):
        finish(chunk)
    lax.fori_loop(1, 2, down_early, 0)
    for block in range(early_blocks, ff_chunks):
        down_copy(block, ff_rest if block == last else BLOCK).wait()
    for chunk in range(2 * ff_pairs - 6, ff_chunks):
        act_copy(chunk).wait()

    def out_block(owner, chunk):
        pair, block = chunk // 2, chunk % 2
        return out_ref.at[sub_rows(2 * owner + block), wide_cols(pair)]

    def final_x(chunk):
        target = out_block(my, chunk)
        return to_chip(target, target, side_x, ag_sems.at[0, 0, chunk], ag_sems.at[0, 1, chunk])

    def final_y(chunk):
        target = out_block(my, chunk)
        return to_chip(target, target, side_y, ag_sems.at[1, 0, chunk], ag_sems.at[1, 1, chunk])

    def final_cross(chunk):
        target = out_block(first_side(chunk % 2), chunk)
        return to_chip(target, target, second_side(chunk % 2), ag_sems.at[2, 0, chunk], ag_sems.at[2, 1, chunk])

    def out_end(chunk):
        pair, block = chunk // 2, chunk % 2
        value = mid[sub_rows(block), wide_cols(pair)] + scatter_end(chunk, block)
        out_ref[sub_rows(2 * my + block), wide_cols(pair)] = value.astype(BF16)
        final_x(chunk).start()
        final_y(chunk).start()

    def out_pass(chunk):
        (final_x if chunk % 2 == 0 else final_y)(chunk).wait_recv()
        final_cross(chunk).start()

    def scatter_start(pair, total):
        scatter_store(pair, total)
        for block in range(2):
            scatter_one(2 * pair + block, block).start()

    def down_rest(pair, carry):
        total = jnp.dot(act[:, :late_lanes], pool[down_slot * BLOCK:late_row, wide_cols(pair)], preferred_element_type=F32)
        pieces = [gu_own[early_slot + 2 * pair + piece // 2, piece % 2] for piece in range(4)]
        scatter_start(pair, jnp.concatenate(pieces, axis=1) + total)
        return carry

    def down_pair(pair, carry):
        scatter_start(pair, jnp.dot(act[...], pool[down_slot * BLOCK:, wide_cols(pair)], preferred_element_type=F32))

        @pl.when(pair >= 2)
        def _():
            for parity in range(2):
                scatter_pass(2 * (pair - 2) + parity, parity)
        return carry

    lax.fori_loop(0, 2, down_rest, 0)
    lax.fori_loop(2, pairs, down_pair, 0)

    def each(step, pair):
        for chunk in (2 * pair, 2 * pair + 1):
            if step is scatter_pass:
                step(chunk, chunk % 2)
            else:
                step(chunk)

    each(out_end, 0)
    for pair in range(pairs - 2, pairs):
        each(scatter_pass, pair)
        each(out_end, pair - pairs + 3)
    each(out_pass, 0)
    for pair in range(3, pairs):
        each(out_end, pair)
        each(out_pass, pair - 2)
    for pair in range(pairs - 2, pairs):
        each(out_pass, pair)
    for chunk in range(col_chunks):
        (final_y if chunk % 2 == 0 else final_x)(chunk).wait_recv()
        final_cross(chunk).wait_recv()
    for chunk in range(col_chunks):
        final_cross(chunk).wait_send()
        final_x(chunk).wait_send()
        final_y(chunk).wait_send()


def tail(attn_rows, gain, x_in, w_o, wg_rows, wu_rows, w_down):
    half, depth = attn_rows.shape
    rows, hidden = x_in.shape
    quarter = rows // 4
    chunks = hidden // BLOCK
    ff_chunks = pl.cdiv(w_down.shape[0], BLOCK)
    return pl.pallas_call(
        tail_kernel,
        name="tail",
        out_shape=jax.ShapeDtypeStruct((rows, hidden), BF16),
        in_specs=any_specs(7),
        out_specs=vmem_specs(1)[0],
        scratch_shapes=[
            VMEM((hidden // HEAD, HEAD), BF16),
            DMA,
            VMEM((RING * BLOCK, hidden), BF16),
            VMEM((chunks, 2 * quarter, 2 * BLOCK), BF16),
            VMEM((chunks, 3, quarter // 2, 2 * BLOCK), F32),
            VMEM((chunks, quarter, 2 * BLOCK), BF16),
            VMEM((chunks, quarter // 2, 2 * BLOCK), BF16),
            VMEM((chunks, quarter // 2, 2 * BLOCK), BF16),
            VMEM((quarter, hidden), BF16),
            VMEM((quarter, hidden), F32),
            VMEM((quarter, HEAD), F32),
            VMEM((quarter, HEAD), F32),
            VMEM((rows, hidden), BF16),
            VMEM((hidden, rows), BF16),
            VMEM((8, 2, BLOCK, half), BF16),
            VMEM((8, 2, BLOCK, half), BF16),
            VMEM((8, 2, BLOCK, half), F32),
            VMEM((rows, ff_chunks * BLOCK), BF16),
            DMA((RING,)),
            DMA,
            DMA,
            DMA((6,)),
            DMA((2, 2, chunks)),
            DMA((3, 2, chunks)),
            DMA((2, 8)),
            DMA((2, 8)),
        ],
        compiler_params=pltpu.CompilerParams(collective_id=1, has_side_effects=True, vmem_limit_bytes=67043328),
    )(lane_rows(gain), attn_rows, x_in, w_o, wg_rows, wu_rows, w_down)


def solution(mesh):
    act_spec = P(None, "mx")
    cache_spec = P("mx", None, "my", None)
    in_specs = (act_spec, P("mx"), P("mx"), P("mx"), P("mx", "my"), P("my"), P("mx", "my"), P("my"), P("mx", "my"), P("my"), P("my", "mx"), P("mx", "my"), P("mx", "my"), P("my", "mx"), cache_spec, cache_spec)
    out_specs = (act_spec, cache_spec, cache_spec)

    def local_layer(x_in, seq_lens, gain_attn, gain_mlp, w_q, b_q, w_k, b_k, w_v, b_v, w_o, w_gate, w_up, w_down, k_cache, v_cache):
        q_rot, kv_new = project(x_in, seq_lens, gain_attn, b_q, b_k, b_v, w_q, w_k, w_v)
        attn_rows, k_cache_out, v_cache_out = attend(seq_lens, q_rot, kv_new, k_cache, v_cache)
        x_out = tail(attn_rows, gain_mlp, x_in, w_o, w_gate.T, w_up.T, w_down)
        return x_out, k_cache_out, v_cache_out

    return jax.shard_map(local_layer, mesh=mesh, in_specs=in_specs, out_specs=out_specs, check_vma=False)
```

```python
import jax
import jax.numpy as jnp
import numpy as np
from jax import lax
from jax.experimental import pallas as pl
from jax.experimental.pallas import tpu as pltpu
from jax.sharding import PartitionSpec as P

HEAD = 128
NORM_EPS = 1e-6
ROPE_THETA = 1000000.0
MESH = pl.DeviceIdType.MESH
F32 = jnp.float32
BF16 = jnp.bfloat16
QPAD = 16
VMEM = pltpu.VMEM
DMA = pltpu.SemaphoreType.DMA


def any_specs(count):
    return [pl.BlockSpec(memory_space=pl.ANY)] * count


def vmem_specs(count):
    return [pl.BlockSpec(memory_space=pltpu.VMEM)] * count


def lane_rows(vector):
    return vector.reshape(-1, HEAD)


def rotary_frequencies():
    half_dim = HEAD // 2
    inv_freq = np.float32(ROPE_THETA) ** (np.float32(-2.0) * np.arange(half_dim, dtype=np.float32) / np.float32(HEAD))
    return jnp.asarray(np.concatenate([inv_freq, inv_freq])[None, :], F32)


def project_kernel(gain_hbm, bq_hbm, bk_hbm, bv_hbm, lens_hbm, freq_hbm, x_hbm, wq_hbm, wk_hbm, wv_hbm, q_out, kv_out,
                   gain_ref, bq_ref, bk_ref, bv_ref, lens_ref, freq_ref, small_sems, x_ref, x_sem, w_buf, normed, sq_send, sq_recv, part_send, part_recv, part_own, w_sems, send_sems, recv_sems):
    me = lax.axis_index("mx")
    peer = 1 - me
    rows, depth = x_hbm.shape
    half = rows // 2
    width = 2 * HEAD
    q_chunks = wq_hbm.shape[1] // width
    chunks = q_chunks + 2

    def weight_copy(index):
        if index < q_chunks:
            source = wq_hbm.at[:, pl.ds(index * width, width)]
        else:
            source = (wk_hbm, wv_hbm)[index - q_chunks]
        return pltpu.make_async_copy(source, w_buf.at[:, pl.ds(index * width, width)], w_sems.at[index])

    def weight_wait(index):
        lanes = pl.ds(pl.multiple_of(index * width, width), width)
        pltpu.make_async_copy(wk_hbm, w_buf.at[:, lanes], w_sems.at[index]).wait()

    smalls = [pltpu.make_async_copy(source, target, small_sems.at[slot]) for slot, (source, target) in enumerate((
        (lens_hbm, lens_ref), (freq_hbm, freq_ref), (gain_hbm, gain_ref), (bq_hbm, bq_ref), (bk_hbm, bk_ref), (bv_hbm, bv_ref)))]
    for copy in smalls:
        copy.start()
    x_copy = pltpu.make_async_copy(x_hbm, x_ref, x_sem)
    x_copy.start()
    barrier = pltpu.get_barrier_semaphore()
    pl.semaphore_signal(barrier, inc=1, device_id={"mx": peer}, device_id_type=MESH)

    for copy in smalls:
        copy.wait()
    positions = jnp.broadcast_to(lens_ref[...].astype(F32), (half, half)).T
    angles = positions * freq_ref[...]
    cos_tab = jnp.cos(angles)
    lane = lax.broadcasted_iota(jnp.int32, (half, HEAD), 1)
    sin_tab = jnp.where(lane < HEAD // 2, -1.0, 1.0) * jnp.sin(angles)

    x_copy.wait()
    for index in range(chunks):
        weight_copy(index).start()
    total = jnp.zeros((rows, HEAD), F32)
    for start in range(0, depth, HEAD):
        block = x_ref[:, start:start + HEAD].astype(F32)
        total = total + block * block
    sq_own = jnp.sum(total, axis=1, keepdims=True)
    sq_send[...] = jnp.broadcast_to(sq_own, (rows, HEAD))
    pl.semaphore_wait(barrier, 1)

    def remote(source, target, slot):
        return pltpu.make_async_remote_copy(
            src_ref=source, dst_ref=target, send_sem=send_sems.at[slot], recv_sem=recv_sems.at[slot],
            device_id={"mx": peer}, device_id_type=MESH)

    sq_copy = remote(sq_send, sq_recv, chunks)
    sq_copy.start()
    sq_copy.wait()
    own_rows = pl.ds(pl.multiple_of(me * half, half), half)
    peer_rows = pl.ds(pl.multiple_of(peer * half, half), half)
    scale = lax.rsqrt((sq_send[...] + sq_recv[...]) / (2 * depth) + NORM_EPS)
    gains = gain_ref[...].astype(F32)
    for start in range(0, depth, HEAD):
        block = x_ref[:, start:start + HEAD].astype(F32)
        gain = gains[start // HEAD:start // HEAD + 1, :]
        value = (block * scale * gain).astype(BF16)
        normed[own_rows, start:start + HEAD] = value[:half]
        normed[peer_rows, start:start + HEAD] = value[half:]

    def part_copy(index):
        return remote(part_send.at[index], part_recv.at[index], index)

    def multiply(first, count):
        for index in range(count):
            weight_wait(first + index)
        lanes = pl.ds(pl.multiple_of(first * width, width), count * width)
        product = jnp.dot(normed[...], w_buf[:, lanes], preferred_element_type=F32)
        for index in range(count):
            value = product[:, index * width:(index + 1) * width]
            part_own[first + index] = value[:half]
            part_send[first + index] = value[half:].astype(BF16)
        for index in range(count):
            part_copy(first + index).start()

    def multiply_pair(pair, carry):
        multiply(2 * pair, 2)
        return carry

    def multiply_last(index, carry):
        multiply(index, 1)
        return carry

    lax.fori_loop(0, chunks // 2, multiply_pair, 0)
    lax.fori_loop(chunks - chunks % 2, chunks, multiply_last, 0)
    biases = [ref[...].astype(F32) for ref in (bq_ref, bk_ref, bv_ref)]
    for index in range(chunks):
        part_copy(index).wait()
        for head in range(2):
            lanes = slice(head * HEAD, (head + 1) * HEAD)
            columns = slice(index * width + head * HEAD, index * width + (head + 1) * HEAD)
            if index < q_chunks:
                bias = biases[0][2 * index + head:2 * index + head + 1, :]
            else:
                bias = biases[index - q_chunks + 1][head:head + 1, :]
            value = part_own[index][:, lanes] + part_recv[index][:, lanes].astype(F32) + bias
            if index < chunks - 1:
                value = value * cos_tab + pltpu.roll(value, HEAD // 2, 1) * sin_tab
            if index < q_chunks:
                q_out[:, columns] = value.astype(BF16)
            else:
                kv_out[:, (index - q_chunks) * width + head * HEAD:(index - q_chunks) * width + (head + 1) * HEAD] = value.astype(BF16)


def project(x_in, seq_lens, gain, b_q, b_k, b_v, w_q, w_k, w_v):
    rows, depth = x_in.shape
    half = rows // 2
    width = 2 * HEAD
    chunks = w_q.shape[1] // width + 2
    return pl.pallas_call(
        project_kernel,
        name="project",
        out_shape=(jax.ShapeDtypeStruct((half, w_q.shape[1]), BF16), jax.ShapeDtypeStruct((half, 2 * width), BF16)),
        in_specs=any_specs(10),
        out_specs=tuple(vmem_specs(2)),
        scratch_shapes=[
            VMEM((depth // HEAD, HEAD), BF16),
            VMEM((w_q.shape[1] // HEAD, HEAD), BF16),
            VMEM((2, HEAD), BF16),
            VMEM((2, HEAD), BF16),
            VMEM((1, half), jnp.int32),
            VMEM((1, HEAD), F32),
            DMA((6,)),
            VMEM((rows, depth), BF16),
            DMA,
            VMEM((depth, chunks * width), BF16),
            VMEM((rows, depth), BF16),
            VMEM((rows, HEAD), F32),
            VMEM((rows, HEAD), F32),
            VMEM((chunks, half, width), BF16),
            VMEM((chunks, half, width), BF16),
            VMEM((chunks, half, width), F32),
            DMA((chunks,)),
            DMA((chunks + 1,)),
            DMA((chunks + 1,)),
        ],
        compiler_params=pltpu.CompilerParams(collective_id=0, has_side_effects=True, vmem_limit_bytes=67043328),
    )(lane_rows(gain), lane_rows(b_q), lane_rows(b_k), lane_rows(b_v), seq_lens[None, :], rotary_frequencies(), x_in, w_q, w_k, w_v)


SLOTS = 6
ROWS_STEP = 8


def attend_kernel(lens_ref, q_hbm, kv_hbm, k_hbm, v_hbm, o_ref, k_out, v_out,
                  q_ref, kv_ref, small_sems, k_buf, v_buf, q_wide, q_packed, kv_wide, o_wide, parity, scores, weights, sums, in_sems, out_sems):
    batch, kv_rows, _ = k_hbm.shape
    q_heads = q_hbm.shape[1] // HEAD
    group = q_heads // 2
    steps = batch // ROWS_STEP

    def load(step, kind):
        slot = lax.rem(step, SLOTS)
        source, target = ((k_hbm, k_buf), (v_hbm, v_buf))[kind]
        return pltpu.make_async_copy(source.at[pl.ds(step * ROWS_STEP, ROWS_STEP)], target.at[slot], in_sems.at[kind, slot])

    def save(step, kind):
        slot = lax.rem(step, SLOTS)
        source, target = ((k_buf, k_out), (v_buf, v_out))[kind]
        return pltpu.make_async_copy(source.at[slot], target.at[pl.ds(step * ROWS_STEP, ROWS_STEP)], out_sems.at[kind, slot])

    q_copy = pltpu.make_async_copy(q_hbm, q_ref, small_sems.at[0])
    kv_copy = pltpu.make_async_copy(kv_hbm, kv_ref, small_sems.at[1])
    q_copy.start()
    kv_copy.start()
    for kind in range(2):
        load(0, kind).start()

    q_wide[...] = jnp.zeros_like(q_wide)
    q_copy.wait()
    kv_copy.wait()
    for step in range(1, 3):
        for kind in range(2):
            load(step, kind).start()
    for head in range(q_heads):
        q_wide[pl.ds(head, batch, stride=QPAD), :] = q_ref[:, head * HEAD:(head + 1) * HEAD].astype(F32)
    q_packed[...] = q_wide[...].astype(BF16)
    for kind in range(2):
        for head in range(2):
            start = (kind * 2 + head) * HEAD
            kv_wide[kind, pl.ds(head, batch, stride=2), :] = kv_ref[:, start:start + HEAD].astype(F32)
    row_head = lax.broadcasted_iota(jnp.int32, (QPAD, kv_rows), 0) >= group
    col_head = lax.rem(lax.broadcasted_iota(jnp.int32, (QPAD, kv_rows), 1), 2) == 1
    parity[...] = jnp.where(row_head == col_head, 0.0, -jnp.inf)
    columns = lax.broadcasted_iota(jnp.int32, (QPAD, kv_rows), 1)
    tile_row = lax.broadcasted_iota(jnp.int32, (16, HEAD), 0)
    tile_pos = lax.div(tile_row, 2)
    tile_odd = lax.rem(tile_row, 2) == 1

    def body(step, carry):
        slot = lax.rem(step, SLOTS)

        @pl.when(step + 3 < steps)
        def _():
            @pl.when(step >= 3)
            def _():
                for kind in range(2):
                    save(step - 3, kind).wait()
            for kind in range(2):
                load(step + 3, kind).start()

        for kind in range(2):
            load(step, kind).wait()
        for row in range(ROWS_STEP):
            index = step * ROWS_STEP + row
            position = lens_ref[index]
            base = pl.multiple_of(lax.div(position, 8) * 16, 16)
            offset = lax.rem(position, 8)
            for kind, buffer in ((0, k_buf), (1, v_buf)):
                low = kv_wide[kind, pl.ds(2 * index, 1), :]
                high = kv_wide[kind, pl.ds(2 * index + 1, 1), :]
                fresh = jnp.where(tile_odd, high, low).astype(BF16)
                tile = buffer[slot, row, pl.ds(base, 16), :]
                buffer[slot, row, pl.ds(base, 16), :] = jnp.where(tile_pos == offset, fresh, tile)
        for row in range(ROWS_STEP):
            q_start = pl.multiple_of((step * ROWS_STEP + row) * QPAD, QPAD)
            scores[row] = lax.dot_general(q_packed[pl.ds(q_start, QPAD), :], k_buf[slot, row], (((1,), (1,)), ((), ())),
                                          preferred_element_type=F32)
        for kind in range(2):
            save(step, kind).start()
        for row in range(ROWS_STEP):
            limit = 2 * lens_ref[step * ROWS_STEP + row] + 2
            masked = jnp.where(columns < limit, scores[row] * HEAD ** -0.5 + parity[...], -jnp.inf)
            weight = jnp.exp(masked - jnp.max(masked, axis=1, keepdims=True))
            sums[row] = jnp.broadcast_to(jnp.sum(weight, axis=1, keepdims=True), (QPAD, HEAD))
            weights[row] = weight.astype(BF16)
        for row in range(ROWS_STEP):
            q_start = pl.multiple_of((step * ROWS_STEP + row) * QPAD, QPAD)
            mixed = jnp.dot(weights[row], v_buf[slot, row], preferred_element_type=F32)
            o_wide[pl.ds(q_start, QPAD), :] = mixed / sums[row]
        return carry

    lax.fori_loop(0, steps, body, 0)
    for head in range(q_heads):
        o_ref[:, head * HEAD:(head + 1) * HEAD] = o_wide[pl.ds(head, batch, stride=QPAD), :].astype(BF16)
    for step in range(steps - SLOTS, steps):
        for kind in range(2):
            save(step, kind).wait()


def attend(seq_lens, q_rot, kv_new, k_cache, v_cache):
    batch, seq_len, kv_heads, _ = k_cache.shape
    rows = seq_len * kv_heads
    flat = (batch, rows, HEAD)
    out, k_out, v_out = pl.pallas_call(
        attend_kernel,
        name="attend",
        out_shape=(jax.ShapeDtypeStruct(q_rot.shape, BF16), jax.ShapeDtypeStruct(flat, BF16), jax.ShapeDtypeStruct(flat, BF16)),
        in_specs=[pl.BlockSpec(memory_space=pltpu.SMEM)] + any_specs(4),
        out_specs=tuple(vmem_specs(1) + any_specs(2)),
        scratch_shapes=[
            VMEM(q_rot.shape, BF16),
            VMEM(kv_new.shape, BF16),
            DMA((2,)),
            VMEM((SLOTS, ROWS_STEP, rows, HEAD), BF16),
            VMEM((SLOTS, ROWS_STEP, rows, HEAD), BF16),
            VMEM((batch * QPAD, HEAD), F32),
            VMEM((batch * QPAD, HEAD), BF16),
            VMEM((2, batch * 2, HEAD), F32),
            VMEM((batch * QPAD, HEAD), F32),
            VMEM((QPAD, rows), F32),
            VMEM((ROWS_STEP, QPAD, rows), F32),
            VMEM((ROWS_STEP, QPAD, rows), BF16),
            VMEM((ROWS_STEP, QPAD, HEAD), F32),
            DMA((2, SLOTS)),
            DMA((2, SLOTS)),
        ],
        compiler_params=pltpu.CompilerParams(vmem_limit_bytes=64 << 20),
    )(seq_lens, q_rot, kv_new, k_cache.reshape(flat), v_cache.reshape(flat))
    return out, k_out.reshape(k_cache.shape), v_out.reshape(v_cache.shape)


BLOCK = 256
RING = 36


def tail_kernel(gain_hbm, attn_hbm, x_hbm, wo_hbm, wg_hbm, wu_hbm, wd_hbm, out_ref,
                gain_ref, gain_sem, pool, part, keep, recv_one, send_two, recv_two, x_own, mid, sq_send, sq_recv,
                h_rows, h_cols, gu_send, gu_recv, gu_own, act,
                pool_sems, x_sem, attn_sem, core_sems, rs_sems, ag_sems, gu_sems, act_sems):
    my = lax.axis_index("my")
    me = lax.axis_index("mx")
    peer = 1 - me
    side_x = my + 1 - 2 * lax.rem(my, 2)
    side_y = lax.rem(my + 2, 4)
    cross = 3 - my
    half, depth = attn_hbm.shape
    batch = 2 * half
    quarter = batch // 4
    hidden = x_hbm.shape[1]
    ff = wg_hbm.shape[0]
    col_chunks = hidden // BLOCK
    ff_chunks = pl.cdiv(ff, BLOCK)
    ff_rest = ff - (ff_chunks - 1) * BLOCK
    chunk_ring = RING // 2
    out_blocks = depth // BLOCK
    out_slot = RING - 6
    down_slot = RING - ff_chunks
    early_blocks = chunk_ring
    late_chunk = chunk_ring + chunk_ring // 2 - (down_slot // 2)
    late_count = ff_chunks - late_chunk

    def slot_rows(slot, count=BLOCK):
        return pl.ds(pl.multiple_of(slot * BLOCK, BLOCK), count)

    def block_copy(source, block, slot, count=BLOCK):
        return pltpu.make_async_copy(source.at[slot_rows(block, count)], pool.at[slot_rows(slot, count)], pool_sems.at[slot])

    def ff_slot(chunk):
        return 2 * jnp.where(chunk < chunk_ring, chunk, jnp.where(chunk < late_chunk, chunk - late_chunk + chunk_ring // 2, chunk - late_chunk))

    def ff_copies(chunk, count=BLOCK):
        slot = ff_slot(chunk)
        return block_copy(wg_hbm, chunk, slot, count), block_copy(wu_hbm, chunk, slot + 1, count)

    def down_copy(block, count=BLOCK):
        slot = down_slot + jnp.where(block < early_blocks, block + ff_chunks - early_blocks, block - early_blocks)
        return block_copy(wd_hbm, block, slot, count)

    def out_copy(block):
        return block_copy(wo_hbm, block, out_slot + block)

    def to_core(source, target, slot):
        return pltpu.make_async_remote_copy(src_ref=source, dst_ref=target, send_sem=slot[0], recv_sem=slot[1],
                                            device_id={"mx": peer}, device_id_type=MESH)

    def to_chip(source, target, chip, send_sem, recv_sem):
        return pltpu.make_async_remote_copy(src_ref=source, dst_ref=target, send_sem=send_sem, recv_sem=recv_sem,
                                            device_id={"my": chip}, device_id_type=MESH)

    own_half = pl.ds(pl.multiple_of(me * half, half), half)
    peer_half = pl.ds(pl.multiple_of(peer * half, half), half)
    rows_in = h_rows.at[:, pl.ds(0, depth)]
    full = h_rows.at[:, pl.ds(depth, depth)]
    attn_load = pltpu.make_async_copy(attn_hbm, full.at[own_half], attn_sem)
    attn_load.start()
    for block in range(2):
        out_copy(block).start()
    own_rows = pl.ds(pl.multiple_of(my * quarter, quarter), quarter)
    x_copy = pltpu.make_async_copy(x_hbm.at[own_rows], x_own, x_sem)
    x_copy.start()
    gain_copy = pltpu.make_async_copy(gain_hbm, gain_ref, gain_sem)
    gain_copy.start()

    barrier = pltpu.get_barrier_semaphore()
    pl.semaphore_signal(barrier, inc=1, device_id={"mx": peer}, device_id_type=MESH)
    pl.semaphore_signal(barrier, inc=1, device_id={"my": side_x}, device_id_type=MESH)
    pl.semaphore_signal(barrier, inc=1, device_id={"my": side_y}, device_id_type=MESH)
    attn_load.wait()
    for block in range(2, out_blocks):
        out_copy(block).start()
    pl.semaphore_wait(barrier, 3)
    attn_copy = to_core(full.at[own_half], full.at[own_half], (core_sems.at[0], core_sems.at[1]))
    attn_copy.start()
    attn_copy.wait()
    for place, owner in enumerate((my, side_x, cross, side_y)):
        rows_in[place * quarter:(place + 1) * quarter, :] = full[pl.ds(pl.multiple_of(owner * quarter, quarter), quarter), :]

    sub = quarter // 2
    wide = 2 * BLOCK
    pairs = hidden // wide

    def wide_cols(pair):
        if isinstance(pair, int):
            return slice(pair * wide, (pair + 1) * wide)
        return pl.ds(pl.multiple_of(pair * wide, wide), wide)

    def first_side(parity):
        return side_x + parity * (side_y - side_x)

    def second_side(parity):
        return side_y + parity * (side_x - side_y)

    def sub_rows(index):
        if isinstance(index, int):
            return slice(index * sub, (index + 1) * sub)
        return pl.ds(pl.multiple_of(index * sub, sub), sub)

    def scatter_one(chunk, parity):
        lead = pl.ds(pl.multiple_of(sub * (1 + parity), sub), 2 * sub)
        return to_chip(part.at[chunk, lead], recv_one.at[chunk], first_side(parity), rs_sems.at[0, 0, chunk], rs_sems.at[0, 1, chunk])

    def scatter_two(chunk, parity):
        return to_chip(send_two.at[chunk], recv_two.at[chunk], second_side(parity), rs_sems.at[1, 0, chunk], rs_sems.at[1, 1, chunk])

    def scatter_store(pair, total):
        for block in range(2):
            chunk = 2 * pair + block
            pieces = [total[place * quarter + block * sub:place * quarter + (block + 1) * sub] for place in range(4)]
            for place in range(1, 4):
                part[chunk, sub_rows(place), :] = pieces[place].astype(BF16)
            keep[chunk, 0] = pieces[0]
            keep[chunk, 1] = pieces[1]
            keep[chunk, 2] = pieces[3]

    def scatter_pass(chunk, parity):
        scatter_one(chunk, parity).wait()
        send_two[chunk] = (keep[chunk, 2 - parity] + recv_one[chunk, sub_rows(1 - parity), :].astype(F32)).astype(BF16)
        scatter_two(chunk, parity).start()
        keep[chunk, 0] = keep[chunk, 0] + recv_one[chunk, sub_rows(parity), :].astype(F32)

    def scatter_end(chunk, parity):
        scatter_two(chunk, parity).wait()
        return keep[chunk, 0] + recv_two[chunk].astype(F32)

    def turn(pair, block):
        return (pair + block) % 2

    def mid_end(pair, block):
        before = x_own[sub_rows(block), wide_cols(pair)].astype(F32)
        mid[sub_rows(block), wide_cols(pair)] = (before + scatter_end(2 * pair + block, turn(pair, block))).astype(BF16).astype(F32)

    x_copy.wait()
    gain_copy.wait()
    for block in range(out_blocks):
        out_copy(block).wait()
    for chunk in range(out_slot // 2):
        for copy in ff_copies(chunk):
            copy.start()
    def out_product(pair, carry):
        weights = pool[out_slot * BLOCK:out_slot * BLOCK + depth, wide_cols(pair)]
        scatter_store(pair, jnp.dot(rows_in[...], weights, preferred_element_type=F32))
        scatter_one(2 * pair, lax.rem(pair, 2)).start()
        return carry

    lax.fori_loop(0, pairs, out_product, 0)
    gains = gain_ref[...].astype(F32)

    def square_copy(block):
        return to_core(sq_send.at[sub_rows(block)], sq_recv.at[sub_rows(block)], (core_sems.at[2 + 2 * block], core_sems.at[3 + 2 * block]))

    def square_start(block):
        square = jnp.zeros((sub, HEAD), F32)
        for start in range(0, hidden, HEAD):
            value = mid[sub_rows(block), start:start + HEAD]
            square = square + value * value
        sq_send[sub_rows(block), :] = jnp.broadcast_to(jnp.sum(square, axis=1, keepdims=True), (sub, HEAD))
        square_copy(block).start()

    def norm_rows(block):
        square_copy(block).wait()
        scale = lax.rsqrt((sq_send[sub_rows(block), :] + sq_recv[sub_rows(block), :]) / (2 * hidden) + NORM_EPS)
        for start in range(0, hidden, HEAD):
            gain = gains[start // HEAD:start // HEAD + 1, :]
            h_rows[sub_rows(block), start:start + HEAD] = (mid[sub_rows(block), start:start + HEAD] * scale * gain).astype(BF16)

    def h_block(place, pair, block):
        return h_rows.at[sub_rows(2 * place + block), wide_cols(pair)]

    def gather_x(pair, block):
        chunk = 2 * pair + block
        return to_chip(h_block(0, pair, block), h_block(1, pair, block), side_x, ag_sems.at[0, 0, chunk], ag_sems.at[0, 1, chunk])

    def gather_y(pair, block):
        chunk = 2 * pair + block
        return to_chip(h_block(0, pair, block), h_block(3, pair, block), side_y, ag_sems.at[1, 0, chunk], ag_sems.at[1, 1, chunk])

    def gather_cross(pair, block):
        chunk = 2 * pair + block
        source = 1 if turn(pair, block) == 0 else 3
        return to_chip(h_block(source, pair, block), h_block(2, pair, block), second_side(turn(pair, block)),
                       ag_sems.at[2, 0, chunk], ag_sems.at[2, 1, chunk])

    def gather_send(pair, block):
        gather_x(pair, block).start()
        gather_y(pair, block).start()

    def gather_pass(pair, block):
        (gather_y if turn(pair, block) else gather_x)(pair, block).wait_recv()
        gather_cross(pair, block).start()

    def start_late(pair):
        scatter_one(2 * pair + 1, turn(pair, 1)).start()

    def pass_late(pair):
        scatter_pass(2 * pair + 1, turn(pair, 1))

    for pair in range(2):
        start_late(pair)
    for chunk in range(out_slot // 2, chunk_ring):
        for copy in ff_copies(chunk):
            copy.start()
    for pair in range(pairs):
        scatter_pass(2 * pair, turn(pair, 0))
        if 1 <= pair < pairs - 1:
            start_late(pair + 1)
    for pair in range(2):
        pass_late(pair)
    for pair in range(pairs):
        mid_end(pair, 0)
    square_start(0)
    norm_rows(0)
    for pair in range(2):
        gather_send(pair, 0)
    for pair in range(2, pairs):
        pass_late(pair)
    for pair in range(2, pairs):
        gather_send(pair, 0)
    for pair in range(pairs):
        mid_end(pair, 1)
    square_start(1)
    for pair in range(2):
        gather_pass(pair, 0)
    norm_rows(1)
    for pair in range(pairs):
        gather_send(pair, 1)
    for pair in range(2, pairs):
        gather_pass(pair, 0)
    for pair in range(pairs):
        gather_pass(pair, 1)
    for pair in range(pairs):
        for block in range(2):
            (gather_x if turn(pair, block) else gather_y)(pair, block).wait_recv()
            gather_cross(pair, block).wait_recv()
        for place, source in enumerate((own_half, peer_half)):
            h_cols[wide_cols(pair), place * half:(place + 1) * half] = h_rows[source, wide_cols(pair)].astype(F32).T.astype(BF16)
        for block in range(2):
            gather_x(pair, block).wait_send()
            gather_y(pair, block).wait_send()
            gather_cross(pair, block).wait_send()

    def gu_copy(chunk):
        slot = lax.rem(chunk, 8)
        return to_core(gu_send.at[slot], gu_recv.at[slot], (gu_sems.at[0, slot], gu_sems.at[1, slot]))

    def act_lanes(chunk):
        place = jnp.where(chunk < early_blocks, chunk + ff_chunks - early_blocks, chunk - early_blocks)
        return pl.ds(pl.multiple_of(place * BLOCK, BLOCK), BLOCK)

    def act_copy(chunk):
        lanes = act_lanes(chunk)
        return to_core(act.at[own_half, lanes], act.at[own_half, lanes], (act_sems.at[0, lax.rem(chunk, 8)], act_sems.at[1, lax.rem(chunk, 8)]))

    def ff_products(chunk):
        slot = lax.rem(chunk, 8)
        base = ff_slot(chunk)
        product = jnp.dot(pool[slot_rows(base, 2 * BLOCK), :], h_cols[...], preferred_element_type=F32)
        for kind in range(2):
            rows = slice(kind * BLOCK, (kind + 1) * BLOCK)
            gu_own[slot, kind] = product[rows, :half]
            gu_send[slot, kind] = product[rows, half:].astype(BF16)

    def activate(chunk):
        slot = lax.rem(chunk, 8)
        gate = gu_own[slot, 0] + gu_recv[slot, 0].astype(F32)
        up = gu_own[slot, 1] + gu_recv[slot, 1].astype(F32)
        value = gate * jax.nn.sigmoid(gate) * up
        row = chunk * BLOCK + lax.broadcasted_iota(jnp.int32, value.shape, 0)
        value = jnp.where(row < ff, value, 0.0)
        lanes = act_lanes(chunk)
        act[own_half, lanes] = value.T.astype(BF16)

    def refill(chunk):
        half_ring = chunk_ring // 2

        @pl.when(chunk < late_count - 1)
        def _():
            for copy in ff_copies(late_chunk + chunk):
                copy.start()

        @pl.when(chunk == late_count - 1)
        def _():
            for copy in ff_copies(ff_chunks - 1, ff_rest):
                copy.start()

        @pl.when((chunk >= late_count) & (chunk < half_ring))
        def _():
            for copy in ff_copies(chunk - late_count + chunk_ring):
                copy.start()

        @pl.when((chunk >= half_ring) & (chunk < chunk_ring))
        def _():
            down_copy(2 * (chunk - half_ring)).start()
            down_copy(2 * (chunk - half_ring) + 1).start()

        free = 2 * (chunk - chunk_ring + late_count) - down_slot + early_blocks

        @pl.when((chunk >= chunk_ring) & (chunk < late_chunk) & (free >= early_blocks))
        def _():
            down_copy(free).start()

        @pl.when((chunk >= chunk_ring) & (chunk < late_chunk - 1))
        def _():
            down_copy(free + 1).start()

        @pl.when(chunk == late_chunk - 1)
        def _():
            down_copy(ff_chunks - 1, ff_rest).start()

    def ff_pair(pair, active):
        chunks = (2 * pair, 2 * pair + 1)
        if active:
            for chunk in chunks:
                gu_copy(chunk - 4).wait()
        for chunk in chunks:
            for copy in ff_copies(chunk):
                copy.wait()
        if active:
            for chunk in chunks:
                activate(chunk - 4)
        for chunk in chunks:
            ff_products(chunk)
        for chunk in chunks:
            gu_copy(chunk).start()
        if active:
            for chunk in chunks:
                act_copy(chunk - 4).start()
        for chunk in chunks:
            refill(chunk)

    def ff_first(pair, carry):
        ff_pair(pair, False)
        return carry

    def ff_step(pair, carry):
        @pl.when(pair >= 4)
        def _():
            for parity in range(2):
                act_copy(2 * (pair - 4) + parity).wait()
        ff_pair(pair, True)
        return carry

    last = ff_chunks - 1
    ff_pairs = last // 2
    lax.fori_loop(0, 2, ff_first, 0)
    lax.fori_loop(2, ff_pairs, ff_step, 0)

    def finish(chunk):
        gu_copy(chunk).wait()
        activate(chunk)
        act_copy(chunk).start()

    for chunk in range(2 * ff_pairs - 8, 2 * ff_pairs - 6):
        act_copy(chunk).wait()

    def ff_last(chunk, carry):
        for copy in ff_copies(chunk, ff_rest):
            copy.wait()
        ff_products(chunk)
        gu_copy(chunk).start()
        return carry

    lax.fori_loop(last, last + 1, ff_last, 0)
    for chunk in range(last - 4, last - 2):
        finish(chunk)
    for block in range(early_blocks):
        down_copy(block).wait()
    late_lanes = (ff_chunks - early_blocks) * BLOCK
    late_row = down_slot * BLOCK + late_lanes

    early_slot = 3

    def down_early(pair, carry):
        value = jnp.dot(act[:, late_lanes:], pool[late_row:, wide_cols(pair)], preferred_element_type=F32)
        for piece in range(4):
            gu_own[early_slot + 2 * pair + piece // 2, piece % 2] = value[:, piece * half:(piece + 1) * half]
        return carry

    lax.fori_loop(0, 1, down_early, 0)
    for chunk in range(last - 2, ff_chunks):
        finish(chunk)
    lax.fori_loop(1, 2, down_early, 0)
    for block in range(early_blocks, ff_chunks):
        down_copy(block, ff_rest if block == last else BLOCK).wait()
    for chunk in range(2 * ff_pairs - 6, ff_chunks):
        act_copy(chunk).wait()

    def out_block(owner, chunk):
        pair, block = chunk // 2, chunk % 2
        return out_ref.at[sub_rows(2 * owner + block), wide_cols(pair)]

    def final_x(chunk):
        target = out_block(my, chunk)
        return to_chip(target, target, side_x, ag_sems.at[0, 0, chunk], ag_sems.at[0, 1, chunk])

    def final_y(chunk):
        target = out_block(my, chunk)
        return to_chip(target, target, side_y, ag_sems.at[1, 0, chunk], ag_sems.at[1, 1, chunk])

    def final_cross(chunk):
        target = out_block(first_side(chunk % 2), chunk)
        return to_chip(target, target, second_side(chunk % 2), ag_sems.at[2, 0, chunk], ag_sems.at[2, 1, chunk])

    def out_end(chunk):
        pair, block = chunk // 2, chunk % 2
        value = mid[sub_rows(block), wide_cols(pair)] + scatter_end(chunk, block)
        out_ref[sub_rows(2 * my + block), wide_cols(pair)] = value.astype(BF16)
        final_x(chunk).start()
        final_y(chunk).start()

    def out_pass(chunk):
        (final_x if chunk % 2 == 0 else final_y)(chunk).wait_recv()
        final_cross(chunk).start()

    def scatter_start(pair, total):
        scatter_store(pair, total)
        for block in range(2):
            scatter_one(2 * pair + block, block).start()

    def down_rest(pair, carry):
        total = jnp.dot(act[:, :late_lanes], pool[down_slot * BLOCK:late_row, wide_cols(pair)], preferred_element_type=F32)
        pieces = [gu_own[early_slot + 2 * pair + piece // 2, piece % 2] for piece in range(4)]
        scatter_start(pair, jnp.concatenate(pieces, axis=1) + total)
        return carry

    def down_pair(pair, carry):
        scatter_start(pair, jnp.dot(act[...], pool[down_slot * BLOCK:, wide_cols(pair)], preferred_element_type=F32))

        @pl.when(pair >= 3)
        def _():
            for parity in range(2):
                scatter_pass(2 * (pair - 3) + parity, parity)
        return carry

    lax.fori_loop(0, 2, down_rest, 0)
    lax.fori_loop(2, pairs, down_pair, 0)

    def each(step, pair):
        for chunk in (2 * pair, 2 * pair + 1):
            if step is scatter_pass:
                step(chunk, chunk % 2)
            else:
                step(chunk)

    for pair in range(pairs - 3, pairs):
        each(scatter_pass, pair)
        each(out_end, pair - pairs + 3)
    each(out_pass, 0)
    for pair in range(3, pairs):
        each(out_end, pair)
        each(out_pass, pair - 2)
    for pair in range(pairs - 2, pairs):
        each(out_pass, pair)
    for chunk in range(col_chunks):
        (final_y if chunk % 2 == 0 else final_x)(chunk).wait_recv()
        final_cross(chunk).wait_recv()
    for chunk in range(col_chunks):
        final_cross(chunk).wait_send()
        final_x(chunk).wait_send()
        final_y(chunk).wait_send()


def tail(attn_rows, gain, x_in, w_o, wg_rows, wu_rows, w_down):
    half, depth = attn_rows.shape
    rows, hidden = x_in.shape
    quarter = rows // 4
    chunks = hidden // BLOCK
    ff_chunks = pl.cdiv(w_down.shape[0], BLOCK)
    return pl.pallas_call(
        tail_kernel,
        name="tail",
        out_shape=jax.ShapeDtypeStruct((rows, hidden), BF16),
        in_specs=any_specs(7),
        out_specs=vmem_specs(1)[0],
        scratch_shapes=[
            VMEM((hidden // HEAD, HEAD), BF16),
            DMA,
            VMEM((RING * BLOCK, hidden), BF16),
            VMEM((chunks, 2 * quarter, 2 * BLOCK), BF16),
            VMEM((chunks, 3, quarter // 2, 2 * BLOCK), F32),
            VMEM((chunks, quarter, 2 * BLOCK), BF16),
            VMEM((chunks, quarter // 2, 2 * BLOCK), BF16),
            VMEM((chunks, quarter // 2, 2 * BLOCK), BF16),
            VMEM((quarter, hidden), BF16),
            VMEM((quarter, hidden), F32),
            VMEM((quarter, HEAD), F32),
            VMEM((quarter, HEAD), F32),
            VMEM((rows, hidden), BF16),
            VMEM((hidden, rows), BF16),
            VMEM((8, 2, BLOCK, half), BF16),
            VMEM((8, 2, BLOCK, half), BF16),
            VMEM((8, 2, BLOCK, half), F32),
            VMEM((rows, ff_chunks * BLOCK), BF16),
            DMA((RING,)),
            DMA,
            DMA,
            DMA((6,)),
            DMA((2, 2, chunks)),
            DMA((3, 2, chunks)),
            DMA((2, 8)),
            DMA((2, 8)),
        ],
        compiler_params=pltpu.CompilerParams(collective_id=1, has_side_effects=True, vmem_limit_bytes=67043328),
    )(lane_rows(gain), attn_rows, x_in, w_o, wg_rows, wu_rows, w_down)


def solution(mesh):
    act_spec = P(None, "mx")
    cache_spec = P("mx", None, "my", None)
    in_specs = (act_spec, P("mx"), P("mx"), P("mx"), P("mx", "my"), P("my"), P("mx", "my"), P("my"), P("mx", "my"), P("my"), P("my", "mx"), P("mx", "my"), P("mx", "my"), P("my", "mx"), cache_spec, cache_spec)
    out_specs = (act_spec, cache_spec, cache_spec)

    def local_layer(x_in, seq_lens, gain_attn, gain_mlp, w_q, b_q, w_k, b_k, w_v, b_v, w_o, w_gate, w_up, w_down, k_cache, v_cache):
        q_rot, kv_new = project(x_in, seq_lens, gain_attn, b_q, b_k, b_v, w_q, w_k, w_v)
        attn_rows, k_cache_out, v_cache_out = attend(seq_lens, q_rot, kv_new, k_cache, v_cache)
        x_out = tail(attn_rows, gain_mlp, x_in, w_o, w_gate.T, w_up.T, w_down)
        return x_out, k_cache_out, v_cache_out

    return jax.shard_map(local_layer, mesh=mesh, in_specs=in_specs, out_specs=out_specs, check_vma=False)
```

```python
import jax
import jax.numpy as jnp
import numpy as np
from jax import lax
from jax.experimental import pallas as pl
from jax.experimental.pallas import tpu as pltpu
from jax.sharding import PartitionSpec as P

HEAD = 128
NORM_EPS = 1e-6
ROPE_THETA = 1000000.0
MESH = pl.DeviceIdType.MESH
F32 = jnp.float32
BF16 = jnp.bfloat16
QPAD = 16
VMEM = pltpu.VMEM
DMA = pltpu.SemaphoreType.DMA


def any_specs(count):
    return [pl.BlockSpec(memory_space=pl.ANY)] * count


def vmem_specs(count):
    return [pl.BlockSpec(memory_space=pltpu.VMEM)] * count


def lane_rows(vector):
    return vector.reshape(-1, HEAD)


def rotary_frequencies():
    half_dim = HEAD // 2
    inv_freq = np.float32(ROPE_THETA) ** (np.float32(-2.0) * np.arange(half_dim, dtype=np.float32) / np.float32(HEAD))
    return jnp.asarray(np.concatenate([inv_freq, inv_freq])[None, :], F32)


def project_kernel(gain_hbm, bq_hbm, bk_hbm, bv_hbm, lens_hbm, freq_hbm, x_hbm, wq_hbm, wk_hbm, wv_hbm, q_out, kv_out,
                   gain_ref, bq_ref, bk_ref, bv_ref, lens_ref, freq_ref, small_sems, x_ref, x_sem, w_buf, normed, sq_send, sq_recv, part_send, part_recv, part_own, w_sems, send_sems, recv_sems):
    me = lax.axis_index("mx")
    peer = 1 - me
    rows, depth = x_hbm.shape
    half = rows // 2
    width = 2 * HEAD
    q_chunks = wq_hbm.shape[1] // width
    chunks = q_chunks + 2

    def weight_copy(index):
        if index < q_chunks:
            source = wq_hbm.at[:, pl.ds(index * width, width)]
        else:
            source = (wk_hbm, wv_hbm)[index - q_chunks]
        return pltpu.make_async_copy(source, w_buf.at[:, pl.ds(index * width, width)], w_sems.at[index])

    def weight_wait(index):
        lanes = pl.ds(pl.multiple_of(index * width, width), width)
        pltpu.make_async_copy(wk_hbm, w_buf.at[:, lanes], w_sems.at[index]).wait()

    smalls = [pltpu.make_async_copy(source, target, small_sems.at[slot]) for slot, (source, target) in enumerate((
        (lens_hbm, lens_ref), (freq_hbm, freq_ref), (gain_hbm, gain_ref), (bq_hbm, bq_ref), (bk_hbm, bk_ref), (bv_hbm, bv_ref)))]
    for copy in smalls:
        copy.start()
    x_copy = pltpu.make_async_copy(x_hbm, x_ref, x_sem)
    x_copy.start()
    barrier = pltpu.get_barrier_semaphore()
    pl.semaphore_signal(barrier, inc=1, device_id={"mx": peer}, device_id_type=MESH)

    for copy in smalls:
        copy.wait()
    positions = jnp.broadcast_to(lens_ref[...].astype(F32), (half, half)).T
    angles = positions * freq_ref[...]
    cos_tab = jnp.cos(angles)
    lane = lax.broadcasted_iota(jnp.int32, (half, HEAD), 1)
    sin_tab = jnp.where(lane < HEAD // 2, -1.0, 1.0) * jnp.sin(angles)

    x_copy.wait()
    for index in range(chunks):
        weight_copy(index).start()
    total = jnp.zeros((rows, HEAD), F32)
    for start in range(0, depth, HEAD):
        block = x_ref[:, start:start + HEAD].astype(F32)
        total = total + block * block
    sq_own = jnp.sum(total, axis=1, keepdims=True)
    sq_send[...] = jnp.broadcast_to(sq_own, (rows, HEAD))
    pl.semaphore_wait(barrier, 1)

    def remote(source, target, slot):
        return pltpu.make_async_remote_copy(
            src_ref=source, dst_ref=target, send_sem=send_sems.at[slot], recv_sem=recv_sems.at[slot],
            device_id={"mx": peer}, device_id_type=MESH)

    sq_copy = remote(sq_send, sq_recv, chunks)
    sq_copy.start()
    sq_copy.wait()
    own_rows = pl.ds(pl.multiple_of(me * half, half), half)
    peer_rows = pl.ds(pl.multiple_of(peer * half, half), half)
    scale = lax.rsqrt((sq_send[...] + sq_recv[...]) / (2 * depth) + NORM_EPS)
    gains = gain_ref[...].astype(F32)
    for start in range(0, depth, HEAD):
        block = x_ref[:, start:start + HEAD].astype(F32)
        gain = gains[start // HEAD:start // HEAD + 1, :]
        value = (block * scale * gain).astype(BF16)
        normed[own_rows, start:start + HEAD] = value[:half]
        normed[peer_rows, start:start + HEAD] = value[half:]

    def part_copy(index):
        return remote(part_send.at[index], part_recv.at[index], index)

    def multiply(first, count):
        for index in range(count):
            weight_wait(first + index)
        lanes = pl.ds(pl.multiple_of(first * width, width), count * width)
        product = jnp.dot(normed[...], w_buf[:, lanes], preferred_element_type=F32)
        for index in range(count):
            value = product[:, index * width:(index + 1) * width]
            part_own[first + index] = value[:half]
            part_send[first + index] = value[half:].astype(BF16)
        for index in range(count):
            part_copy(first + index).start()

    def multiply_pair(pair, carry):
        multiply(2 * pair, 2)
        return carry

    def multiply_last(index, carry):
        multiply(index, 1)
        return carry

    lax.fori_loop(0, chunks // 2, multiply_pair, 0)
    lax.fori_loop(chunks - chunks % 2, chunks, multiply_last, 0)
    biases = [ref[...].astype(F32) for ref in (bq_ref, bk_ref, bv_ref)]
    for index in range(chunks):
        part_copy(index).wait()
        for head in range(2):
            lanes = slice(head * HEAD, (head + 1) * HEAD)
            columns = slice(index * width + head * HEAD, index * width + (head + 1) * HEAD)
            if index < q_chunks:
                bias = biases[0][2 * index + head:2 * index + head + 1, :]
            else:
                bias = biases[index - q_chunks + 1][head:head + 1, :]
            value = part_own[index][:, lanes] + part_recv[index][:, lanes].astype(F32) + bias
            if index < chunks - 1:
                value = value * cos_tab + pltpu.roll(value, HEAD // 2, 1) * sin_tab
            if index < q_chunks:
                q_out[:, columns] = value.astype(BF16)
            else:
                kv_out[:, (index - q_chunks) * width + head * HEAD:(index - q_chunks) * width + (head + 1) * HEAD] = value.astype(BF16)


def project(x_in, seq_lens, gain, b_q, b_k, b_v, w_q, w_k, w_v):
    rows, depth = x_in.shape
    half = rows // 2
    width = 2 * HEAD
    chunks = w_q.shape[1] // width + 2
    return pl.pallas_call(
        project_kernel,
        name="project",
        out_shape=(jax.ShapeDtypeStruct((half, w_q.shape[1]), BF16), jax.ShapeDtypeStruct((half, 2 * width), BF16)),
        in_specs=any_specs(10),
        out_specs=tuple(vmem_specs(2)),
        scratch_shapes=[
            VMEM((depth // HEAD, HEAD), BF16),
            VMEM((w_q.shape[1] // HEAD, HEAD), BF16),
            VMEM((2, HEAD), BF16),
            VMEM((2, HEAD), BF16),
            VMEM((1, half), jnp.int32),
            VMEM((1, HEAD), F32),
            DMA((6,)),
            VMEM((rows, depth), BF16),
            DMA,
            VMEM((depth, chunks * width), BF16),
            VMEM((rows, depth), BF16),
            VMEM((rows, HEAD), F32),
            VMEM((rows, HEAD), F32),
            VMEM((chunks, half, width), BF16),
            VMEM((chunks, half, width), BF16),
            VMEM((chunks, half, width), F32),
            DMA((chunks,)),
            DMA((chunks + 1,)),
            DMA((chunks + 1,)),
        ],
        compiler_params=pltpu.CompilerParams(collective_id=0, has_side_effects=True, vmem_limit_bytes=67043328),
    )(lane_rows(gain), lane_rows(b_q), lane_rows(b_k), lane_rows(b_v), seq_lens[None, :], rotary_frequencies(), x_in, w_q, w_k, w_v)


SLOTS = 6
ROWS_STEP = 8


def attend_kernel(lens_ref, q_hbm, kv_hbm, k_hbm, v_hbm, o_ref, k_out, v_out,
                  q_ref, kv_ref, small_sems, k_buf, v_buf, q_wide, q_packed, kv_wide, o_wide, parity, scores, weights, sums, in_sems, out_sems):
    batch, kv_rows, _ = k_hbm.shape
    q_heads = q_hbm.shape[1] // HEAD
    group = q_heads // 2
    steps = batch // ROWS_STEP

    def load(step, kind):
        slot = lax.rem(step, SLOTS)
        source, target = ((k_hbm, k_buf), (v_hbm, v_buf))[kind]
        return pltpu.make_async_copy(source.at[pl.ds(step * ROWS_STEP, ROWS_STEP)], target.at[slot], in_sems.at[kind, slot])

    def save(step, kind):
        slot = lax.rem(step, SLOTS)
        source, target = ((k_buf, k_out), (v_buf, v_out))[kind]
        return pltpu.make_async_copy(source.at[slot], target.at[pl.ds(step * ROWS_STEP, ROWS_STEP)], out_sems.at[kind, slot])

    q_copy = pltpu.make_async_copy(q_hbm, q_ref, small_sems.at[0])
    kv_copy = pltpu.make_async_copy(kv_hbm, kv_ref, small_sems.at[1])
    q_copy.start()
    kv_copy.start()
    for kind in range(2):
        load(0, kind).start()

    q_wide[...] = jnp.zeros_like(q_wide)
    q_copy.wait()
    kv_copy.wait()
    for step in range(1, 3):
        for kind in range(2):
            load(step, kind).start()
    for head in range(q_heads):
        q_wide[pl.ds(head, batch, stride=QPAD), :] = q_ref[:, head * HEAD:(head + 1) * HEAD].astype(F32)
    q_packed[...] = q_wide[...].astype(BF16)
    for kind in range(2):
        for head in range(2):
            start = (kind * 2 + head) * HEAD
            kv_wide[kind, pl.ds(head, batch, stride=2), :] = kv_ref[:, start:start + HEAD].astype(F32)
    row_head = lax.broadcasted_iota(jnp.int32, (QPAD, kv_rows), 0) >= group
    col_head = lax.rem(lax.broadcasted_iota(jnp.int32, (QPAD, kv_rows), 1), 2) == 1
    parity[...] = jnp.where(row_head == col_head, 0.0, -jnp.inf)
    columns = lax.broadcasted_iota(jnp.int32, (QPAD, kv_rows), 1)
    tile_row = lax.broadcasted_iota(jnp.int32, (16, HEAD), 0)
    tile_pos = lax.div(tile_row, 2)
    tile_odd = lax.rem(tile_row, 2) == 1

    def body(step, carry):
        slot = lax.rem(step, SLOTS)

        @pl.when(step + 3 < steps)
        def _():
            @pl.when(step >= 3)
            def _():
                for kind in range(2):
                    save(step - 3, kind).wait()
            for kind in range(2):
                load(step + 3, kind).start()

        for kind in range(2):
            load(step, kind).wait()
        for row in range(ROWS_STEP):
            index = step * ROWS_STEP + row
            position = lens_ref[index]
            base = pl.multiple_of(lax.div(position, 8) * 16, 16)
            offset = lax.rem(position, 8)
            for kind, buffer in ((0, k_buf), (1, v_buf)):
                low = kv_wide[kind, pl.ds(2 * index, 1), :]
                high = kv_wide[kind, pl.ds(2 * index + 1, 1), :]
                fresh = jnp.where(tile_odd, high, low).astype(BF16)
                tile = buffer[slot, row, pl.ds(base, 16), :]
                buffer[slot, row, pl.ds(base, 16), :] = jnp.where(tile_pos == offset, fresh, tile)
        for row in range(ROWS_STEP):
            q_start = pl.multiple_of((step * ROWS_STEP + row) * QPAD, QPAD)
            scores[row] = lax.dot_general(q_packed[pl.ds(q_start, QPAD), :], k_buf[slot, row], (((1,), (1,)), ((), ())),
                                          preferred_element_type=F32)
        for kind in range(2):
            save(step, kind).start()
        for row in range(ROWS_STEP):
            limit = 2 * lens_ref[step * ROWS_STEP + row] + 2
            masked = jnp.where(columns < limit, scores[row] * HEAD ** -0.5 + parity[...], -jnp.inf)
            weight = jnp.exp(masked - jnp.max(masked, axis=1, keepdims=True))
            sums[row] = jnp.broadcast_to(jnp.sum(weight, axis=1, keepdims=True), (QPAD, HEAD))
            weights[row] = weight.astype(BF16)
        for row in range(ROWS_STEP):
            q_start = pl.multiple_of((step * ROWS_STEP + row) * QPAD, QPAD)
            mixed = jnp.dot(weights[row], v_buf[slot, row], preferred_element_type=F32)
            o_wide[pl.ds(q_start, QPAD), :] = mixed / sums[row]
        return carry

    lax.fori_loop(0, steps, body, 0)
    for head in range(q_heads):
        o_ref[:, head * HEAD:(head + 1) * HEAD] = o_wide[pl.ds(head, batch, stride=QPAD), :].astype(BF16)
    for step in range(steps - SLOTS, steps):
        for kind in range(2):
            save(step, kind).wait()


def attend(seq_lens, q_rot, kv_new, k_cache, v_cache):
    batch, seq_len, kv_heads, _ = k_cache.shape
    rows = seq_len * kv_heads
    flat = (batch, rows, HEAD)
    out, k_out, v_out = pl.pallas_call(
        attend_kernel,
        name="attend",
        out_shape=(jax.ShapeDtypeStruct(q_rot.shape, BF16), jax.ShapeDtypeStruct(flat, BF16), jax.ShapeDtypeStruct(flat, BF16)),
        in_specs=[pl.BlockSpec(memory_space=pltpu.SMEM)] + any_specs(4),
        out_specs=tuple(vmem_specs(1) + any_specs(2)),
        scratch_shapes=[
            VMEM(q_rot.shape, BF16),
            VMEM(kv_new.shape, BF16),
            DMA((2,)),
            VMEM((SLOTS, ROWS_STEP, rows, HEAD), BF16),
            VMEM((SLOTS, ROWS_STEP, rows, HEAD), BF16),
            VMEM((batch * QPAD, HEAD), F32),
            VMEM((batch * QPAD, HEAD), BF16),
            VMEM((2, batch * 2, HEAD), F32),
            VMEM((batch * QPAD, HEAD), F32),
            VMEM((QPAD, rows), F32),
            VMEM((ROWS_STEP, QPAD, rows), F32),
            VMEM((ROWS_STEP, QPAD, rows), BF16),
            VMEM((ROWS_STEP, QPAD, HEAD), F32),
            DMA((2, SLOTS)),
            DMA((2, SLOTS)),
        ],
        compiler_params=pltpu.CompilerParams(vmem_limit_bytes=64 << 20),
    )(seq_lens, q_rot, kv_new, k_cache.reshape(flat), v_cache.reshape(flat))
    return out, k_out.reshape(k_cache.shape), v_out.reshape(v_cache.shape)


BLOCK = 256
RING = 36


def tail_kernel(gain_hbm, attn_hbm, x_hbm, wo_hbm, wg_hbm, wu_hbm, wd_hbm, out_ref,
                gain_ref, gain_sem, pool, part, keep, recv_one, send_two, recv_two, x_own, mid, sq_send, sq_recv,
                h_rows, h_cols, gu_send, gu_recv, gu_own, act,
                pool_sems, x_sem, attn_sem, core_sems, rs_sems, ag_sems, gu_sems, act_sems):
    my = lax.axis_index("my")
    me = lax.axis_index("mx")
    peer = 1 - me
    side_x = my + 1 - 2 * lax.rem(my, 2)
    side_y = lax.rem(my + 2, 4)
    cross = 3 - my
    half, depth = attn_hbm.shape
    batch = 2 * half
    quarter = batch // 4
    hidden = x_hbm.shape[1]
    ff = wg_hbm.shape[0]
    col_chunks = hidden // BLOCK
    ff_chunks = pl.cdiv(ff, BLOCK)
    ff_rest = ff - (ff_chunks - 1) * BLOCK
    chunk_ring = RING // 2
    out_blocks = depth // BLOCK
    out_slot = RING - 6
    down_slot = RING - ff_chunks
    early_blocks = chunk_ring
    late_chunk = chunk_ring + chunk_ring // 2 - (down_slot // 2)
    late_count = ff_chunks - late_chunk

    def slot_rows(slot, count=BLOCK):
        return pl.ds(pl.multiple_of(slot * BLOCK, BLOCK), count)

    def block_copy(source, block, slot, count=BLOCK):
        return pltpu.make_async_copy(source.at[slot_rows(block, count)], pool.at[slot_rows(slot, count)], pool_sems.at[slot])

    def ff_slot(chunk):
        return 2 * jnp.where(chunk < chunk_ring, chunk, jnp.where(chunk < late_chunk, chunk - late_chunk + chunk_ring // 2, chunk - late_chunk))

    def ff_copies(chunk, count=BLOCK):
        slot = ff_slot(chunk)
        return block_copy(wg_hbm, chunk, slot, count), block_copy(wu_hbm, chunk, slot + 1, count)

    def down_copy(block, count=BLOCK):
        slot = down_slot + jnp.where(block < early_blocks, block + ff_chunks - early_blocks, block - early_blocks)
        return block_copy(wd_hbm, block, slot, count)

    def out_copy(block):
        return block_copy(wo_hbm, block, out_slot + block)

    def to_core(source, target, slot):
        return pltpu.make_async_remote_copy(src_ref=source, dst_ref=target, send_sem=slot[0], recv_sem=slot[1],
                                            device_id={"mx": peer}, device_id_type=MESH)

    def to_chip(source, target, chip, send_sem, recv_sem):
        return pltpu.make_async_remote_copy(src_ref=source, dst_ref=target, send_sem=send_sem, recv_sem=recv_sem,
                                            device_id={"my": chip}, device_id_type=MESH)

    own_half = pl.ds(pl.multiple_of(me * half, half), half)
    peer_half = pl.ds(pl.multiple_of(peer * half, half), half)
    rows_in = h_rows.at[:, pl.ds(0, depth)]
    full = h_rows.at[:, pl.ds(depth, depth)]
    attn_load = pltpu.make_async_copy(attn_hbm, full.at[own_half], attn_sem)
    attn_load.start()
    for block in range(2):
        out_copy(block).start()
    own_rows = pl.ds(pl.multiple_of(my * quarter, quarter), quarter)
    x_copy = pltpu.make_async_copy(x_hbm.at[own_rows], x_own, x_sem)
    x_copy.start()
    gain_copy = pltpu.make_async_copy(gain_hbm, gain_ref, gain_sem)
    gain_copy.start()

    barrier = pltpu.get_barrier_semaphore()
    pl.semaphore_signal(barrier, inc=1, device_id={"mx": peer}, device_id_type=MESH)
    pl.semaphore_signal(barrier, inc=1, device_id={"my": side_x}, device_id_type=MESH)
    pl.semaphore_signal(barrier, inc=1, device_id={"my": side_y}, device_id_type=MESH)
    attn_load.wait()
    for block in range(2, out_blocks):
        out_copy(block).start()
    pl.semaphore_wait(barrier, 3)
    attn_copy = to_core(full.at[own_half], full.at[own_half], (core_sems.at[0], core_sems.at[1]))
    attn_copy.start()
    attn_copy.wait()
    for place, owner in enumerate((my, side_x, cross, side_y)):
        rows_in[place * quarter:(place + 1) * quarter, :] = full[pl.ds(pl.multiple_of(owner * quarter, quarter), quarter), :]

    sub = quarter // 2
    wide = 2 * BLOCK
    pairs = hidden // wide

    def wide_cols(pair):
        if isinstance(pair, int):
            return slice(pair * wide, (pair + 1) * wide)
        return pl.ds(pl.multiple_of(pair * wide, wide), wide)

    def first_side(parity):
        return side_x + parity * (side_y - side_x)

    def second_side(parity):
        return side_y + parity * (side_x - side_y)

    def sub_rows(index):
        if isinstance(index, int):
            return slice(index * sub, (index + 1) * sub)
        return pl.ds(pl.multiple_of(index * sub, sub), sub)

    def scatter_one(chunk, parity):
        lead = pl.ds(pl.multiple_of(sub * (1 + parity), sub), 2 * sub)
        return to_chip(part.at[chunk, lead], recv_one.at[chunk], first_side(parity), rs_sems.at[0, 0, chunk], rs_sems.at[0, 1, chunk])

    def scatter_two(chunk, parity):
        return to_chip(send_two.at[chunk], recv_two.at[chunk], second_side(parity), rs_sems.at[1, 0, chunk], rs_sems.at[1, 1, chunk])

    def scatter_store(pair, total):
        for block in range(2):
            chunk = 2 * pair + block
            pieces = [total[place * quarter + block * sub:place * quarter + (block + 1) * sub] for place in range(4)]
            for place in range(1, 4):
                part[chunk, sub_rows(place), :] = pieces[place].astype(BF16)
            keep[chunk, 0] = pieces[0]
            keep[chunk, 1] = pieces[1]
            keep[chunk, 2] = pieces[3]

    def scatter_pass(chunk, parity):
        scatter_one(chunk, parity).wait()
        send_two[chunk] = (keep[chunk, 2 - parity] + recv_one[chunk, sub_rows(1 - parity), :].astype(F32)).astype(BF16)
        scatter_two(chunk, parity).start()
        keep[chunk, 0] = keep[chunk, 0] + recv_one[chunk, sub_rows(parity), :].astype(F32)

    def scatter_end(chunk, parity):
        scatter_two(chunk, parity).wait()
        return keep[chunk, 0] + recv_two[chunk].astype(F32)

    def turn(pair, block):
        return (pair + block) % 2

    def mid_end(pair, block):
        before = x_own[sub_rows(block), wide_cols(pair)].astype(F32)
        mid[sub_rows(block), wide_cols(pair)] = (before + scatter_end(2 * pair + block, turn(pair, block))).astype(BF16).astype(F32)

    x_copy.wait()
    gain_copy.wait()
    for block in range(out_blocks):
        out_copy(block).wait()
    for chunk in range(out_slot // 2):
        for copy in ff_copies(chunk):
            copy.start()
    def out_product(pair, carry):
        weights = pool[out_slot * BLOCK:out_slot * BLOCK + depth, wide_cols(pair)]
        scatter_store(pair, jnp.dot(rows_in[...], weights, preferred_element_type=F32))
        scatter_one(2 * pair, lax.rem(pair, 2)).start()
        return carry

    lax.fori_loop(0, pairs, out_product, 0)
    gains = gain_ref[...].astype(F32)

    def square_copy(block):
        return to_core(sq_send.at[sub_rows(block)], sq_recv.at[sub_rows(block)], (core_sems.at[2 + 2 * block], core_sems.at[3 + 2 * block]))

    def square_start(block):
        square = jnp.zeros((sub, HEAD), F32)
        for start in range(0, hidden, HEAD):
            value = mid[sub_rows(block), start:start + HEAD]
            square = square + value * value
        sq_send[sub_rows(block), :] = jnp.broadcast_to(jnp.sum(square, axis=1, keepdims=True), (sub, HEAD))
        square_copy(block).start()

    def norm_rows(block):
        square_copy(block).wait()
        scale = lax.rsqrt((sq_send[sub_rows(block), :] + sq_recv[sub_rows(block), :]) / (2 * hidden) + NORM_EPS)
        for start in range(0, hidden, HEAD):
            gain = gains[start // HEAD:start // HEAD + 1, :]
            h_rows[sub_rows(block), start:start + HEAD] = (mid[sub_rows(block), start:start + HEAD] * scale * gain).astype(BF16)

    def h_block(place, pair, block):
        return h_rows.at[sub_rows(2 * place + block), wide_cols(pair)]

    def gather_x(pair, block):
        chunk = 2 * pair + block
        return to_chip(h_block(0, pair, block), h_block(1, pair, block), side_x, ag_sems.at[0, 0, chunk], ag_sems.at[0, 1, chunk])

    def gather_y(pair, block):
        chunk = 2 * pair + block
        return to_chip(h_block(0, pair, block), h_block(3, pair, block), side_y, ag_sems.at[1, 0, chunk], ag_sems.at[1, 1, chunk])

    def gather_cross(pair, block):
        chunk = 2 * pair + block
        source = 1 if turn(pair, block) == 0 else 3
        return to_chip(h_block(source, pair, block), h_block(2, pair, block), second_side(turn(pair, block)),
                       ag_sems.at[2, 0, chunk], ag_sems.at[2, 1, chunk])

    def gather_send(pair, block):
        gather_x(pair, block).start()
        gather_y(pair, block).start()

    def gather_pass(pair, block):
        (gather_y if turn(pair, block) else gather_x)(pair, block).wait_recv()
        gather_cross(pair, block).start()

    def start_late(pair):
        scatter_one(2 * pair + 1, turn(pair, 1)).start()

    def pass_late(pair):
        scatter_pass(2 * pair + 1, turn(pair, 1))

    for pair in range(2):
        start_late(pair)
    for chunk in range(out_slot // 2, chunk_ring):
        for copy in ff_copies(chunk):
            copy.start()
    for pair in range(pairs):
        scatter_pass(2 * pair, turn(pair, 0))
    for pair in range(2, pairs):
        start_late(pair)
    for pair in range(2):
        pass_late(pair)
    for pair in range(pairs):
        mid_end(pair, 0)
    square_start(0)
    norm_rows(0)
    for pair in range(2, pairs):
        pass_late(pair)
    for pair in range(pairs):
        gather_send(pair, 0)
    for pair in range(pairs):
        mid_end(pair, 1)
    square_start(1)
    for pair in range(2):
        gather_pass(pair, 0)
    norm_rows(1)
    for pair in range(pairs):
        gather_send(pair, 1)
    for pair in range(2, pairs):
        gather_pass(pair, 0)
    for pair in range(pairs):
        gather_pass(pair, 1)
    for pair in range(pairs):
        for block in range(2):
            (gather_x if turn(pair, block) else gather_y)(pair, block).wait_recv()
            gather_cross(pair, block).wait_recv()
        for place, source in enumerate((own_half, peer_half)):
            h_cols[wide_cols(pair), place * half:(place + 1) * half] = h_rows[source, wide_cols(pair)].astype(F32).T.astype(BF16)
        for block in range(2):
            gather_x(pair, block).wait_send()
            gather_y(pair, block).wait_send()
            gather_cross(pair, block).wait_send()

    def gu_copy(chunk):
        slot = lax.rem(chunk, 8)
        return to_core(gu_send.at[slot], gu_recv.at[slot], (gu_sems.at[0, slot], gu_sems.at[1, slot]))

    def act_lanes(chunk):
        place = jnp.where(chunk < early_blocks, chunk + ff_chunks - early_blocks, chunk - early_blocks)
        return pl.ds(pl.multiple_of(place * BLOCK, BLOCK), BLOCK)

    def act_copy(chunk):
        lanes = act_lanes(chunk)
        return to_core(act.at[own_half, lanes], act.at[own_half, lanes], (act_sems.at[0, lax.rem(chunk, 8)], act_sems.at[1, lax.rem(chunk, 8)]))

    def ff_products(chunk):
        slot = lax.rem(chunk, 8)
        base = ff_slot(chunk)
        product = jnp.dot(pool[slot_rows(base, 2 * BLOCK), :], h_cols[...], preferred_element_type=F32)
        for kind in range(2):
            rows = slice(kind * BLOCK, (kind + 1) * BLOCK)
            gu_own[slot, kind] = product[rows, :half]
            gu_send[slot, kind] = product[rows, half:].astype(BF16)

    def activate(chunk):
        slot = lax.rem(chunk, 8)
        gate = gu_own[slot, 0] + gu_recv[slot, 0].astype(F32)
        up = gu_own[slot, 1] + gu_recv[slot, 1].astype(F32)
        value = gate * jax.nn.sigmoid(gate) * up
        row = chunk * BLOCK + lax.broadcasted_iota(jnp.int32, value.shape, 0)
        value = jnp.where(row < ff, value, 0.0)
        lanes = act_lanes(chunk)
        act[own_half, lanes] = value.T.astype(BF16)

    def refill(chunk):
        half_ring = chunk_ring // 2

        @pl.when(chunk < late_count - 1)
        def _():
            for copy in ff_copies(late_chunk + chunk):
                copy.start()

        @pl.when(chunk == late_count - 1)
        def _():
            for copy in ff_copies(ff_chunks - 1, ff_rest):
                copy.start()

        @pl.when((chunk >= late_count) & (chunk < half_ring))
        def _():
            for copy in ff_copies(chunk - late_count + chunk_ring):
                copy.start()

        @pl.when((chunk >= half_ring) & (chunk < chunk_ring))
        def _():
            down_copy(2 * (chunk - half_ring)).start()
            down_copy(2 * (chunk - half_ring) + 1).start()

        free = 2 * (chunk - chunk_ring + late_count) - down_slot + early_blocks

        @pl.when((chunk >= chunk_ring) & (chunk < late_chunk) & (free >= early_blocks))
        def _():
            down_copy(free).start()

        @pl.when((chunk >= chunk_ring) & (chunk < late_chunk - 1))
        def _():
            down_copy(free + 1).start()

        @pl.when(chunk == late_chunk - 1)
        def _():
            down_copy(ff_chunks - 1, ff_rest).start()

    def ff_pair(pair, active):
        chunks = (2 * pair, 2 * pair + 1)
        if active:
            for chunk in chunks:
                gu_copy(chunk - 4).wait()
        for chunk in chunks:
            for copy in ff_copies(chunk):
                copy.wait()
        if active:
            for chunk in chunks:
                activate(chunk - 4)
        for chunk in chunks:
            ff_products(chunk)
        for chunk in chunks:
            gu_copy(chunk).start()
        if active:
            for chunk in chunks:
                act_copy(chunk - 4).start()
        for chunk in chunks:
            refill(chunk)

    def ff_first(pair, carry):
        ff_pair(pair, False)
        return carry

    def ff_step(pair, carry):
        @pl.when(pair >= 4)
        def _():
            for parity in range(2):
                act_copy(2 * (pair - 4) + parity).wait()
        ff_pair(pair, True)
        return carry

    last = ff_chunks - 1
    ff_pairs = last // 2
    lax.fori_loop(0, 2, ff_first, 0)
    lax.fori_loop(2, ff_pairs, ff_step, 0)

    def finish(chunk):
        gu_copy(chunk).wait()
        activate(chunk)
        act_copy(chunk).start()

    for chunk in range(2 * ff_pairs - 8, 2 * ff_pairs - 6):
        act_copy(chunk).wait()

    def ff_last(chunk, carry):
        for copy in ff_copies(chunk, ff_rest):
            copy.wait()
        ff_products(chunk)
        gu_copy(chunk).start()
        return carry

    lax.fori_loop(last, last + 1, ff_last, 0)
    for chunk in range(last - 4, last - 2):
        finish(chunk)
    for block in range(early_blocks):
        down_copy(block).wait()
    late_lanes = (ff_chunks - early_blocks) * BLOCK
    late_row = down_slot * BLOCK + late_lanes

    early_slot = 3

    def down_early(pair, carry):
        value = jnp.dot(act[:, late_lanes:], pool[late_row:, wide_cols(pair)], preferred_element_type=F32)
        for piece in range(4):
            gu_own[early_slot + 2 * pair + piece // 2, piece % 2] = value[:, piece * half:(piece + 1) * half]
        return carry

    lax.fori_loop(0, 1, down_early, 0)
    for chunk in range(last - 2, ff_chunks):
        finish(chunk)
    lax.fori_loop(1, 2, down_early, 0)
    for block in range(early_blocks, ff_chunks):
        down_copy(block, ff_rest if block == last else BLOCK).wait()
    for chunk in range(2 * ff_pairs - 6, ff_chunks):
        act_copy(chunk).wait()

    def out_block(owner, chunk):
        pair, block = chunk // 2, chunk % 2
        return out_ref.at[sub_rows(2 * owner + block), wide_cols(pair)]

    def final_x(chunk):
        target = out_block(my, chunk)
        return to_chip(target, target, side_x, ag_sems.at[0, 0, chunk], ag_sems.at[0, 1, chunk])

    def final_y(chunk):
        target = out_block(my, chunk)
        return to_chip(target, target, side_y, ag_sems.at[1, 0, chunk], ag_sems.at[1, 1, chunk])

    def final_cross(chunk):
        target = out_block(first_side(chunk % 2), chunk)
        return to_chip(target, target, second_side(chunk % 2), ag_sems.at[2, 0, chunk], ag_sems.at[2, 1, chunk])

    def out_end(chunk):
        pair, block = chunk // 2, chunk % 2
        value = mid[sub_rows(block), wide_cols(pair)] + scatter_end(chunk, block)
        out_ref[sub_rows(2 * my + block), wide_cols(pair)] = value.astype(BF16)
        final_x(chunk).start()
        final_y(chunk).start()

    def out_pass(chunk):
        (final_x if chunk % 2 == 0 else final_y)(chunk).wait_recv()
        final_cross(chunk).start()

    def scatter_start(pair, total):
        scatter_store(pair, total)
        for block in range(2):
            scatter_one(2 * pair + block, block).start()

    def down_rest(pair, carry):
        total = jnp.dot(act[:, :late_lanes], pool[down_slot * BLOCK:late_row, wide_cols(pair)], preferred_element_type=F32)
        pieces = [gu_own[early_slot + 2 * pair + piece // 2, piece % 2] for piece in range(4)]
        scatter_start(pair, jnp.concatenate(pieces, axis=1) + total)
        return carry

    def down_pair(pair, carry):
        scatter_start(pair, jnp.dot(act[...], pool[down_slot * BLOCK:, wide_cols(pair)], preferred_element_type=F32))

        @pl.when(pair >= 3)
        def _():
            for parity in range(2):
                scatter_pass(2 * (pair - 3) + parity, parity)
        return carry

    lax.fori_loop(0, 2, down_rest, 0)
    lax.fori_loop(2, pairs, down_pair, 0)

    def each(step, pair):
        for chunk in (2 * pair, 2 * pair + 1):
            if step is scatter_pass:
                step(chunk, chunk % 2)
            else:
                step(chunk)

    for pair in range(pairs - 3, pairs):
        each(scatter_pass, pair)
        each(out_end, pair - pairs + 3)
    each(out_pass, 0)
    for pair in range(3, pairs):
        each(out_end, pair)
        each(out_pass, pair - 2)
    for pair in range(pairs - 2, pairs):
        each(out_pass, pair)
    for chunk in range(col_chunks):
        (final_y if chunk % 2 == 0 else final_x)(chunk).wait_recv()
        final_cross(chunk).wait_recv()
    for chunk in range(col_chunks):
        final_cross(chunk).wait_send()
        final_x(chunk).wait_send()
        final_y(chunk).wait_send()


def tail(attn_rows, gain, x_in, w_o, wg_rows, wu_rows, w_down):
    half, depth = attn_rows.shape
    rows, hidden = x_in.shape
    quarter = rows // 4
    chunks = hidden // BLOCK
    ff_chunks = pl.cdiv(w_down.shape[0], BLOCK)
    return pl.pallas_call(
        tail_kernel,
        name="tail",
        out_shape=jax.ShapeDtypeStruct((rows, hidden), BF16),
        in_specs=any_specs(7),
        out_specs=vmem_specs(1)[0],
        scratch_shapes=[
            VMEM((hidden // HEAD, HEAD), BF16),
            DMA,
            VMEM((RING * BLOCK, hidden), BF16),
            VMEM((chunks, 2 * quarter, 2 * BLOCK), BF16),
            VMEM((chunks, 3, quarter // 2, 2 * BLOCK), F32),
            VMEM((chunks, quarter, 2 * BLOCK), BF16),
            VMEM((chunks, quarter // 2, 2 * BLOCK), BF16),
            VMEM((chunks, quarter // 2, 2 * BLOCK), BF16),
            VMEM((quarter, hidden), BF16),
            VMEM((quarter, hidden), F32),
            VMEM((quarter, HEAD), F32),
            VMEM((quarter, HEAD), F32),
            VMEM((rows, hidden), BF16),
            VMEM((hidden, rows), BF16),
            VMEM((8, 2, BLOCK, half), BF16),
            VMEM((8, 2, BLOCK, half), BF16),
            VMEM((8, 2, BLOCK, half), F32),
            VMEM((rows, ff_chunks * BLOCK), BF16),
            DMA((RING,)),
            DMA,
            DMA,
            DMA((6,)),
            DMA((2, 2, chunks)),
            DMA((3, 2, chunks)),
            DMA((2, 8)),
            DMA((2, 8)),
        ],
        compiler_params=pltpu.CompilerParams(collective_id=1, has_side_effects=True, vmem_limit_bytes=67043328),
    )(lane_rows(gain), attn_rows, x_in, w_o, wg_rows, wu_rows, w_down)


def solution(mesh):
    act_spec = P(None, "mx")
    cache_spec = P("mx", None, "my", None)
    in_specs = (act_spec, P("mx"), P("mx"), P("mx"), P("mx", "my"), P("my"), P("mx", "my"), P("my"), P("mx", "my"), P("my"), P("my", "mx"), P("mx", "my"), P("mx", "my"), P("my", "mx"), cache_spec, cache_spec)
    out_specs = (act_spec, cache_spec, cache_spec)

    def local_layer(x_in, seq_lens, gain_attn, gain_mlp, w_q, b_q, w_k, b_k, w_v, b_v, w_o, w_gate, w_up, w_down, k_cache, v_cache):
        q_rot, kv_new = project(x_in, seq_lens, gain_attn, b_q, b_k, b_v, w_q, w_k, w_v)
        attn_rows, k_cache_out, v_cache_out = attend(seq_lens, q_rot, kv_new, k_cache, v_cache)
        x_out = tail(attn_rows, gain_mlp, x_in, w_o, w_gate.T, w_up.T, w_down)
        return x_out, k_cache_out, v_cache_out

    return jax.shard_map(local_layer, mesh=mesh, in_specs=in_specs, out_specs=out_specs, check_vma=False)
```
